8 devices in a mesh: replica: 2 (over z, y), stage: 4 (over x, core).
Axes of the slice: x: 2, y: 2, z: 1, core: 2. Of those that a mesh axis runs over, the one named last changes fastest.
Arguments:
- embeddings: bfloat16 [3072, 2048], P('replica'), parts along dimension 0
- valid_len: int32 [2], P('replica'), parts along dimension 0
- attn_gain: float32 [4, 2048], P('stage')
- w_q: bfloat16 [4, 2048, 32, 64], P('stage')
- w_k: bfloat16 [4, 2048, 8, 64], P('stage')
- w_v: bfloat16 [4, 2048, 8, 64], P('stage')
- w_o: bfloat16 [4, 32, 64, 2048], P('stage')
- mlp_gain: float32 [4, 2048], P('stage')
- w_gate: bfloat16 [4, 2048, 8192], P('stage')
- w_up: bfloat16 [4, 2048, 8192], P('stage')
- w_down: bfloat16 [4, 8192, 2048], P('stage')
Outputs:
- output 1: bfloat16 [3072, 2048], P(('replica', 'stage')), parts along dimension 0
- output 2: bfloat16 [4, 3072, 8, 64], P('stage', 'replica'), parts along dimension 1
- output 3: bfloat16 [4, 3072, 8, 64], P('stage', 'replica'), parts along dimension 1
There are 2 independent parts. The reference program is written for one: setup_inputs(seed, part) draws one part's arguments, and reference() takes and returns one part's arrays. A program takes and returns all parts, laid end to end along the dimension named above; an argument that names none is the same for every part.
All inputs are finite; a program needn't handle non-finite values.
Results may differ from the reference program's by a relative error of at most 0.02.
Values are sent between devices in bfloat16 or wider.
A program may use at most 1 GiB of HBM per device.

```python
import jax
import jax.numpy as jnp
from jax import lax

D = 2048
HEADS = 32
KV_HEADS = 8
HEAD = 64
FF = 8192
LAYERS = 4
SEQ = 1536

GROUP = HEADS // KV_HEADS
HALF = HEAD // 2
QBLOCK = min(SEQ, 128)
EPS = 1e-5
ROPE_BASE = 10000.0
NEG_BIG = -1e30


def setup_inputs(seed: int = 0, part: int = 0) -> dict:
    part_key = jax.random.fold_in(jax.random.key(seed), part)
    embed_key, len_key = jax.random.split(part_key)
    weight_keys = jax.random.split(jax.random.key(seed + 1), 9)

    def normal_weight(draw_key, arr_shape, std_scale):
        return (jax.random.normal(draw_key, arr_shape, jnp.float32) * std_scale).astype(jnp.bfloat16)

    embeddings = jax.random.normal(embed_key, (SEQ, D), jnp.float32).astype(jnp.bfloat16)
    valid_len = jax.random.randint(len_key, (1,), SEQ // 2, SEQ - SEQ // 8 + 1, jnp.int32)
    return {
        'embeddings': embeddings,
        'valid_len': valid_len,
        'attn_gain': jax.random.uniform(weight_keys[0], (LAYERS, D), jnp.float32, 0.6, 1.4),
        'w_q': normal_weight(weight_keys[1], (LAYERS, D, HEADS, HEAD), 2.0 * D ** -0.5),
        'w_k': normal_weight(weight_keys[2], (LAYERS, D, KV_HEADS, HEAD), D ** -0.5),
        'w_v': normal_weight(weight_keys[3], (LAYERS, D, KV_HEADS, HEAD), D ** -0.5),
        'w_o': normal_weight(weight_keys[4], (LAYERS, HEADS, HEAD, D), (HEADS * HEAD) ** -0.5),
        'mlp_gain': jax.random.uniform(weight_keys[5], (LAYERS, D), jnp.float32, 0.6, 1.4),
        'w_gate': normal_weight(weight_keys[6], (LAYERS, D, FF), D ** -0.5),
        'w_up': normal_weight(weight_keys[7], (LAYERS, D, FF), D ** -0.5),
        'w_down': normal_weight(weight_keys[8], (LAYERS, FF, D), FF ** -0.5),
    }


def rms_norm(hidden, norm_gain):
    hid32 = hidden.astype(jnp.float32)
    inv_rms = lax.rsqrt(jnp.mean(hid32 * hid32, axis=-1, keepdims=True) + EPS)
    return (hid32 * inv_rms * norm_gain).astype(jnp.bfloat16)


def apply_rope(values, cos_tab, sin_tab):
    front_half = values[..., :HALF]
    back_half = values[..., HALF:]
    return jnp.concatenate([front_half * cos_tab - back_half * sin_tab, back_half * cos_tab + front_half * sin_tab], axis=-1)


def reference(embeddings, valid_len, attn_gain, w_q, w_k, w_v, w_o, mlp_gain, w_gate, w_up, w_down):
    positions = jnp.arange(SEQ)
    inv_freq = ROPE_BASE ** (-jnp.arange(HALF).astype(jnp.float32) * (2.0 / HEAD))
    angles = positions.astype(jnp.float32)[:, None] * inv_freq[None, :]
    cos_tab = jnp.cos(angles)[:, None, :]
    sin_tab = jnp.sin(angles)[:, None, :]
    key_ok = positions < valid_len[0]
    n_blocks = SEQ // QBLOCK

    def layer_fn(hidden, layer_params):
        a_gain, wq_l, wk_l, wv_l, wo_l, m_gain, wg_l, wu_l, wd_l = layer_params
        normed = rms_norm(hidden, a_gain).astype(jnp.float32)
        q_proj = jnp.einsum('sd,dhk->shk', normed, wq_l.astype(jnp.float32))
        k_proj = jnp.einsum('sd,dhk->shk', normed, wk_l.astype(jnp.float32))
        v_new = jnp.einsum('sd,dhk->shk', normed, wv_l.astype(jnp.float32)).astype(jnp.bfloat16)
        q_rot = apply_rope(q_proj, cos_tab, sin_tab).astype(jnp.bfloat16)
        k_rot = apply_rope(k_proj, cos_tab, sin_tab).astype(jnp.bfloat16)
        q_blocks = q_rot.astype(jnp.float32).reshape(n_blocks, QBLOCK, KV_HEADS, GROUP, HEAD)
        k_all = k_rot.astype(jnp.float32)
        v_all = v_new.astype(jnp.float32)

        def attend(block_in):
            block_idx, q_block = block_in
            q_pos = block_idx * QBLOCK + jnp.arange(QBLOCK)
            scores = jnp.einsum('qhgd,khd->hgqk', q_block, k_all) * (HEAD ** -0.5)
            allowed = (positions[None, :] <= q_pos[:, None]) & key_ok[None, :]
            scores = jnp.where(allowed, scores, NEG_BIG)
            probs_all = jax.nn.softmax(scores, axis=-1).astype(jnp.bfloat16).astype(jnp.float32)
            return jnp.einsum('hgqk,khd->qhgd', probs_all, v_all).astype(jnp.bfloat16)

        attn_heads = lax.map(attend, (jnp.arange(n_blocks), q_blocks)).reshape(SEQ, HEADS, HEAD)
        attn_out = jnp.einsum('shk,hkd->sd', attn_heads.astype(jnp.float32), wo_l.astype(jnp.float32))
        hidden = (hidden.astype(jnp.float32) + attn_out).astype(jnp.bfloat16)
        normed = rms_norm(hidden, m_gain)
        gate_proj = jnp.dot(normed, wg_l, preferred_element_type=jnp.float32)
        up_proj = jnp.dot(normed, wu_l, preferred_element_type=jnp.float32)
        act_val = (jax.nn.silu(gate_proj) * up_proj).astype(jnp.bfloat16)
        down_proj = jnp.dot(act_val, wd_l, preferred_element_type=jnp.float32)
        hidden = (hidden.astype(jnp.float32) + down_proj).astype(jnp.bfloat16)
        return hidden, (k_rot, v_new)

    hidden_out, caches = lax.scan(layer_fn, embeddings, (attn_gain, w_q, w_k, w_v, w_o, mlp_gain, w_gate, w_up, w_down))
    return hidden_out, caches[0], caches[1]
```

```python
import math

import jax
import jax.numpy as jnp
import numpy as np
from jax import lax
from jax.experimental import pallas as pl
from jax.experimental.pallas import tpu as pltpu
from jax.sharding import PartitionSpec as P

EPS = 1e-5
ROPE_BASE = 10000.0
NEG = -1e30

SEQ = 1536
D = 2048
HEADS = 32
KV = 8
HD = 64
FF = 8192
STAGES = 4
B = 192
NB = SEQ // B
F = 512
NC = FF // F
NG = NB * NC
VMIN = 768
VMAX = 1344
KEYMAX = VMAX // B
RG = 4
RD = 3
EXP_SCALE = math.log2(math.e)

F32 = jnp.float32
BF16 = jnp.bfloat16


def rope_tables():
    inv_freq = ROPE_BASE ** (-np.arange(HD // 2, dtype=np.float64) * (2.0 / HD))
    angles = inv_freq[:, None] * np.arange(SEQ, dtype=np.float64)[None, :]
    tab = np.zeros((NB, 2, HD // 2, 256), np.float32)
    for blk in range(NB):
        cols = slice(blk * B, (blk + 1) * B)
        tab[blk, 0, :, :B] = np.cos(angles[:, cols])
        tab[blk, 1, :, :B] = np.sin(angles[:, cols])
    return tab


def dot(a, b):
    return jnp.dot(a, b, preferred_element_type=F32)


def stage_kernel(emb, valid, again, wq, wk, wv, wo, mgain, wg, wu, wd, tab_hbm,
                 hid, kout, vout,
                 tab, wqkv_v, wo_v, wg_r, wu_r, wd_r, resid, kc, kT, vT, act, aT, qT, y, sbuf, ffa,
                 mask_x, mask_y, vbias,
                 w_sem, tab_sem, g_sem, u_sem, d_sem, in_sem, send_sem, kv_sem, out_sem):
    stage = lax.axis_index("stage")
    barrier = pltpu.get_barrier_semaphore()
    for k in range(1, STAGES):
        pl.semaphore_signal(barrier, inc=1, device_id={"stage": lax.rem(stage + k, STAGES)},
                            device_id_type=pl.DeviceIdType.MESH)

    def emb_copy(i):
        return pltpu.make_async_copy(emb.at[pl.ds(pl.multiple_of(i * B, B), B), :], resid.at[i], in_sem.at[i])

    def w_copy(p):
        if p < 4:
            src = wq.at[pl.ds(p * 512, 512), :]
        elif p == 4:
            src = wk
        elif p == 5:
            src = wv
        else:
            src = wo.at[pl.ds((p - 6) * 512, 512), :]
        dst = wqkv_v.at[pl.ds(p * 512, 512), :] if p < 6 else wo_v.at[pl.ds((p - 6) * 512, 512), :]
        return pltpu.make_async_copy(src, dst, w_sem.at[p])

    def g_copy(g):
        cols = pl.ds(pl.multiple_of(lax.rem(g, NC) * F, F), F)
        slot = lax.rem(g, RG)
        return pltpu.make_async_copy(wg.at[:, cols], wg_r.at[slot], g_sem.at[slot])

    def u_copy(g):
        cols = pl.ds(pl.multiple_of(lax.rem(g, NC) * F, F), F)
        slot = lax.rem(g, RG)
        return pltpu.make_async_copy(wu.at[:, cols], wu_r.at[slot], u_sem.at[slot])

    def d_copy(g):
        rows = pl.ds(pl.multiple_of(lax.rem(g, NC) * F, F), F)
        slot = lax.rem(g, RD)
        return pltpu.make_async_copy(wd.at[rows, :], wd_r.at[slot], d_sem.at[slot])

    tab_copy = pltpu.make_async_copy(tab_hbm, tab, tab_sem)

    @pl.when(stage == 0)
    def _():
        emb_copy(0).start()

    w_copy(0).start()
    tab_copy.start()
    for p in range(1, 10):
        w_copy(p).start()
    for g in range(RG - 1):
        g_copy(g).start()
        u_copy(g).start()
    d_copy(0).start()

    act[pl.ds(B, 256 - B), :] = jnp.zeros((256 - B, D), BF16)
    for g in range(KV):
        qT[g, pl.ds((1 - g % 2) * HD, HD), :] = jnp.zeros((HD, 4 * B), BF16)
    valid_pos = valid[0]
    vrow = lax.broadcasted_iota(jnp.int32, vbias.shape, 0) + VMIN
    vbias[...] = jnp.where(vrow < valid_pos, 0.0, NEG).astype(F32)
    tab_copy.wait()
    pl.semaphore_wait(barrier, STAGES - 1)

    def norm(i, gain_ref):
        for r in range(0, B, 16):
            x = resid[i, pl.ds(r, 16), :].astype(F32)
            inv = lax.rsqrt(jnp.mean(x * x, axis=-1, keepdims=True) + EPS)
            act[pl.ds(r, 16), :] = (x * inv * gain_ref[...]).astype(BF16)

    def rope(x, cos, sin):
        front = x[:HD // 2]
        back = x[HD // 2:]
        return front * cos - back * sin, back * cos + front * sin

    def put_tokens(ref, i, rows, val):
        base = (i // 2) * (2 * B)
        lo = pl.multiple_of(base, 128)

        @pl.when(lax.rem(i, 2) == 0)
        def _():
            ref[rows, pl.ds(lo, 256)] = val.astype(BF16)

        @pl.when(lax.rem(i, 2) == 1)
        def _():
            rolled = pltpu.roll(val, 64, 1)
            lane = lax.broadcasted_iota(jnp.int32, (val.shape[0], 128), 1)
            mid = pl.multiple_of(base + 128, 128)
            old = ref[rows, pl.ds(mid, 128)].astype(F32)
            ref[rows, pl.ds(mid, 128)] = jnp.where(lane < 64, old, rolled[:, :128]).astype(BF16)
            hi = pl.multiple_of(base + 256, 128)
            ref[rows, pl.ds(hi, 128)] = rolled[:, 128:].astype(BF16)

    def project(i):
        for n in range(8):
            aT[pl.ds(n * 256, 256), :] = act[:, pl.ds(n * 256, 256)].T
        cos = tab[i, 0]
        sin = tab[i, 1]
        lane = lax.broadcasted_iota(jnp.int32, (HD, 128), 1)

        def q_pair(pair, _):
            rows = pl.ds(pl.multiple_of(pair * 512, 512), 512)
            qt = dot(wqkv_v[rows, :], aT[...])
            for gg in range(2):
                heads = []
                for h in range(4):
                    f, b = rope(qt[(gg * 4 + h) * HD:(gg * 4 + h + 1) * HD], cos, sin)
                    heads.append(jnp.concatenate([f, b], axis=0) * 0.125)
                lead = [x[:, :128] for x in heads]
                tail = [x[:, 128:] for x in heads]
                lead.append(jnp.where(lane < 64, tail[0], pltpu.roll(tail[1], 64, 1)))
                lead.append(jnp.where(lane < 64, tail[2], pltpu.roll(tail[3], 64, 1)))
                for t in range(6):
                    qT[pair * 2 + gg, pl.ds(gg * HD, HD), pl.ds(t * 128, 128)] = lead[t].astype(BF16)
            return 0

        lax.fori_loop(0, 4, q_pair, 0)

        for half in range(2):
            kt = dot(wqkv_v[pl.ds(2048 + half * 256, 256), :], aT[...])
            parts = []
            for h in range(4):
                parts += list(rope(kt[h * HD:(h + 1) * HD], cos, sin))
            kt = jnp.concatenate(parts, axis=0)
            put_tokens(kT, i, pl.ds(half * 256, 256), kt)
            kc[pl.ds(pl.multiple_of(i * B, B), B), pl.ds(half * 256, 256)] = kt.astype(BF16).T[:B]
        for half in range(2):
            vt = dot(wqkv_v[pl.ds(2560 + half * 256, 256), :], aT[...])
            put_tokens(vT, i, pl.ds(half * 256, 256), vt)

    def masks(i):
        key = lax.broadcasted_iota(jnp.int32, (128, 128), 0)
        tok = lax.broadcasted_iota(jnp.int32, (128, 128), 1)
        ok = (key <= tok) & (key + i * B < valid_pos)
        mask_x[...] = jnp.where(ok, 0.0, NEG).astype(F32)
        key = lax.broadcasted_iota(jnp.int32, (B, 128), 0)
        tok = lax.broadcasted_iota(jnp.int32, (B, 128), 1)
        tok = 128 + jnp.where(tok < 64, tok, tok - 64)
        ok = (key <= tok) & (key + i * B < valid_pos)
        mask_y[...] = jnp.where(ok, 0.0, NEG).astype(F32)

    def attend(n):
        chunks = min(n + 1, KEYMAX)

        def group(g, _):
            kcols = pl.ds(pl.multiple_of((g // 2) * 128, 128), 128)
            outs = []
            for t in range(3):
                sref = y if t == 0 else sbuf.at[t - 1]
                q = qT[g, :, pl.ds(t * 256, 256)]
                m = None
                spans = []
                for c in range(chunks):
                    rows = 128 if (c == n and t < 2) else B
                    s = dot(kc[pl.ds(c * B, rows), kcols], q)
                    if c == n:
                        mk = mask_x[...] if t < 2 else mask_y[...]
                        s = s + jnp.concatenate([mk, mk], axis=1)
                    elif c * B >= VMIN:
                        mk = vbias[pl.ds(c * B - VMIN, B), :]
                        s = s + jnp.concatenate([mk, mk], axis=1)
                    sref[pl.ds(c * B, rows), :] = s
                    cm = jnp.max(s.reshape(rows // 8, 8, 256), axis=0)
                    m = cm if m is None else jnp.maximum(m, cm)
                    spans.append((c * B, rows))
                mc = jnp.max(m, axis=0, keepdims=True) * EXP_SCALE
                l = None
                probs = []
                for start, rows in spans:
                    p = jnp.exp2(sref[pl.ds(start, rows), :] * EXP_SCALE - mc)
                    ls = jnp.sum(p.reshape(rows // 8, 8, 256), axis=0)
                    l = ls if l is None else l + ls
                    probs.append(p.astype(BF16))
                total = spans[-1][0] + spans[-1][1]
                o = dot(vT[pl.ds(pl.multiple_of(g * HD, HD), HD), pl.ds(0, total)], jnp.concatenate(probs, axis=0))
                outs.append(o * (1.0 / jnp.sum(l, axis=0, keepdims=True)))
            lead = jnp.concatenate([outs[0][:, :128], outs[0][:, 128:], outs[1][:, :128], outs[1][:, 128:]], axis=0)
            t0 = outs[2][:, :128]
            t1 = outs[2][:, 128:]
            tail = jnp.concatenate([t0, pltpu.roll(t0, 64, 1), t1, pltpu.roll(t1, 64, 1)], axis=0)
            ocols = pl.ds(pl.multiple_of(g * 256, 256), 256)
            act[pl.ds(0, 128), ocols] = lead.astype(BF16).T
            act[pl.ds(128, 64), ocols] = tail.astype(BF16).T[:64]
            return 0

        lax.fori_loop(0, KV, group, 0)

    def out_proj(i):
        for n in range(4):
            cols = pl.ds(n * 512, 512)
            o = dot(act[pl.ds(0, B), :], wo_v[:, cols])
            resid[i, :, cols] = (resid[i, :, cols].astype(F32) + o).astype(BF16)

    def gate_up(g):
        g_copy(g).wait()
        u_copy(g).wait()

        @pl.when(g + RG - 1 < NG)
        def _():
            g_copy(g + RG - 1).start()
            u_copy(g + RG - 1).start()

        @pl.when(g + 1 < NG)
        def _():
            d_copy(g + 1).start()

        slot = lax.rem(g, RG)
        x = act[pl.ds(0, B), :]
        gate = dot(x, wg_r[slot])
        up = dot(x, wu_r[slot])
        ffa[lax.rem(g, 2)] = (gate * jax.nn.sigmoid(gate) * up).astype(BF16)

    def down(g):
        slot = lax.rem(g, RD)
        x = ffa[lax.rem(g, 2)]
        for n in range(8):
            rows = pl.ds(n * B, B)
            y[rows, :] = y[rows, :] + dot(x, wd_r[slot, :, pl.ds(n * 256, 256)])

    def mlp(i):
        for n in range(8):
            y[pl.ds(n * B, B), :] = resid[i, :, pl.ds(n * 256, 256)].astype(F32)
        g0 = i * NC
        gate_up(g0)

        def step(c, _):
            g = g0 + c
            d_copy(g - 1).wait()
            gate_up(g)
            down(g - 1)
            return 0

        lax.fori_loop(1, NC, step, 0)
        d_copy(g0 + NC - 1).wait()
        down(g0 + NC - 1)
        for n in range(8):
            resid[i, :, pl.ds(n * 256, 256)] = y[pl.ds(n * B, B), :].astype(BF16)

    def next_copy(i):
        return pltpu.make_async_remote_copy(resid.at[i], resid.at[i], send_sem.at[i], in_sem.at[i],
                                            device_id={"stage": lax.rem(stage + 1, STAGES)},
                                            device_id_type=pl.DeviceIdType.MESH)

    def owner_copy(i):
        part = lax.rem(i, 2)
        return pltpu.make_async_remote_copy(resid.at[i], hid.at[pl.ds(pl.multiple_of(part * B, B), B), :],
                                            send_sem.at[i], out_sem.at[part],
                                            device_id={"stage": i // 2}, device_id_type=pl.DeviceIdType.MESH)

    def own_copy(i):
        part = lax.rem(i, 2)
        return pltpu.make_async_copy(resid.at[i], hid.at[pl.ds(pl.multiple_of(part * B, B), B), :], out_sem.at[part])

    def kv_copy(j, which):
        cols = pl.ds(pl.multiple_of(j * 2 * B, 2 * B), 2 * B)
        src, dst = ((kT, kout), (vT, vout))[which]
        return pltpu.make_async_copy(src.at[:, cols], dst.at[:, cols], kv_sem.at[which, j])

    def block(i, _):
        emb_copy(i).wait()

        @pl.when((stage == 0) & (i + 1 < NB))
        def _():
            emb_copy(i + 1).start()

        norm(i, again)

        @pl.when(i == 0)
        def _():
            for p in range(6):
                w_copy(p).wait()

        project(i)
        masks(i)
        for n in range(NB):
            @pl.when(i == n)
            def _():
                attend(n)

        @pl.when(i == 0)
        def _():
            for p in range(6, 10):
                w_copy(p).wait()

        out_proj(i)
        norm(i, mgain)
        mlp(i)

        @pl.when(lax.rem(i, 2) == 1)
        def _():
            kv_copy(i // 2, 0).start()
            kv_copy(i // 2, 1).start()

        @pl.when(stage < STAGES - 1)
        def _():
            next_copy(i).start()

        @pl.when((stage == STAGES - 1) & (i < NB - 2))
        def _():
            owner_copy(i).start()

        @pl.when((stage == STAGES - 1) & (i >= NB - 2))
        def _():
            own_copy(i).start()

        return 0

    lax.fori_loop(0, NB, block, 0)

    @pl.when(stage < STAGES - 1)
    def _():
        for i in range(NB):
            next_copy(i).wait_send()

    @pl.when(stage == STAGES - 1)
    def _():
        for i in range(NB - 2):
            owner_copy(i).wait_send()

    for part in range(2):
        own_copy(part).wait()
    for j in range(NB // 2):
        kv_copy(j, 0).wait()
        kv_copy(j, 1).wait()


def solution(mesh):
    gain_spec = P('stage', None)
    spec_three = P('stage', None, None)
    spec_four = P('stage', None, None, None)
    table = rope_tables()
    dma = pltpu.SemaphoreType.DMA

    def stage_program(embeddings, valid_len, attn_gain, w_q, w_k, w_v, w_o, mlp_gain, w_gate, w_up, w_down):
        wq = w_q[0].transpose(1, 2, 0).reshape(HEADS * HD, D)
        wk = w_k[0].transpose(1, 2, 0).reshape(KV * HD, D)
        wv = w_v[0].transpose(1, 2, 0).reshape(KV * HD, D)
        wo = w_o[0].reshape(HEADS * HD, D)
        any_spec = pl.BlockSpec(memory_space=pl.ANY)
        vmem_spec = pl.BlockSpec(memory_space=pltpu.VMEM)
        smem_spec = pl.BlockSpec(memory_space=pltpu.SMEM)
        hid, k_t, v_t = pl.pallas_call(
            stage_kernel,
            name="stage_pipeline",
            out_shape=(jax.ShapeDtypeStruct((SEQ // STAGES, D), BF16),
                       jax.ShapeDtypeStruct((KV * HD, SEQ), BF16),
                       jax.ShapeDtypeStruct((KV * HD, SEQ), BF16)),
            in_specs=[any_spec, smem_spec, vmem_spec, any_spec, any_spec, any_spec, any_spec, vmem_spec,
                      any_spec, any_spec, any_spec, any_spec],
            out_specs=(any_spec, any_spec, any_spec),
            scratch_shapes=[
                pltpu.VMEM((NB, 2, HD // 2, 256), F32),
                pltpu.VMEM((3072, D), BF16),
                pltpu.VMEM((D, D), BF16),
                pltpu.VMEM((RG, D, F), BF16),
                pltpu.VMEM((RG, D, F), BF16),
                pltpu.VMEM((RD, F, D), BF16),
                pltpu.VMEM((NB, B, D), BF16),
                pltpu.VMEM((SEQ, KV * HD), BF16),
                pltpu.VMEM((KV * HD, SEQ), BF16),
                pltpu.VMEM((KV * HD, SEQ), BF16),
                pltpu.VMEM((256, D), BF16),
                pltpu.VMEM((D, 256), BF16),
                pltpu.VMEM((KV, 2 * HD, 4 * B), BF16),
                pltpu.VMEM((8 * B, 256), F32),
                pltpu.VMEM((2, VMAX, 256), F32),
                pltpu.VMEM((2, B, F), BF16),
                pltpu.VMEM((128, 128), F32),
                pltpu.VMEM((B, 128), F32),
                pltpu.VMEM((VMAX - VMIN, 128), F32),
                dma((10,)), dma, dma((RG,)), dma((RG,)), dma((RD,)), dma((NB,)), dma((NB,)),
                dma((2, NB // 2)), dma((2,)),
            ],
            compiler_params=pltpu.CompilerParams(collective_id=0, has_side_effects=True,
                                                 vmem_limit_bytes=67043328),
        )(embeddings, valid_len, attn_gain, wq, wk, wv, wo, mlp_gain, w_gate[0], w_up[0], w_down[0],
          jnp.asarray(table))

        def to_cache(x):
            return x.reshape(KV, HD, SEQ).transpose(2, 0, 1)[None]

        return hid, to_cache(k_t), to_cache(v_t)

    return jax.shard_map(stage_program, mesh=mesh,
                         in_specs=(P('replica', None), P('replica'), gain_spec, spec_four, spec_four, spec_four, spec_four,
                                   gain_spec, spec_three, spec_three, spec_three),
                         out_specs=(P(('replica', 'stage'), None), P('stage', 'replica', None, None), P('stage', 'replica', None, None)),
                         check_vma=False)
```

```python
import math

import jax
import jax.numpy as jnp
import numpy as np
from jax import lax
from jax.experimental import pallas as pl
from jax.experimental.pallas import tpu as pltpu
from jax.sharding import PartitionSpec as P

EPS = 1e-5
ROPE_BASE = 10000.0
NEG = -1e30

SEQ = 1536
D = 2048
HEADS = 32
KV = 8
HD = 64
FF = 8192
STAGES = 4
B = 256
NB = SEQ // B
F = 512
NC = FF // F
NS = 3
VMIN = 768
VMAX = 1344
PIECE = SEQ // STAGES // 3
PER = B // PIECE
R = 4
SB = 2
AHEAD = 1
EXP_SCALE = math.log2(math.e)

F32 = jnp.float32
BF16 = jnp.bfloat16


def rope_tables():
    inv_freq = ROPE_BASE ** (-np.arange(HD // 2, dtype=np.float64) * (2.0 / HD))
    angles = inv_freq[:, None] * np.arange(SEQ, dtype=np.float64)[None, :]
    tab = np.zeros((NB, 2, HD // 2, 256), np.float32)
    for blk in range(NB):
        cols = slice(blk * B, (blk + 1) * B)
        tab[blk, 0, :, :B] = np.cos(angles[:, cols])
        tab[blk, 1, :, :B] = np.sin(angles[:, cols])
    return tab


def dot(a, b):
    return jnp.dot(a, b, preferred_element_type=F32)


def stage_kernel(emb, valid, again, wq, wk, wv, wo, mgain, wg, wu, wd, tab_hbm,
                 hid, kout, vout,
                 tab, wqkv_v, wo_v, wg_s, wu_s, wd_s, resid, kc, kst, vT, act, aT, qT, y, sbuf, mbuf, ff_s,
                 mask, vbias,
                 w_sem, tab_sem, g_sem, u_sem, d_sem, in_sem, send_sem, kv_sem, piece_sem, out_sem, credit):
    stage = lax.axis_index("stage")
    barrier = pltpu.get_barrier_semaphore()
    for k in range(1, STAGES):
        pl.semaphore_signal(barrier, inc=1, device_id={"stage": lax.rem(stage + k, STAGES)},
                            device_id_type=pl.DeviceIdType.MESH)

    def emb_copy(i):
        return pltpu.make_async_copy(emb.at[pl.ds(pl.multiple_of(i * B, B), B), :], resid.at[lax.rem(i, NS)], in_sem.at[lax.rem(i, NS)])

    def w_copy(p):
        if p < 4:
            src = wq.at[pl.ds(p * 512, 512), :]
        elif p == 4:
            src = wk
        elif p == 5:
            src = wv
        else:
            src = wo.at[pl.ds((p - 6) * 512, 512), :]
        dst = wqkv_v.at[pl.ds(p * 512, 512), :] if p < 6 else wo_v.at[pl.ds((p - 6) * 512, 512), :]
        return pltpu.make_async_copy(src, dst, w_sem.at[p])

    def gu_copy(c, s):
        cols = pl.ds(pl.multiple_of(c * F, F), F)
        return (pltpu.make_async_copy(wg.at[:, cols], wg_s[s], g_sem.at[s]),
                pltpu.make_async_copy(wu.at[:, cols], wu_s[s], u_sem.at[s]))

    def dn_copy(c, s):
        rows = pl.ds(pl.multiple_of(c * F, F), F)
        return pltpu.make_async_copy(wd.at[rows, :], wd_s[s], d_sem.at[s])

    tab_copy = pltpu.make_async_copy(tab_hbm, tab, tab_sem)

    @pl.when(stage == 0)
    def _():
        emb_copy(0).start()

    w_copy(0).start()
    tab_copy.start()
    for p in range(1, 10):
        w_copy(p).start()
    for c in range(R):
        for cp in gu_copy(c, c):
            cp.start()
        dn_copy(c, c).start()

    for g in range(KV):
        qT[g, pl.ds((1 - g % 2) * HD, HD), :] = jnp.zeros((HD, 4 * B), BF16)
    valid_pos = valid[0]
    vrow = lax.broadcasted_iota(jnp.int32, vbias.shape, 0) + VMIN
    vbias[...] = jnp.where(vrow < valid_pos, 0.0, NEG).astype(F32)
    tab_copy.wait()
    pl.semaphore_wait(barrier, STAGES - 1)

    def norm(slot, gain_ref):
        for r in range(0, B, 16):
            x = resid[slot, pl.ds(r, 16), :].astype(F32)
            inv = lax.rsqrt(jnp.mean(x * x, axis=-1, keepdims=True) + EPS)
            act[pl.ds(r, 16), :] = (x * inv * gain_ref[...]).astype(BF16)

    def rope(x, cos, sin):
        front = x[:HD // 2]
        back = x[HD // 2:]
        return front * cos - back * sin, back * cos + front * sin

    def project(i):
        for n in range(8):
            aT[pl.ds(n * 256, 256), :] = act[:, pl.ds(n * 256, 256)].T
        cos = tab[i, 0]
        sin = tab[i, 1]

        kt = dot(wqkv_v[pl.ds(2048, 512), :], aT[...])
        parts = []
        for h in range(KV):
            parts += list(rope(kt[h * HD:(h + 1) * HD], cos, sin))
        for half in range(2):
            kh = jnp.concatenate(parts[half * 8:half * 8 + 8], axis=0).astype(BF16)
            kst[pl.ds(half * 256, 256), :] = kh
            kc[pl.ds(pl.multiple_of(i * B, B), B), pl.ds(half * 256, 256)] = kh.T
        vt = dot(wqkv_v[pl.ds(2560, 512), :], aT[...])
        vT[:, pl.ds(pl.multiple_of(i * B, B), B)] = vt.astype(BF16)

        for pair in range(4):
            qt = dot(wqkv_v[pl.ds(pair * 512, 512), :], aT[...])
            for h in range(8):
                f, b = rope(qt[h * HD:(h + 1) * HD], cos, sin)
                g = pair * 2 + h // 4
                row = (g % 2) * HD
                cols = pl.ds((h % 4) * B, B)
                qT[g, pl.ds(row, HD // 2), cols] = (f * 0.125).astype(BF16)
                qT[g, pl.ds(row + HD // 2, HD // 2), cols] = (b * 0.125).astype(BF16)

    def make_mask(i):
        key = lax.broadcasted_iota(jnp.int32, (B, B), 0)
        tok = lax.broadcasted_iota(jnp.int32, (B, B), 1)
        ok = (key <= tok) & (key + i * B < valid_pos)
        mask[...] = jnp.where(ok, 0.0, NEG).astype(F32)

    def attend(n):
        spans = [(c * B, min(B, VMAX - c * B)) for c in range(n + 1)]
        total = spans[-1][0] + spans[-1][1]

        def sbuffer(u):
            return y if u % SB == 0 else sbuf.at[u % SB - 1]

        def scores(g, u):
            sref = sbuffer(u)
            kcols = pl.ds(pl.multiple_of((g // 2) * 128, 128), 128)
            q = qT[g, :, pl.ds((u % 4) * B, B)]
            m = None
            for start, rows in spans:
                s = dot(kc[pl.ds(start, rows), kcols], q)
                if start == n * B:
                    s = s + mask[pl.ds(0, rows), :]
                elif start >= VMIN:
                    mk = vbias[pl.ds(start - VMIN, rows), :]
                    s = s + jnp.concatenate([mk, mk], axis=1)
                sref[pl.ds(start, rows), :] = s
                cm = jnp.max(s.reshape(rows // 8, 8, B), axis=0)
                m = cm if m is None else jnp.maximum(m, cm)
            mbuf[u % SB] = m

        def weighted(g, u):
            sref = sbuffer(u)
            mc = jnp.max(mbuf[u % SB], axis=0, keepdims=True) * EXP_SCALE
            l = None
            probs = []
            for start, rows in spans:
                p = jnp.exp2(sref[pl.ds(start, rows), :] * EXP_SCALE - mc)
                ls = jnp.sum(p.reshape(rows // 8, 8, B), axis=0)
                l = ls if l is None else l + ls
                probs.append(p.astype(BF16))
            o = dot(vT[pl.ds(pl.multiple_of(g * HD, HD), HD), pl.ds(0, total)], jnp.concatenate(probs, axis=0))
            return (o * (1.0 / jnp.sum(l, axis=0, keepdims=True))).astype(BF16)

        for u in range(AHEAD):
            scores(0, u)

        def group_pair(pair, _):
            g = pair * 2
            g_next = lax.rem(g + 2, KV)
            outs = []
            for u in range(8):
                ahead = u + AHEAD
                scores(g + ahead // 4 if ahead < 8 else g_next, ahead)
                outs.append(weighted(g + u // 4, u))
                if u % 4 == 3:
                    act[:, pl.ds(pl.multiple_of((g + u // 4) * 256, 256), 256)] = jnp.concatenate(outs, axis=0).T
                    outs = []
            return 0

        lax.fori_loop(0, KV // 2, group_pair, 0)

    def out_proj(slot):
        for n in range(4):
            cols = pl.ds(n * 512, 512)
            o = dot(act[pl.ds(0, B), :], wo_v[:, cols])
            resid[slot, :, cols] = (resid[slot, :, cols].astype(F32) + o).astype(BF16)

    def gate_up(s):
        x = act[pl.ds(0, B), :]
        gate = dot(x, wg_s[s][...])
        up = dot(x, wu_s[s][...])
        ff_s[s % 2][...] = (gate * jax.nn.sigmoid(gate) * up).astype(BF16)

    def down(s):
        x = ff_s[s % 2][...]
        for n in range(8):
            rows = pl.ds(n * B, B)
            y[rows, :] = y[rows, :] + dot(x, wd_s[s][:, pl.ds(n * 256, 256)])

    def wait_gu(s):
        for cp in gu_copy(0, s):
            cp.wait()

    def wait_dn(s):
        dn_copy(0, s).wait()

    def start_gu(c, s, ok):
        @pl.when(ok)
        def _():
            for cp in gu_copy(lax.rem(c, NC), s):
                cp.start()

    def start_dn(c, s, ok):
        @pl.when(ok)
        def _():
            dn_copy(lax.rem(c, NC), s).start()

    def mlp(i, slot):
        for n in range(8):
            y[pl.ds(n * B, B), :] = resid[slot, :, pl.ds(n * 256, 256)].astype(F32)
        more = i + 1 < NB
        wait_gu(0)
        gate_up(0)
        start_gu(R, 0, True)

        def steps(it, _):
            c = it * R
            for u in range(R):
                if u % 2 == 0:
                    wait_gu((u + 1) % R)
                    wait_gu((u + 2) % R)
                    wait_dn(u)
                    wait_dn(u + 1)
                gate_up((u + 1) % R)
                start_gu(c + u + 1 + R, (u + 1) % R, more | (c + u + 1 + R < NC))
                down(u)
                start_dn(c + u + R, u, more | (c + u + R < NC))
            return 0

        lax.fori_loop(0, NC // R - 1, steps, 0)
        for u in range(R):
            if u % 2 == 0:
                wait_gu(u + 1)
                if u + 2 < R:
                    wait_gu(u + 2)
                wait_dn(u)
                wait_dn(u + 1)
            if u + 1 < R:
                gate_up(u + 1)
                start_gu(u + 1, u + 1, more)
            down(u)
            start_dn(u, u, more)
        for n in range(8):
            resid[slot, :, pl.ds(n * 256, 256)] = y[pl.ds(n * B, B), :].astype(BF16)

    def next_copy(i):
        slot = lax.rem(i, NS)
        return pltpu.make_async_remote_copy(resid.at[slot], resid.at[slot], send_sem.at[slot], in_sem.at[slot],
                                            device_id={"stage": lax.rem(stage + 1, STAGES)},
                                            device_id_type=pl.DeviceIdType.MESH)

    def piece_copy(i, r):
        slot = lax.rem(i, NS)
        piece = i * PER + r
        row = lax.rem(piece, 3)
        src = resid.at[slot, pl.ds(r * PIECE, PIECE), :]
        dst = hid.at[pl.ds(pl.multiple_of(row * PIECE, PIECE), PIECE), :]
        remote = pltpu.make_async_remote_copy(src, dst, piece_sem.at[slot, r], out_sem.at[row],
                                              device_id={"stage": piece // 3}, device_id_type=pl.DeviceIdType.MESH)
        return remote, pltpu.make_async_copy(src, dst, out_sem.at[row]), piece // 3 == STAGES - 1

    def k_copy(i):
        cols = pl.ds(pl.multiple_of(i * B, B), B)
        return pltpu.make_async_copy(kst, kout.at[:, cols], kv_sem.at[0])

    def v_copy(i):
        cols = pl.ds(pl.multiple_of(i * B, B), B)
        return pltpu.make_async_copy(vT.at[:, cols], vout.at[:, cols], kv_sem.at[1])

    last = stage == STAGES - 1

    def block(i, _):
        slot = lax.rem(i, NS)
        emb_copy(i).wait()

        @pl.when((stage == 0) & (i + 1 < NB))
        def _():
            emb_copy(i + 1).start()

        @pl.when(i > 0)
        def _():
            k_copy(0).wait()
            v_copy(0).wait()

        norm(slot, again)

        @pl.when(i == 0)
        def _():
            for p in range(6):
                w_copy(p).wait()

        project(i)
        make_mask(i)
        for n in range(NB):
            @pl.when(i == n)
            def _():
                attend(n)

        @pl.when(i == 0)
        def _():
            for p in range(6, 10):
                w_copy(p).wait()

        out_proj(slot)
        norm(slot, mgain)
        mlp(i, slot)

        k_copy(i).start()
        v_copy(i).start()

        @pl.when(jnp.logical_not(last) & (i >= NS))
        def _():
            pl.semaphore_wait(credit, 1)

        @pl.when(jnp.logical_not(last))
        def _():
            next_copy(i).start()

        for r in range(PER):
            remote, local, mine = piece_copy(i, r)

            @pl.when(last & jnp.logical_not(mine))
            def _():
                remote.start()

            @pl.when(last & mine)
            def _():
                local.start()

        @pl.when((i >= 1) & jnp.logical_not(last))
        def _():
            next_copy(i - 1).wait_send()

        for r in range(PER):
            remote, local, mine = piece_copy(i - 1, r)

            @pl.when((i >= 1) & last & jnp.logical_not(mine))
            def _():
                remote.wait_send()

        @pl.when((stage > 0) & (i >= 1) & (i - 1 + NS < NB))
        def _():
            pl.semaphore_signal(credit, inc=1, device_id={"stage": lax.rem(stage + STAGES - 1, STAGES)},
                                device_id_type=pl.DeviceIdType.MESH)

        return 0

    lax.fori_loop(0, NB, block, 0)

    @pl.when(jnp.logical_not(last))
    def _():
        next_copy(NB - 1).wait_send()

    for row in range(3):
        piece_copy(row // PER, row % PER)[1].wait()
    k_copy(0).wait()
    v_copy(0).wait()


def solution(mesh):
    gain_spec = P('stage', None)
    spec_three = P('stage', None, None)
    spec_four = P('stage', None, None, None)
    table = rope_tables()
    dma = pltpu.SemaphoreType.DMA

    def stage_program(embeddings, valid_len, attn_gain, w_q, w_k, w_v, w_o, mlp_gain, w_gate, w_up, w_down):
        wq = w_q[0].transpose(1, 2, 0).reshape(HEADS * HD, D)
        wk = w_k[0].transpose(1, 2, 0).reshape(KV * HD, D)
        wv = w_v[0].transpose(1, 2, 0).reshape(KV * HD, D)
        wo = w_o[0].reshape(HEADS * HD, D)
        any_spec = pl.BlockSpec(memory_space=pl.ANY)
        vmem_spec = pl.BlockSpec(memory_space=pltpu.VMEM)
        smem_spec = pl.BlockSpec(memory_space=pltpu.SMEM)
        hid, k_t, v_t = pl.pallas_call(
            stage_kernel,
            name="stage_pipeline",
            out_shape=(jax.ShapeDtypeStruct((SEQ // STAGES, D), BF16),
                       jax.ShapeDtypeStruct((KV * HD, SEQ), BF16),
                       jax.ShapeDtypeStruct((KV * HD, SEQ), BF16)),
            in_specs=[any_spec, smem_spec, vmem_spec, any_spec, any_spec, any_spec, any_spec, vmem_spec,
                      any_spec, any_spec, any_spec, any_spec],
            out_specs=(any_spec, any_spec, any_spec),
            scratch_shapes=[
                pltpu.VMEM((NB, 2, HD // 2, 256), F32),
                pltpu.VMEM((3072, D), BF16),
                pltpu.VMEM((D, D), BF16),
                [pltpu.VMEM((D, F), BF16)] * R,
                [pltpu.VMEM((D, F), BF16)] * R,
                [pltpu.VMEM((F, D), BF16)] * R,
                pltpu.VMEM((NS, B, D), BF16),
                pltpu.VMEM((SEQ, KV * HD), BF16),
                pltpu.VMEM((KV * HD, B), BF16),
                pltpu.VMEM((KV * HD, SEQ), BF16),
                pltpu.VMEM((256, D), BF16),
                pltpu.VMEM((D, 256), BF16),
                pltpu.VMEM((KV, 2 * HD, 4 * B), BF16),
                pltpu.VMEM((8 * B, 256), F32),
                pltpu.VMEM((SB - 1, VMAX, B), F32),
                pltpu.VMEM((SB, 8, B), F32),
                [pltpu.VMEM((B, F), BF16)] * 2,
                pltpu.VMEM((B, B), F32),
                pltpu.VMEM((VMAX - VMIN, 128), F32),
                dma((10,)), dma, dma((R,)), dma((R,)), dma((R,)), dma((NS,)), dma((NS,)), dma((2,)), dma((NS, PER)), dma((3,)),
                pltpu.SemaphoreType.REGULAR,
            ],
            compiler_params=pltpu.CompilerParams(collective_id=0, has_side_effects=True,
                                                 vmem_limit_bytes=67043328),
        )(embeddings, valid_len, attn_gain, wq, wk, wv, wo, mlp_gain, w_gate[0], w_up[0], w_down[0],
          jnp.asarray(table))

        def to_cache(x):
            return x.reshape(KV, HD, SEQ).transpose(2, 0, 1)[None]

        return hid, to_cache(k_t), to_cache(v_t)

    return jax.shard_map(stage_program, mesh=mesh,
                         in_specs=(P('replica', None), P('replica'), gain_spec, spec_four, spec_four, spec_four, spec_four,
                                   gain_spec, spec_three, spec_three, spec_three),
                         out_specs=(P(('replica', 'stage'), None), P('stage', 'replica', None, None), P('stage', 'replica', None, None)),
                         check_vma=False)
```

```python
import math

import jax
import jax.numpy as jnp
import numpy as np
from jax import lax
from jax.experimental import pallas as pl
from jax.experimental.pallas import tpu as pltpu
from jax.sharding import PartitionSpec as P

EPS = 1e-5
ROPE_BASE = 10000.0
NEG = -1e30

SEQ = 1536
D = 2048
HEADS = 32
KV = 8
HD = 64
FF = 8192
STAGES = 4
B = 256
NB = SEQ // B
F = 512
NC = FF // F
NS = 3
VMIN = 768
VMAX = 1344
PIECE = SEQ // STAGES // 3
PER = B // PIECE
R = 4
SB = 4
AHEAD = 2
EXP_SCALE = math.log2(math.e)

F32 = jnp.float32
BF16 = jnp.bfloat16


def rope_tables():
    inv_freq = ROPE_BASE ** (-np.arange(HD // 2, dtype=np.float64) * (2.0 / HD))
    angles = inv_freq[:, None] * np.arange(SEQ, dtype=np.float64)[None, :]
    tab = np.zeros((NB, 2, HD // 2, 256), np.float32)
    for blk in range(NB):
        cols = slice(blk * B, (blk + 1) * B)
        tab[blk, 0, :, :B] = np.cos(angles[:, cols])
        tab[blk, 1, :, :B] = np.sin(angles[:, cols])
    return tab


def dot(a, b):
    return jnp.dot(a, b, preferred_element_type=F32)


def dot_t(a, b):
    return lax.dot_general(a, b, (((1,), (1,)), ((), ())), preferred_element_type=F32)


def stage_kernel(emb, valid, again, wq, wk, wv, wo, mgain, wg, wu, wd, tab_hbm,
                 hid, kout, vout,
                 tab, wqkv_v, wo_v, wg_s, wu_s, wd_s, resid, kc, vT, act, qT, y, mbuf, ff_s,
                 mask, vbias,
                 w_sem, tab_sem, g_sem, u_sem, d_sem, in_sem, send_sem, kv_sem, piece_sem, out_sem, credit):
    stage = lax.axis_index("stage")
    barrier = pltpu.get_barrier_semaphore()
    for k in range(1, STAGES):
        pl.semaphore_signal(barrier, inc=1, device_id={"stage": lax.rem(stage + k, STAGES)},
                            device_id_type=pl.DeviceIdType.MESH)

    def emb_copy(i):
        return pltpu.make_async_copy(emb.at[pl.ds(pl.multiple_of(i * B, B), B), :], resid.at[lax.rem(i, NS)], in_sem.at[lax.rem(i, NS)])

    def w_copy(p):
        if p < 4:
            src = wq.at[pl.ds(p * 512, 512), :]
        elif p == 4:
            src = wk
        elif p == 5:
            src = wv
        else:
            src = wo.at[pl.ds((p - 6) * 512, 512), :]
        dst = wqkv_v.at[pl.ds(p * 512, 512), :] if p < 6 else wo_v.at[pl.ds((p - 6) * 512, 512), :]
        return pltpu.make_async_copy(src, dst, w_sem.at[p])

    def gu_copy(c, s):
        cols = pl.ds(pl.multiple_of(c * F, F), F)
        return (pltpu.make_async_copy(wg.at[:, cols], wg_s[s], g_sem.at[s]),
                pltpu.make_async_copy(wu.at[:, cols], wu_s[s], u_sem.at[s]))

    def dn_copy(c, s):
        rows = pl.ds(pl.multiple_of(c * F, F), F)
        return pltpu.make_async_copy(wd.at[rows, :], wd_s[s], d_sem.at[s])

    tab_copy = pltpu.make_async_copy(tab_hbm, tab, tab_sem)

    @pl.when(stage == 0)
    def _():
        emb_copy(0).start()

    w_copy(4).start()
    tab_copy.start()
    for p in (5, 0, 1, 2, 3, 6, 7, 8, 9):
        w_copy(p).start()
    for c in range(R):
        for cp in gu_copy(c, c):
            cp.start()
        dn_copy(c, c).start()

    for g in range(KV):
        qT[g, pl.ds((1 - g % 2) * HD, HD), :] = jnp.zeros((HD, 4 * B), BF16)
    valid_pos = valid[0]
    vrow = lax.broadcasted_iota(jnp.int32, vbias.shape, 0) + VMIN
    vbias[...] = jnp.where(vrow < valid_pos, 0.0, NEG).astype(F32)

    def norm(slot, gain_ref):
        for r in range(0, B, 16):
            x = resid[slot, pl.ds(r, 16), :].astype(F32)
            inv = lax.rsqrt(jnp.mean(x * x, axis=-1, keepdims=True) + EPS)
            act[pl.ds(r, 16), :] = (x * inv * gain_ref[...]).astype(BF16)

    def rope(x, cos, sin):
        front = x[:HD // 2]
        back = x[HD // 2:]
        return front * cos - back * sin, back * cos + front * sin

    def project(i):
        cos = tab[i, 0]
        sin = tab[i, 1]

        kt = dot_t(wqkv_v[pl.ds(2048, 512), :], act[...])
        parts = []
        for h in range(KV):
            parts += list(rope(kt[h * HD:(h + 1) * HD], cos, sin))
        for half in range(2):
            kh = jnp.concatenate(parts[half * 8:half * 8 + 8], axis=0).astype(BF16)
            ff_s[1][:, pl.ds(half * 256, 256)] = kh
            kc[pl.ds(pl.multiple_of(i * B, B), B), pl.ds(half * 256, 256)] = kh.T
        vt = dot_t(wqkv_v[pl.ds(2560, 512), :], act[...])
        vT[:, pl.ds(pl.multiple_of(i * B, B), B)] = vt.astype(BF16)

        for pair in range(4):
            qt = dot_t(wqkv_v[pl.ds(pair * 512, 512), :], act[...])
            for h in range(8):
                f, b = rope(qt[h * HD:(h + 1) * HD], cos, sin)
                g = pair * 2 + h // 4
                row = (g % 2) * HD
                cols = pl.ds((h % 4) * B, B)
                qT[g, pl.ds(row, HD // 2), cols] = (f * 0.125).astype(BF16)
                qT[g, pl.ds(row + HD // 2, HD // 2), cols] = (b * 0.125).astype(BF16)

    def make_mask(i):
        key = lax.broadcasted_iota(jnp.int32, (B, B), 0)
        tok = lax.broadcasted_iota(jnp.int32, (B, B), 1)
        ok = (key <= tok) & (key + i * B < valid_pos)
        mask[...] = jnp.where(ok, 0.0, NEG).astype(F32)

    def attend(n):
        spans = [(c * B, min(B, VMAX - c * B)) for c in range(n + 1)]
        total = spans[-1][0] + spans[-1][1]

        def scores(g, u):
            kcols = pl.ds(pl.multiple_of((g // 2) * 128, 128), 128)
            q = qT[g, :, pl.ds((u % 4) * B, B)]
            m = None
            for start, rows in spans:
                s = dot(kc[pl.ds(start, rows), kcols], q)
                if start == n * B:
                    s = s + mask[pl.ds(0, rows), :]
                elif start >= VMIN:
                    mk = vbias[pl.ds(start - VMIN, rows), :]
                    s = s + jnp.concatenate([mk, mk], axis=1)
                y[pl.ds((u % SB) * total + start, rows), :] = s
                cm = jnp.max(s.reshape(rows // 8, 8, B), axis=0)
                m = cm if m is None else jnp.maximum(m, cm)
            mbuf[u % SB] = m

        def weighted(g, u):
            mc = jnp.max(mbuf[u % SB], axis=0, keepdims=True) * EXP_SCALE
            l = None
            probs = []
            for start, rows in spans:
                p = jnp.exp2(y[pl.ds((u % SB) * total + start, rows), :] * EXP_SCALE - mc)
                ls = jnp.sum(p.reshape(rows // 8, 8, B), axis=0)
                l = ls if l is None else l + ls
                probs.append(p.astype(BF16))
            o = dot(vT[pl.ds(pl.multiple_of(g * HD, HD), HD), pl.ds(0, total)], jnp.concatenate(probs, axis=0))
            return (o * (1.0 / jnp.sum(l, axis=0, keepdims=True))).astype(BF16)

        for u in range(AHEAD):
            scores(0, u)

        def group_pair(pair, _):
            g = pair * 2
            outs = []
            for u in range(8):
                ahead = u + AHEAD
                scores(g + ahead // 4 if ahead < 8 else lax.rem(g + 2, KV), ahead)
                outs.append(weighted(g + u // 4, u))
                if u % 4 == 3:
                    act[:, pl.ds(pl.multiple_of((g + u // 4) * 256, 256), 256)] = jnp.concatenate(outs, axis=0).T
                    outs = []
            return 0

        lax.fori_loop(0, KV // 2, group_pair, 0)

    def out_proj(slot):
        for n in range(4):
            cols = pl.ds(n * 512, 512)
            o = dot(act[pl.ds(0, B), :], wo_v[:, cols])
            resid[slot, :, cols] = (resid[slot, :, cols].astype(F32) + o).astype(BF16)

    def gate_up(s):
        x = act[pl.ds(0, B), :]
        gate = dot(x, wg_s[s][...])
        up = dot(x, wu_s[s][...])
        ff_s[s % 2][...] = (gate * jax.nn.sigmoid(gate) * up).astype(BF16)

    def down(s):
        x = ff_s[s % 2][...]
        for n in range(8):
            rows = pl.ds(n * B, B)
            y[rows, :] = y[rows, :] + dot(x, wd_s[s][:, pl.ds(n * 256, 256)])

    def wait_gu(s):
        for cp in gu_copy(0, s):
            cp.wait()

    def wait_dn(s):
        dn_copy(0, s).wait()

    def start_gu(c, s, ok):
        @pl.when(ok)
        def _():
            for cp in gu_copy(lax.rem(c, NC), s):
                cp.start()

    def start_dn(c, s, ok):
        @pl.when(ok)
        def _():
            dn_copy(lax.rem(c, NC), s).start()

    def mlp(i, slot):
        for n in range(8):
            y[pl.ds(n * B, B), :] = resid[slot, :, pl.ds(n * 256, 256)].astype(F32)
        more = i + 1 < NB

        def steps(it, _):
            again_ok = more | (it < NC // R - 1)
            c = (it + 1) * R
            wait_gu(0)
            wait_gu(1)
            wait_dn(0)
            gate_up(0)
            start_gu(c, 0, again_ok)
            gate_up(1)
            start_gu(c + 1, 1, again_ok)
            down(0)
            start_dn(c, 0, again_ok)
            wait_gu(2)
            wait_dn(1)
            gate_up(2)
            start_gu(c + 2, 2, again_ok)
            down(1)
            start_dn(c + 1, 1, again_ok)
            wait_gu(3)
            wait_dn(2)
            wait_dn(3)
            gate_up(3)
            start_gu(c + 3, 3, again_ok)
            down(2)
            start_dn(c + 2, 2, again_ok)
            down(3)
            start_dn(c + 3, 3, again_ok)
            return 0

        lax.fori_loop(0, NC // R, steps, 0)
        for n in range(8):
            resid[slot, :, pl.ds(n * 256, 256)] = y[pl.ds(n * B, B), :].astype(BF16)

    def next_copy(i):
        slot = lax.rem(i, NS)
        return pltpu.make_async_remote_copy(resid.at[slot], resid.at[slot], send_sem.at[slot], in_sem.at[slot],
                                            device_id={"stage": lax.rem(stage + 1, STAGES)},
                                            device_id_type=pl.DeviceIdType.MESH)

    def piece_copy(i, r):
        slot = lax.rem(i, NS)
        piece = i * PER + r
        row = lax.rem(piece, 3)
        src = resid.at[slot, pl.ds(r * PIECE, PIECE), :]
        dst = hid.at[pl.ds(pl.multiple_of(row * PIECE, PIECE), PIECE), :]
        remote = pltpu.make_async_remote_copy(src, dst, piece_sem.at[slot, r], out_sem.at[row],
                                              device_id={"stage": piece // 3}, device_id_type=pl.DeviceIdType.MESH)
        return remote, pltpu.make_async_copy(src, dst, out_sem.at[row]), piece // 3 == STAGES - 1

    def k_copy(i, half):
        cols = pl.ds(pl.multiple_of(i * B, B), B)
        return pltpu.make_async_copy(ff_s[1].at[:, pl.ds(half * 256, 256)], kout.at[pl.ds(half * 256, 256), cols],
                                     kv_sem.at[half])

    def v_copy(i):
        cols = pl.ds(pl.multiple_of(i * B, B), B)
        return pltpu.make_async_copy(vT.at[:, cols], vout.at[:, cols], kv_sem.at[2])

    last = stage == STAGES - 1

    def block(i, _):
        slot = lax.rem(i, NS)
        emb_copy(i).wait()

        norm(slot, again)

        @pl.when(i == 0)
        def _():
            tab_copy.wait()
            for p in range(6):
                w_copy(p).wait()

        project(i)
        make_mask(i)
        k_copy(i, 0).start()
        k_copy(i, 1).start()
        v_copy(i).start()
        for n in range(NB):
            @pl.when(i == n)
            def _():
                attend(n)

        @pl.when(i == 0)
        def _():
            pl.semaphore_wait(barrier, STAGES - 1)

        @pl.when((i >= 1) & jnp.logical_not(last))
        def _():
            next_copy(i - 1).wait_send()

        for r in range(PER):
            remote, local, mine = piece_copy(i - 1, r)

            @pl.when((i >= 1) & last & jnp.logical_not(mine))
            def _():
                remote.wait_send()

        @pl.when((stage > 0) & (i >= 1) & (i - 1 + NS < NB))
        def _():
            pl.semaphore_signal(credit, inc=1, device_id={"stage": lax.rem(stage + STAGES - 1, STAGES)},
                                device_id_type=pl.DeviceIdType.MESH)

        @pl.when((stage == 0) & (i + 1 < NB))
        def _():
            emb_copy(i + 1).start()


        @pl.when(i == 0)
        def _():
            for p in range(6, 10):
                w_copy(p).wait()

        k_copy(i, 0).wait()
        k_copy(i, 1).wait()
        v_copy(i).wait()
        out_proj(slot)
        norm(slot, mgain)
        mlp(i, slot)


        @pl.when(jnp.logical_not(last) & (i >= NS))
        def _():
            pl.semaphore_wait(credit, 1)

        @pl.when(jnp.logical_not(last))
        def _():
            next_copy(i).start()

        for r in range(PER):
            remote, local, mine = piece_copy(i, r)

            @pl.when(last & jnp.logical_not(mine))
            def _():
                remote.start()

            @pl.when(last & mine)
            def _():
                local.start()

        return 0

    lax.fori_loop(0, NB, block, 0)

    @pl.when(jnp.logical_not(last))
    def _():
        next_copy(NB - 1).wait_send()

    for row in range(3):
        piece_copy(row // PER, row % PER)[1].wait()

def solution(mesh):
    gain_spec = P('stage', None)
    spec_three = P('stage', None, None)
    spec_four = P('stage', None, None, None)
    table = rope_tables()
    dma = pltpu.SemaphoreType.DMA

    def stage_program(embeddings, valid_len, attn_gain, w_q, w_k, w_v, w_o, mlp_gain, w_gate, w_up, w_down):
        wq = w_q[0].transpose(1, 2, 0).reshape(HEADS * HD, D)
        wk = w_k[0].transpose(1, 2, 0).reshape(KV * HD, D)
        wv = w_v[0].transpose(1, 2, 0).reshape(KV * HD, D)
        wo = w_o[0].reshape(HEADS * HD, D)
        any_spec = pl.BlockSpec(memory_space=pl.ANY)
        vmem_spec = pl.BlockSpec(memory_space=pltpu.VMEM)
        smem_spec = pl.BlockSpec(memory_space=pltpu.SMEM)
        hid, k_t, v_t = pl.pallas_call(
            stage_kernel,
            name="stage_pipeline",
            out_shape=(jax.ShapeDtypeStruct((SEQ // STAGES, D), BF16),
                       jax.ShapeDtypeStruct((KV * HD, SEQ), BF16),
                       jax.ShapeDtypeStruct((KV * HD, SEQ), BF16)),
            in_specs=[any_spec, smem_spec, vmem_spec, any_spec, any_spec, any_spec, any_spec, vmem_spec,
                      any_spec, any_spec, any_spec, any_spec],
            out_specs=(any_spec, any_spec, any_spec),
            scratch_shapes=[
                pltpu.VMEM((NB, 2, HD // 2, 256), F32),
                pltpu.VMEM((3072, D), BF16),
                pltpu.VMEM((D, D), BF16),
                [pltpu.VMEM((D, F), BF16)] * R,
                [pltpu.VMEM((D, F), BF16)] * R,
                [pltpu.VMEM((F, D), BF16)] * R,
                pltpu.VMEM((NS, B, D), BF16),
                pltpu.VMEM((SEQ, KV * HD), BF16),
                pltpu.VMEM((KV * HD, SEQ), BF16),
                pltpu.VMEM((256, D), BF16),
                pltpu.VMEM((KV, 2 * HD, 4 * B), BF16),
                pltpu.VMEM((SB * VMAX, B), F32),
                pltpu.VMEM((SB, 8, B), F32),
                [pltpu.VMEM((B, F), BF16)] * 2,
                pltpu.VMEM((B, B), F32),
                pltpu.VMEM((VMAX - VMIN, 128), F32),
                dma((10,)), dma, dma((R,)), dma((R,)), dma((R,)), dma((NS,)), dma((NS,)), dma((3,)), dma((NS, PER)), dma((3,)),
                pltpu.SemaphoreType.REGULAR,
            ],
            compiler_params=pltpu.CompilerParams(collective_id=0, has_side_effects=True,
                                                 vmem_limit_bytes=67043328),
        )(embeddings, valid_len, attn_gain, wq, wk, wv, wo, mlp_gain, w_gate[0], w_up[0], w_down[0],
          jnp.asarray(table))

        def to_cache(x):
            return x.reshape(KV, HD, SEQ).transpose(2, 0, 1)[None]

        return hid, to_cache(k_t), to_cache(v_t)

    return jax.shard_map(stage_program, mesh=mesh,
                         in_specs=(P('replica', None), P('replica'), gain_spec, spec_four, spec_four, spec_four, spec_four,
                                   gain_spec, spec_three, spec_three, spec_three),
                         out_specs=(P(('replica', 'stage'), None), P('stage', 'replica', None, None), P('stage', 'replica', None, None)),
                         check_vma=False)
```

```python
import math

import jax
import jax.numpy as jnp
import numpy as np
from jax import lax
from jax.experimental import pallas as pl
from jax.experimental.pallas import tpu as pltpu
from jax.sharding import PartitionSpec as P

EPS = 1e-5
ROPE_BASE = 10000.0
NEG = -1e30

SEQ = 1536
D = 2048
HEADS = 32
KV = 8
HD = 64
FF = 8192
STAGES = 4
B = 256
NB = SEQ // B
F = 512
NC = FF // F
NS = 3
VMIN = 768
VMAX = 1344
PIECE = SEQ // STAGES // 3
PER = B // PIECE
R = 4
SB = 4
EXP_SCALE = math.log2(math.e)

F32 = jnp.float32
BF16 = jnp.bfloat16


def rope_tables():
    inv_freq = ROPE_BASE ** (-np.arange(HD // 2, dtype=np.float64) * (2.0 / HD))
    angles = inv_freq[:, None] * np.arange(SEQ, dtype=np.float64)[None, :]
    tab = np.zeros((NB, 2, HD // 2, 256), np.float32)
    for blk in range(NB):
        cols = slice(blk * B, (blk + 1) * B)
        tab[blk, 0, :, :B] = np.cos(angles[:, cols])
        tab[blk, 1, :, :B] = np.sin(angles[:, cols])
    return tab


def dot(a, b):
    return jnp.dot(a, b, preferred_element_type=F32)


def dot_t(a, b):
    return lax.dot_general(a, b, (((1,), (1,)), ((), ())), preferred_element_type=F32)


def stage_kernel(emb, valid, again_hbm, wq, wk, wv, wo, mgain_hbm, wg, wu, wd, tab_hbm,
                 hid, kout, vout,
                 tab, again, mgain, wqkv_v, wo_v, wg_s, wu_s, wd_s, resid, kc, vT, act, qT, y, mbuf, ff_s,
                 mask, vbias, kbias, qones,
                 w_sem, tab_sem, g_sem, u_sem, d_sem, in_sem, send_sem, kv_sem, piece_sem, out_sem, credit):
    stage = lax.axis_index("stage")
    barrier = pltpu.get_barrier_semaphore()
    for k in range(1, STAGES):
        pl.semaphore_signal(barrier, inc=1, device_id={"stage": lax.rem(stage + k, STAGES)},
                            device_id_type=pl.DeviceIdType.MESH)

    def emb_copy(i):
        return pltpu.make_async_copy(emb.at[pl.ds(pl.multiple_of(i * B, B), B), :], resid.at[lax.rem(i, NS)], in_sem.at[lax.rem(i, NS)])

    def w_copy(p):
        if p < 4:
            src = wq.at[pl.ds(p * 512, 512), :]
        elif p == 4:
            src = wk
        elif p == 5:
            src = wv
        else:
            src = wo.at[pl.ds((p - 6) * 512, 512), :]
        dst = wqkv_v.at[pl.ds(p * 512, 512), :] if p < 6 else wo_v.at[pl.ds((p - 6) * 512, 512), :]
        return pltpu.make_async_copy(src, dst, w_sem.at[p])

    def gu_copy(c, s):
        cols = pl.ds(pl.multiple_of(c * F, F), F)
        return (pltpu.make_async_copy(wg.at[:, cols], wg_s[s], g_sem.at[s]),
                pltpu.make_async_copy(wu.at[:, cols], wu_s[s], u_sem.at[s]))

    def dn_copy(c, s):
        rows = pl.ds(pl.multiple_of(c * F, F), F)
        return pltpu.make_async_copy(wd.at[rows, :], wd_s[s], d_sem.at[s])

    small_copies = [pltpu.make_async_copy(src, dst, tab_sem.at[n])
                    for n, (src, dst) in enumerate(((again_hbm, again), (mgain_hbm, mgain), (tab_hbm, tab)))]

    @pl.when(stage == 0)
    def _():
        emb_copy(0).start()

    for cp in small_copies:
        cp.start()
    for p in range(6):
        w_copy(p).start()

    for g in range(KV):
        qT[g, pl.ds((1 - g % 2) * HD, HD), :] = jnp.zeros((HD, 4 * B), BF16)
    valid_pos = valid[0]
    row = lax.broadcasted_iota(jnp.int32, vbias.shape, 0) + VMIN
    vbias[...] = jnp.where(row < valid_pos, 0.0, NEG).astype(F32)
    row = lax.broadcasted_iota(jnp.int32, kbias.shape, 0) + VMIN
    lane = lax.broadcasted_iota(jnp.int32, kbias.shape, 1)
    kbias[...] = jnp.where((lane == 0) & (row >= valid_pos), NEG, 0.0).astype(BF16)
    row = lax.broadcasted_iota(jnp.int32, qones.shape, 0)
    qones[...] = jnp.where(row == 0, 1.0, 0.0).astype(BF16)

    def norm(slot, gain_ref):
        for r in range(0, B, 16):
            x = resid[slot, pl.ds(r, 16), :].astype(F32)
            inv = lax.rsqrt(jnp.mean(x * x, axis=-1, keepdims=True) + EPS)
            act[pl.ds(r, 16), :] = (x * inv * gain_ref[...]).astype(BF16)

    def rope(x, cos, sin):
        front = x[:HD // 2]
        back = x[HD // 2:]
        return front * cos - back * sin, back * cos + front * sin

    def project(i):
        cos = tab[i, 0]
        sin = tab[i, 1]

        kt = dot_t(wqkv_v[pl.ds(2048, 512), :], act[...])
        parts = []
        for h in range(KV):
            parts += list(rope(kt[h * HD:(h + 1) * HD], cos, sin))
        for half in range(2):
            kh = jnp.concatenate(parts[half * 8:half * 8 + 8], axis=0).astype(BF16)
            ff_s[1][:, pl.ds(half * 256, 256)] = kh
            kc[pl.ds(pl.multiple_of(i * B, B), B), pl.ds(half * 256, 256)] = kh.T
        vt = dot_t(wqkv_v[pl.ds(2560, 512), :], act[...])
        vT[:, pl.ds(pl.multiple_of(i * B, B), B)] = vt.astype(BF16)

        for pair in range(4):
            qt = dot_t(wqkv_v[pl.ds(pair * 512, 512), :], act[...])
            for h in range(8):
                f, b = rope(qt[h * HD:(h + 1) * HD], cos, sin)
                g = pair * 2 + h // 4
                row = (g % 2) * HD
                cols = pl.ds((h % 4) * B, B)
                qT[g, pl.ds(row, HD // 2), cols] = (f * 0.125).astype(BF16)
                qT[g, pl.ds(row + HD // 2, HD // 2), cols] = (b * 0.125).astype(BF16)

    def make_mask(i):
        key = lax.broadcasted_iota(jnp.int32, mask.shape, 0)
        tok = lax.broadcasted_iota(jnp.int32, mask.shape, 1)
        key = jnp.where(tok < B, key, key + B // 2)
        tok = jnp.where(tok < B, tok, tok - B // 2)
        ok = (key <= tok) & (key + i * B < valid_pos)
        mask[...] = jnp.where(ok, 0.0, NEG).astype(F32)

    def attend(n):
        spans = [(c * B, min(B, VMAX - c * B), 0) for c in range(n + 1)]
        if spans[-1][1] == B:
            spans[-1:] = [(n * B, B // 2, 0), (n * B + B // 2, B // 2, B // 2)]
        total = spans[-1][0] + spans[-1][1]
        ahead_by = 1 if n == NB - 2 else 2

        def scores(g, u):
            kcols = pl.ds(pl.multiple_of((g // 2) * 128, 128), 128)
            q = qT[g, :, pl.ds((u % 4) * B, B)]
            m = None
            for start, rows, lane in spans:
                keys = kc[pl.ds(start, rows), kcols]
                if start >= n * B:
                    s = dot(keys, q[:, lane:]) + mask[pl.ds(0, rows), pl.ds(2 * lane, B - lane)]
                elif start >= VMIN and n == NB - 1:
                    bias = vbias[pl.ds(start - VMIN, rows), :]
                    s = dot(keys, q) + jnp.concatenate([bias, bias], axis=1)
                elif start >= VMIN:
                    bias = kbias[pl.ds(start - VMIN, rows), :]
                    s = dot(jnp.concatenate([keys, bias], axis=1), jnp.concatenate([q, qones[...]], axis=0))
                else:
                    s = dot(keys, q)
                y[pl.ds((u % SB) * total + start, rows), pl.ds(lane, B - lane)] = s
                cm = jnp.max(s.reshape(rows // 8, 8, B - lane), axis=0)
                if lane:
                    m = jnp.concatenate([m[:, :lane], jnp.maximum(m[:, lane:], cm)], axis=1)
                else:
                    m = cm if m is None else jnp.maximum(m, cm)
            mbuf[u % SB] = m

        def weighted(g, u):
            mc = jnp.max(mbuf[u % SB], axis=0, keepdims=True) * EXP_SCALE
            l = None
            probs = []
            for start, rows, lane in spans:
                sc = y[pl.ds((u % SB) * total + start, rows), pl.ds(lane, B - lane)]
                p = jnp.exp2(sc * EXP_SCALE - mc[:, lane:])
                ls = jnp.sum(p.reshape(rows // 8, 8, B - lane), axis=0)
                p = p.astype(BF16)
                if lane:
                    l = jnp.concatenate([l[:, :lane], l[:, lane:] + ls], axis=1)
                    p = jnp.concatenate([jnp.zeros((rows, lane), BF16), p], axis=1)
                else:
                    l = ls if l is None else l + ls
                probs.append(p)
            o = dot(vT[pl.ds(pl.multiple_of(g * HD, HD), HD), pl.ds(0, total)], jnp.concatenate(probs, axis=0))
            return (o * (1.0 / jnp.sum(l, axis=0, keepdims=True))).astype(BF16)

        for u in range(ahead_by):
            scores(0, u)

        def group_pair(pair, _):
            g = pair * 2
            outs = []
            for u in range(8):
                ahead = u + ahead_by
                scores(g + ahead // 4 if ahead < 8 else lax.rem(g + 2, KV), ahead)
                outs.append(weighted(g + u // 4, u))
                if u % 4 == 3:
                    act[:, pl.ds(pl.multiple_of((g + u // 4) * 256, 256), 256)] = jnp.concatenate(outs, axis=0).T
                    outs = []
            return 0

        lax.fori_loop(0, KV // 2, group_pair, 0)

    def out_proj(slot):
        for n in range(4):
            cols = pl.ds(n * 512, 512)
            o = dot(act[pl.ds(0, B), :], wo_v[:, cols])
            resid[slot, :, cols] = (resid[slot, :, cols].astype(F32) + o).astype(BF16)

    def gate_up(s):
        x = act[pl.ds(0, B), :]
        gate = dot(x, wg_s[s][...])
        up = dot(x, wu_s[s][...])
        ff_s[s % 2][...] = (gate * jax.nn.sigmoid(gate) * up).astype(BF16)

    def down(s):
        x = ff_s[s % 2][...]
        for n in range(8):
            rows = pl.ds(n * B, B)
            y[rows, :] = y[rows, :] + dot(x, wd_s[s][:, pl.ds(n * 256, 256)])

    def wait_gu(s):
        for cp in gu_copy(0, s):
            cp.wait()

    def wait_dn(s):
        dn_copy(0, s).wait()

    def start_gu(c, s, ok):
        @pl.when(ok)
        def _():
            for cp in gu_copy(lax.rem(c, NC), s):
                cp.start()

    def start_dn(c, s, ok):
        @pl.when(ok)
        def _():
            dn_copy(lax.rem(c, NC), s).start()

    def mlp(i, slot):
        for n in range(8):
            y[pl.ds(n * B, B), :] = resid[slot, :, pl.ds(n * 256, 256)].astype(F32)
        more = i + 1 < NB
        wait_gu(0)
        gate_up(0)
        start_gu(R, 0, True)

        def steps(it, _):
            c = it * R
            for u in range(R):
                if u % 2 == 0:
                    wait_gu((u + 1) % R)
                    wait_gu((u + 2) % R)
                    wait_dn(u)
                    wait_dn(u + 1)
                gate_up((u + 1) % R)
                start_gu(c + u + 1 + R, (u + 1) % R, more | (c + u + 1 + R < NC))
                down(u)
                start_dn(c + u + R, u, more | (c + u + R < NC))
            return 0

        lax.fori_loop(0, NC // R - 1, steps, 0)
        for u in range(R):
            if u % 2 == 0:
                wait_gu(u + 1)
                if u + 2 < R:
                    wait_gu(u + 2)
                wait_dn(u)
                wait_dn(u + 1)
            if u + 1 < R:
                gate_up(u + 1)
                start_gu(u + 1, u + 1, more)
            down(u)
            start_dn(u, u, more)
        for n in range(8):
            resid[slot, :, pl.ds(n * 256, 256)] = y[pl.ds(n * B, B), :].astype(BF16)

    def next_copy(i):
        slot = lax.rem(i, NS)
        return pltpu.make_async_remote_copy(resid.at[slot], resid.at[slot], send_sem.at[slot], in_sem.at[slot],
                                            device_id={"stage": lax.rem(stage + 1, STAGES)},
                                            device_id_type=pl.DeviceIdType.MESH)

    def piece_copy(i, r):
        slot = lax.rem(i, NS)
        piece = i * PER + r
        row = lax.rem(piece, 3)
        src = resid.at[slot, pl.ds(r * PIECE, PIECE), :]
        dst = hid.at[pl.ds(pl.multiple_of(row * PIECE, PIECE), PIECE), :]
        remote = pltpu.make_async_remote_copy(src, dst, piece_sem.at[slot, r], out_sem.at[row],
                                              device_id={"stage": piece // 3}, device_id_type=pl.DeviceIdType.MESH)
        return remote, pltpu.make_async_copy(src, dst, out_sem.at[row]), piece // 3 == STAGES - 1

    def k_copy(i, half):
        cols = pl.ds(pl.multiple_of(i * B, B), B)
        return pltpu.make_async_copy(ff_s[1].at[:, pl.ds(half * 256, 256)], kout.at[pl.ds(half * 256, 256), cols],
                                     kv_sem.at[half])

    def v_copy(i):
        cols = pl.ds(pl.multiple_of(i * B, B), B)
        return pltpu.make_async_copy(vT.at[:, cols], vout.at[:, cols], kv_sem.at[2])

    last = stage == STAGES - 1

    def block(i, _):
        slot = lax.rem(i, NS)
        emb_copy(i).wait()

        @pl.when(i == 0)
        def _():
            for cp in small_copies:
                cp.wait()

        norm(slot, again)

        @pl.when(i == 0)
        def _():
            for p in range(6):
                w_copy(p).wait()
            for p in range(6, 10):
                w_copy(p).start()
            for c in range(2):
                start_gu(c, c, True)
                start_dn(c, c, True)

        project(i)

        @pl.when(i == 0)
        def _():
            for c in range(2, R):
                start_gu(c, c, True)
                start_dn(c, c, True)

        make_mask(i)
        k_copy(i, 0).start()
        k_copy(i, 1).start()
        v_copy(i).start()
        for n in range(NB):
            @pl.when(i == n)
            def _():
                attend(n)

        @pl.when(i == 0)
        def _():
            pl.semaphore_wait(barrier, STAGES - 1)

        @pl.when((i >= 1) & jnp.logical_not(last))
        def _():
            next_copy(i - 1).wait_send()

        for r in range(PER):
            remote, local, mine = piece_copy(i - 1, r)

            @pl.when((i >= 1) & last & jnp.logical_not(mine))
            def _():
                remote.wait_send()

        @pl.when((stage > 0) & (i >= 1) & (i - 1 + NS < NB))
        def _():
            pl.semaphore_signal(credit, inc=1, device_id={"stage": lax.rem(stage + STAGES - 1, STAGES)},
                                device_id_type=pl.DeviceIdType.MESH)

        @pl.when((stage == 0) & (i + 1 < NB))
        def _():
            emb_copy(i + 1).start()


        @pl.when(i == 0)
        def _():
            for p in range(6, 10):
                w_copy(p).wait()

        k_copy(i, 0).wait()
        k_copy(i, 1).wait()
        v_copy(i).wait()
        out_proj(slot)
        norm(slot, mgain)
        mlp(i, slot)


        @pl.when(jnp.logical_not(last) & (i >= NS))
        def _():
            pl.semaphore_wait(credit, 1)

        @pl.when(jnp.logical_not(last))
        def _():
            next_copy(i).start()

        for r in range(PER):
            remote, local, mine = piece_copy(i, r)

            @pl.when(last & jnp.logical_not(mine))
            def _():
                remote.start()

            @pl.when(last & mine)
            def _():
                local.start()

        return 0

    lax.fori_loop(0, NB, block, 0)

    @pl.when(jnp.logical_not(last))
    def _():
        next_copy(NB - 1).wait_send()

    for row in range(3):
        piece_copy(row // PER, row % PER)[1].wait()

def place_kernel(hid, k_t, v_t, hid_out, k_out, v_out, hid_v, k_v, v_v, in_sem, out_sem):
    halves = []
    for n, (src, buf, dst) in enumerate(((hid, hid_v, hid_out), (k_t, k_v, k_out), (v_t, v_v, v_out))):
        rows = src.shape[0] // 2
        for half in range(2):
            part = pl.ds(half * rows, rows)
            halves.append((pltpu.make_async_copy(src.at[part], buf.at[part], in_sem.at[n, half]),
                           pltpu.make_async_copy(buf.at[part], dst.at[part], out_sem.at[n, half])))
    for load, _ in halves:
        load.start()
    for load, store in halves:
        load.wait()
        store.start()
    for _, store in halves:
        store.wait()


def solution(mesh):
    gain_spec = P('stage', None)
    spec_three = P('stage', None, None)
    spec_four = P('stage', None, None, None)
    table = rope_tables()
    dma = pltpu.SemaphoreType.DMA

    def stage_program(embeddings, valid_len, attn_gain, w_q, w_k, w_v, w_o, mlp_gain, w_gate, w_up, w_down):
        wq = w_q[0].transpose(1, 2, 0).reshape(HEADS * HD, D)
        wk = w_k[0].transpose(1, 2, 0).reshape(KV * HD, D)
        wv = w_v[0].transpose(1, 2, 0).reshape(KV * HD, D)
        wo = w_o[0].reshape(HEADS * HD, D)
        any_spec = pl.BlockSpec(memory_space=pl.ANY)
        vmem_spec = pl.BlockSpec(memory_space=pltpu.VMEM)
        smem_spec = pl.BlockSpec(memory_space=pltpu.SMEM)
        hid, k_t, v_t = pl.pallas_call(
            stage_kernel,
            name="stage_pipeline",
            out_shape=(jax.ShapeDtypeStruct((SEQ // STAGES, D), BF16),
                       jax.ShapeDtypeStruct((KV * HD, SEQ), BF16),
                       jax.ShapeDtypeStruct((KV * HD, SEQ), BF16)),
            in_specs=[any_spec, smem_spec, any_spec, any_spec, any_spec, any_spec, any_spec, any_spec,
                      any_spec, any_spec, any_spec, any_spec],
            out_specs=(any_spec, any_spec, any_spec),
            scratch_shapes=[
                pltpu.VMEM((NB, 2, HD // 2, 256), F32),
                pltpu.VMEM((1, D), F32),
                pltpu.VMEM((1, D), F32),
                pltpu.VMEM((3072, D), BF16),
                pltpu.VMEM((D, D), BF16),
                [pltpu.VMEM((D, F), BF16)] * R,
                [pltpu.VMEM((D, F), BF16)] * R,
                [pltpu.VMEM((F, D), BF16)] * R,
                pltpu.VMEM((NS, B, D), BF16),
                pltpu.VMEM((SEQ, KV * HD), BF16),
                pltpu.VMEM((KV * HD, SEQ), BF16),
                pltpu.VMEM((256, D), BF16),
                pltpu.VMEM((KV, 2 * HD, 4 * B), BF16),
                pltpu.VMEM((SB * VMAX, B), F32),
                pltpu.VMEM((SB, 8, B), F32),
                [pltpu.VMEM((B, F), BF16)] * 2,
                pltpu.VMEM((B // 2, B + B // 2), F32),
                pltpu.VMEM((VMAX - VMIN, 128), F32),
                pltpu.VMEM((B, 128), BF16),
                pltpu.VMEM((128, B), BF16),
                dma((10,)), dma((3,)), dma((R,)), dma((R,)), dma((R,)), dma((NS,)), dma((NS,)), dma((3,)), dma((NS, PER)), dma((3,)),
                pltpu.SemaphoreType.REGULAR,
            ],
            compiler_params=pltpu.CompilerParams(collective_id=0, has_side_effects=True,
                                                 vmem_limit_bytes=67043328),
        )(embeddings, valid_len, attn_gain, wq, wk, wv, wo, mlp_gain, w_gate[0], w_up[0], w_down[0],
          jnp.asarray(table))

        hid, k_t, v_t = pl.pallas_call(
            place_kernel,
            name="place",
            out_shape=tuple(jax.ShapeDtypeStruct(x.shape, BF16) for x in (hid, k_t, v_t)),
            in_specs=[any_spec] * 3,
            out_specs=(any_spec,) * 3,
            scratch_shapes=[pltpu.VMEM(x.shape, BF16) for x in (hid, k_t, v_t)] + [dma((3, 2)), dma((3, 2))],
            compiler_params=pltpu.CompilerParams(vmem_limit_bytes=67043328),
        )(hid, k_t, v_t)

        def to_cache(x):
            return x.reshape(KV, HD, SEQ).transpose(2, 0, 1)[None]

        return hid, to_cache(k_t), to_cache(v_t)

    return jax.shard_map(stage_program, mesh=mesh,
                         in_specs=(P('replica', None), P('replica'), gain_spec, spec_four, spec_four, spec_four, spec_four,
                                   gain_spec, spec_three, spec_three, spec_three),
                         out_specs=(P(('replica', 'stage'), None), P('stage', 'replica', None, None), P('stage', 'replica', None, None)),
                         check_vma=False)
```

```python
import math

import jax
import jax.numpy as jnp
import numpy as np
from jax import lax
from jax.experimental import pallas as pl
from jax.experimental.pallas import tpu as pltpu
from jax.sharding import PartitionSpec as P

EPS = 1e-5
ROPE_BASE = 10000.0
NEG = -1e30

SEQ = 1536
D = 2048
HEADS = 32
KV = 8
HD = 64
FF = 8192
STAGES = 4
B = 256
NB = SEQ // B
F = 512
NC = FF // F
NS = 3
VMIN = 768
VMAX = 1344
PIECE = SEQ // STAGES // 3
PER = B // PIECE
R = 4
LENT = R * F
SB = 4
EXP_SCALE = math.log2(math.e)

F32 = jnp.float32
BF16 = jnp.bfloat16


def rope_tables():
    inv_freq = ROPE_BASE ** (-np.arange(HD // 2, dtype=np.float64) * (2.0 / HD))
    angles = inv_freq[:, None] * np.arange(SEQ, dtype=np.float64)[None, :]
    tab = np.zeros((NB, 2, HD // 2, 256), np.float32)
    for blk in range(NB):
        cols = slice(blk * B, (blk + 1) * B)
        tab[blk, 0, :, :B] = np.cos(angles[:, cols])
        tab[blk, 1, :, :B] = np.sin(angles[:, cols])
    return tab


def dot(a, b):
    return jnp.dot(a, b, preferred_element_type=F32)


def dot_t(a, b):
    return lax.dot_general(a, b, (((1,), (1,)), ((), ())), preferred_element_type=F32)


def stage_kernel(emb, valid, again_hbm, wq, wk, wv, wo, mgain_hbm, wg, wu, wd, tab_hbm,
                 hid, kout, vout, wg_x, wu_x, wd_x,
                 tab, again, mgain, wqkv_v, wo_v, wg_s, wu_s, wd_s, resid, kc, vT, act, qT, y, mbuf, ff_s,
                 mask, vbias, kbias, qones,
                 w_sem, tab_sem, g_sem, u_sem, d_sem, in_sem, send_sem, kv_sem, piece_sem, out_sem, lend_sem, borrow_sem, pair_sem,
                 credit):
    stage = lax.axis_index("stage")
    helper = lax.rem(stage, 2) == 0
    partner = stage + 1 - 2 * lax.rem(stage, 2)
    barrier = pltpu.get_barrier_semaphore()
    for k in range(1, STAGES):
        pl.semaphore_signal(barrier, inc=1, device_id={"stage": lax.rem(stage + k, STAGES)},
                            device_id_type=pl.DeviceIdType.MESH)

    def emb_copy(i):
        return pltpu.make_async_copy(emb.at[pl.ds(pl.multiple_of(i * B, B), B), :], resid.at[lax.rem(i, NS)], in_sem.at[lax.rem(i, NS)])

    def w_copy(p):
        if p < 4:
            src = wq.at[pl.ds(p * 512, 512), :]
        elif p == 4:
            src = wk
        elif p == 5:
            src = wv
        else:
            src = wo.at[pl.ds((p - 6) * 512, 512), :]
        dst = wqkv_v.at[pl.ds(p * 512, 512), :] if p < 6 else wo_v.at[pl.ds((p - 6) * 512, 512), :]
        return pltpu.make_async_copy(src, dst, w_sem.at[p])

    def gu_copy(c, s):
        cols = pl.ds(pl.multiple_of(c * F, F), F)
        return (pltpu.make_async_copy(wg.at[:, cols], wg_s[s], g_sem.at[s]),
                pltpu.make_async_copy(wu.at[:, cols], wu_s[s], u_sem.at[s]))

    def dn_copy(c, s):
        rows = pl.ds(pl.multiple_of(c * F, F), F)
        return pltpu.make_async_copy(wd.at[rows, :], wd_s[s], d_sem.at[s])

    small_copies = [pltpu.make_async_copy(src, dst, tab_sem.at[n])
                    for n, (src, dst) in enumerate(((again_hbm, again), (mgain_hbm, mgain), (tab_hbm, tab)))]

    @pl.when(stage == 0)
    def _():
        emb_copy(0).start()

    for cp in small_copies:
        cp.start()
    for p in range(6):
        w_copy(p).start()

    for g in range(KV):
        qT[g, pl.ds((1 - g % 2) * HD, HD), :] = jnp.zeros((HD, 4 * B), BF16)
    valid_pos = valid[0]
    row = lax.broadcasted_iota(jnp.int32, vbias.shape, 0) + VMIN
    vbias[...] = jnp.where(row < valid_pos, 0.0, NEG).astype(F32)
    row = lax.broadcasted_iota(jnp.int32, kbias.shape, 0) + VMIN
    lane = lax.broadcasted_iota(jnp.int32, kbias.shape, 1)
    kbias[...] = jnp.where((lane == 0) & (row >= valid_pos), NEG, 0.0).astype(BF16)
    row = lax.broadcasted_iota(jnp.int32, qones.shape, 0)
    qones[...] = jnp.where(row == 0, 1.0, 0.0).astype(BF16)

    def norm(slot, gain_ref):
        for r in range(0, B, 16):
            x = resid[slot, pl.ds(r, 16), :].astype(F32)
            inv = lax.rsqrt(jnp.mean(x * x, axis=-1, keepdims=True) + EPS)
            act[pl.ds(r, 16), :] = (x * inv * gain_ref[...]).astype(BF16)

    def rope(x, cos, sin):
        front = x[:HD // 2]
        back = x[HD // 2:]
        return front * cos - back * sin, back * cos + front * sin

    def project(i):
        cos = tab[i, 0]
        sin = tab[i, 1]

        kt = dot_t(wqkv_v[pl.ds(2048, 512), :], act[...])
        parts = []
        for h in range(KV):
            parts += list(rope(kt[h * HD:(h + 1) * HD], cos, sin))
        for half in range(2):
            kh = jnp.concatenate(parts[half * 8:half * 8 + 8], axis=0).astype(BF16)
            ff_s[1][:, pl.ds(half * 256, 256)] = kh
            kc[pl.ds(pl.multiple_of(i * B, B), B), pl.ds(half * 256, 256)] = kh.T
        vt = dot_t(wqkv_v[pl.ds(2560, 512), :], act[...])
        vT[:, pl.ds(pl.multiple_of(i * B, B), B)] = vt.astype(BF16)

        for pair in range(4):
            qt = dot_t(wqkv_v[pl.ds(pair * 512, 512), :], act[...])
            for h in range(8):
                f, b = rope(qt[h * HD:(h + 1) * HD], cos, sin)
                g = pair * 2 + h // 4
                row = (g % 2) * HD
                cols = pl.ds((h % 4) * B, B)
                qT[g, pl.ds(row, HD // 2), cols] = (f * 0.125).astype(BF16)
                qT[g, pl.ds(row + HD // 2, HD // 2), cols] = (b * 0.125).astype(BF16)

    def make_mask(i):
        key = lax.broadcasted_iota(jnp.int32, mask.shape, 0)
        tok = lax.broadcasted_iota(jnp.int32, mask.shape, 1)
        key = jnp.where(tok < B, key, key + B // 2)
        tok = jnp.where(tok < B, tok, tok - B // 2)
        ok = (key <= tok) & (key + i * B < valid_pos)
        mask[...] = jnp.where(ok, 0.0, NEG).astype(F32)

    def attend(n):
        spans = [(c * B, min(B, VMAX - c * B), 0) for c in range(n + 1)]
        if spans[-1][1] == B:
            spans[-1:] = [(n * B, B // 2, 0), (n * B + B // 2, B // 2, B // 2)]
        total = spans[-1][0] + spans[-1][1]
        ahead_by = 1 if n == NB - 2 else 2

        def scores(g, u):
            kcols = pl.ds(pl.multiple_of((g // 2) * 128, 128), 128)
            q = qT[g, :, pl.ds((u % 4) * B, B)]
            m = None
            for start, rows, lane in spans:
                keys = kc[pl.ds(start, rows), kcols]
                if start >= n * B:
                    s = dot(keys, q[:, lane:]) + mask[pl.ds(0, rows), pl.ds(2 * lane, B - lane)]
                elif start >= VMIN and n == NB - 1:
                    bias = vbias[pl.ds(start - VMIN, rows), :]
                    s = dot(keys, q) + jnp.concatenate([bias, bias], axis=1)
                elif start >= VMIN:
                    bias = kbias[pl.ds(start - VMIN, rows), :]
                    s = dot(jnp.concatenate([keys, bias], axis=1), jnp.concatenate([q, qones[...]], axis=0))
                else:
                    s = dot(keys, q)
                y[pl.ds((u % SB) * total + start, rows), pl.ds(lane, B - lane)] = s
                cm = jnp.max(s.reshape(rows // 8, 8, B - lane), axis=0)
                if lane:
                    m = jnp.concatenate([m[:, :lane], jnp.maximum(m[:, lane:], cm)], axis=1)
                else:
                    m = cm if m is None else jnp.maximum(m, cm)
            mbuf[u % SB] = m

        def weighted(g, u):
            mc = jnp.max(mbuf[u % SB], axis=0, keepdims=True) * EXP_SCALE
            l = None
            probs = []
            for start, rows, lane in spans:
                sc = y[pl.ds((u % SB) * total + start, rows), pl.ds(lane, B - lane)]
                p = jnp.exp2(sc * EXP_SCALE - mc[:, lane:])
                ls = jnp.sum(p.reshape(rows // 8, 8, B - lane), axis=0)
                p = p.astype(BF16)
                if lane:
                    l = jnp.concatenate([l[:, :lane], l[:, lane:] + ls], axis=1)
                    p = jnp.concatenate([jnp.zeros((rows, lane), BF16), p], axis=1)
                else:
                    l = ls if l is None else l + ls
                probs.append(p)
            o = dot(vT[pl.ds(pl.multiple_of(g * HD, HD), HD), pl.ds(0, total)], jnp.concatenate(probs, axis=0))
            return (o * (1.0 / jnp.sum(l, axis=0, keepdims=True))).astype(BF16)

        for u in range(ahead_by):
            scores(0, u)

        def group_pair(pair, _):
            g = pair * 2
            outs = []
            for u in range(8):
                ahead = u + ahead_by
                scores(g + ahead // 4 if ahead < 8 else lax.rem(g + 2, KV), ahead)
                outs.append(weighted(g + u // 4, u))
                if u % 4 == 3:
                    act[:, pl.ds(pl.multiple_of((g + u // 4) * 256, 256), 256)] = jnp.concatenate(outs, axis=0).T
                    outs = []
            return 0

        lax.fori_loop(0, KV // 2, group_pair, 0)

    def out_proj(slot):
        for n in range(4):
            cols = pl.ds(n * 512, 512)
            o = dot(act[pl.ds(0, B), :], wo_v[:, cols])
            resid[slot, :, cols] = (resid[slot, :, cols].astype(F32) + o).astype(BF16)

    def lend_copies(c):
        sem = lend_sem
        cols = pl.ds(pl.multiple_of(FF - LENT + c * F, F), F)
        rows = pl.ds(pl.multiple_of(c * F, F), F)
        return [pltpu.make_async_remote_copy(src, dst, sem.at[n], borrow_sem.at[n, c], device_id={"stage": partner},
                                             device_id_type=pl.DeviceIdType.MESH)
                for n, (src, dst) in enumerate(((wg.at[:, cols], wg_x.at[:, rows]), (wu.at[:, cols], wu_x.at[:, rows]),
                                                (wd.at[cols, :], wd_x.at[rows, :])))]

    def borrowed_copies(c):
        part = pl.ds(c * F, F)
        return (pltpu.make_async_copy(wg_x.at[:, part], wg_s[c], g_sem.at[c]),
                pltpu.make_async_copy(wu_x.at[:, part], wu_s[c], u_sem.at[c]),
                pltpu.make_async_copy(wd_x.at[part, :], wd_s[c], d_sem.at[c]))

    def pair_copy(src, dst, n):
        return pltpu.make_async_remote_copy(src, dst, pair_sem.at[2 * n], pair_sem.at[2 * n + 1],
                                            device_id={"stage": partner}, device_id_type=pl.DeviceIdType.MESH)

    def act_copy():
        return pair_copy(act, act, 0)

    def sum_copy():
        return pair_copy(y.at[pl.ds(0, 8 * B), :], y.at[pl.ds(8 * B, 8 * B), :], 1)

    def gate_up(s):
        x = act[pl.ds(0, B), :]
        gate = dot(x, wg_s[s][...])
        up = dot(x, wu_s[s][...])
        ff_s[s % 2][...] = (gate * jax.nn.sigmoid(gate) * up).astype(BF16)

    def down(s):
        x = ff_s[s % 2][...]
        for n in range(8):
            rows = pl.ds(n * B, B)
            y[rows, :] = y[rows, :] + dot(x, wd_s[s][:, pl.ds(n * 256, 256)])

    def wait_gu(s):
        for cp in gu_copy(0, s):
            cp.wait()

    def wait_dn(s):
        dn_copy(0, s).wait()

    def start_gu(c, s, ok):
        @pl.when(ok)
        def _():
            for cp in gu_copy(lax.rem(c, NC), s):
                cp.start()

    def start_dn(c, s, ok):
        @pl.when(ok)
        def _():
            dn_copy(lax.rem(c, NC), s).start()

    def mlp(i):
        more = i + 1 < NB
        shared = (i == NB - 1) & jnp.logical_not(helper)
        mine = jnp.where(shared, NC - R, NC)
        wait_gu(0)
        gate_up(0)
        start_gu(R, 0, i < NB)

        def steps(it, _):
            c = it * R
            for u in range(R):
                if u % 2 == 0:
                    wait_gu((u + 1) % R)
                    wait_gu((u + 2) % R)
                    wait_dn(u)
                    wait_dn(u + 1)
                gate_up((u + 1) % R)
                start_gu(c + u + 1 + R, (u + 1) % R, more | (c + u + 1 + R < mine))
                down(u)
                start_dn(c + u + R, u, more | (c + u + R < mine))
            return 0

        lax.fori_loop(0, jnp.where(i < NB, jnp.where(shared, NC // R - 2, NC // R - 1), 0), steps, 0)
        for u in range(R):
            if u % 2 == 0:
                wait_gu(u + 1)
                if u + 2 < R:
                    wait_gu(u + 2)
                wait_dn(u)
                wait_dn(u + 1)
            if u + 1 < R:
                gate_up(u + 1)
                start_gu(u + 1, u + 1, more)
            down(u)
            start_dn(u, u, more)

    def next_copy(i):
        slot = lax.rem(i, NS)
        return pltpu.make_async_remote_copy(resid.at[slot], resid.at[slot], send_sem.at[slot], in_sem.at[slot],
                                            device_id={"stage": lax.rem(stage + 1, STAGES)},
                                            device_id_type=pl.DeviceIdType.MESH)

    def piece_copy(i, r):
        slot = lax.rem(i, NS)
        piece = i * PER + r
        row = lax.rem(piece, 3)
        src = resid.at[slot, pl.ds(r * PIECE, PIECE), :]
        dst = hid.at[pl.ds(pl.multiple_of(row * PIECE, PIECE), PIECE), :]
        remote = pltpu.make_async_remote_copy(src, dst, piece_sem.at[slot, r], out_sem.at[row],
                                              device_id={"stage": piece // 3}, device_id_type=pl.DeviceIdType.MESH)
        return remote, pltpu.make_async_copy(src, dst, out_sem.at[row]), piece // 3 == STAGES - 1

    def k_copy(i, half):
        cols = pl.ds(pl.multiple_of(i * B, B), B)
        return pltpu.make_async_copy(ff_s[1].at[:, pl.ds(half * 256, 256)], kout.at[pl.ds(half * 256, 256), cols],
                                     kv_sem.at[half])

    def v_copy(i):
        cols = pl.ds(pl.multiple_of(i * B, B), B)
        return pltpu.make_async_copy(vT.at[:, cols], vout.at[:, cols], kv_sem.at[2])

    last = stage == STAGES - 1

    def block(i, _):
        slot = lax.rem(i, NS)
        main = i < NB
        shared = (i == NB - 1) & jnp.logical_not(helper)

        @pl.when(main)
        def _():
            emb_copy(i).wait()

            @pl.when(i == 0)
            def _():
                for cp in small_copies:
                    cp.wait()

            norm(slot, again)

            @pl.when(i == 0)
            def _():
                for p in range(6):
                    w_copy(p).wait()
                for p in range(6, 10):
                    w_copy(p).start()
                for c in range(2):
                    start_gu(c, c, True)
                    start_dn(c, c, True)

            project(i)

            @pl.when(i == 0)
            def _():
                for c in range(2, R):
                    start_gu(c, c, True)
                    start_dn(c, c, True)
                pl.semaphore_wait(barrier, STAGES - 1)

            make_mask(i)
            k_copy(i, 0).start()
            k_copy(i, 1).start()
            v_copy(i).start()

            @pl.when(jnp.logical_not(helper) & (i < R))
            def _():
                for cp in lend_copies(i):
                    cp.start()

        for n in range(NB):
            @pl.when(i == n)
            def _():
                attend(n)

        @pl.when(main)
        def _():
            @pl.when((i >= 1) & jnp.logical_not(last))
            def _():
                next_copy(i - 1).wait_send()

            for r in range(PER):
                remote, local, mine = piece_copy(i - 1, r)

                @pl.when((i >= 1) & last & jnp.logical_not(mine))
                def _():
                    remote.wait_send()

            @pl.when((stage > 0) & (i >= 1) & (i - 1 + NS < NB))
            def _():
                pl.semaphore_signal(credit, inc=1, device_id={"stage": lax.rem(stage + STAGES - 1, STAGES)},
                                    device_id_type=pl.DeviceIdType.MESH)

            @pl.when((stage == 0) & (i + 1 < NB))
            def _():
                emb_copy(i + 1).start()

            @pl.when(i == 0)
            def _():
                for p in range(6, 10):
                    w_copy(p).wait()

            @pl.when(jnp.logical_not(helper) & (i < R))
            def _():
                for cp in lend_copies(i):
                    cp.wait_send()

            k_copy(i, 0).wait()
            k_copy(i, 1).wait()
            v_copy(i).wait()
            out_proj(slot)
            norm(slot, mgain)
            for n in range(8):
                y[pl.ds(n * B, B), :] = resid[slot, :, pl.ds(n * 256, 256)].astype(F32)

            @pl.when(shared)
            def _():
                act_copy().start()

        @pl.when(jnp.logical_not(main))
        def _():
            for c in range(R):
                for cp in lend_copies(c):
                    cp.wait_recv()
                for cp in borrowed_copies(c):
                    cp.start()
            y[pl.ds(0, 8 * B), :] = jnp.zeros((8 * B, B), F32)
            act_copy().wait_recv()

        mlp(i)

        @pl.when(shared)
        def _():
            act_copy().wait_send()
            sum_copy().wait_recv()
            for n in range(8):
                rows = pl.ds(n * B, B)
                y[rows, :] = y[rows, :] + y[pl.ds((n + 8) * B, B), :]

        @pl.when(jnp.logical_not(main))
        def _():
            sum_copy().start()
            sum_copy().wait_send()

        @pl.when(main)
        def _():
            for n in range(8):
                resid[slot, :, pl.ds(n * 256, 256)] = y[pl.ds(n * B, B), :].astype(BF16)

            @pl.when(jnp.logical_not(last) & (i >= NS))
            def _():
                pl.semaphore_wait(credit, 1)

            @pl.when(jnp.logical_not(last))
            def _():
                next_copy(i).start()

            for r in range(PER):
                remote, local, mine = piece_copy(i, r)

                @pl.when(last & jnp.logical_not(mine))
                def _():
                    remote.start()

                @pl.when(last & mine)
                def _():
                    local.start()

        return 0

    lax.fori_loop(0, NB + jnp.where(helper, 1, 0), block, 0)

    @pl.when(jnp.logical_not(last))
    def _():
        next_copy(NB - 1).wait_send()

    for row in range(3):
        piece_copy(row // PER, row % PER)[1].wait()

def place_kernel(hid, k_t, v_t, hid_out, k_out, v_out, hid_v, k_v, v_v, in_sem, out_sem):
    halves = []
    for n, (src, buf, dst) in enumerate(((hid, hid_v, hid_out), (k_t, k_v, k_out), (v_t, v_v, v_out))):
        rows = src.shape[0] // 2
        for half in range(2):
            part = pl.ds(half * rows, rows)
            halves.append((pltpu.make_async_copy(src.at[part], buf.at[part], in_sem.at[n, half]),
                           pltpu.make_async_copy(buf.at[part], dst.at[part], out_sem.at[n, half])))
    for load, _ in halves:
        load.start()
    for load, store in halves:
        load.wait()
        store.start()
    for _, store in halves:
        store.wait()


def solution(mesh):
    gain_spec = P('stage', None)
    spec_three = P('stage', None, None)
    spec_four = P('stage', None, None, None)
    table = rope_tables()
    dma = pltpu.SemaphoreType.DMA

    def stage_program(embeddings, valid_len, attn_gain, w_q, w_k, w_v, w_o, mlp_gain, w_gate, w_up, w_down):
        wq = w_q[0].transpose(1, 2, 0).reshape(HEADS * HD, D)
        wk = w_k[0].transpose(1, 2, 0).reshape(KV * HD, D)
        wv = w_v[0].transpose(1, 2, 0).reshape(KV * HD, D)
        wo = w_o[0].reshape(HEADS * HD, D)
        any_spec = pl.BlockSpec(memory_space=pl.ANY)
        vmem_spec = pl.BlockSpec(memory_space=pltpu.VMEM)
        smem_spec = pl.BlockSpec(memory_space=pltpu.SMEM)
        hid, k_t, v_t, _, _, _ = pl.pallas_call(
            stage_kernel,
            name="stage_pipeline",
            out_shape=(jax.ShapeDtypeStruct((SEQ // STAGES, D), BF16),
                       jax.ShapeDtypeStruct((KV * HD, SEQ), BF16),
                       jax.ShapeDtypeStruct((KV * HD, SEQ), BF16),
                       jax.ShapeDtypeStruct((D, LENT), BF16),
                       jax.ShapeDtypeStruct((D, LENT), BF16),
                       jax.ShapeDtypeStruct((LENT, D), BF16)),
            in_specs=[any_spec, smem_spec, any_spec, any_spec, any_spec, any_spec, any_spec, any_spec,
                      any_spec, any_spec, any_spec, any_spec],
            out_specs=(any_spec,) * 6,
            scratch_shapes=[
                pltpu.VMEM((NB, 2, HD // 2, 256), F32),
                pltpu.VMEM((1, D), F32),
                pltpu.VMEM((1, D), F32),
                pltpu.VMEM((3072, D), BF16),
                pltpu.VMEM((D, D), BF16),
                [pltpu.VMEM((D, F), BF16)] * R,
                [pltpu.VMEM((D, F), BF16)] * R,
                [pltpu.VMEM((F, D), BF16)] * R,
                pltpu.VMEM((NS, B, D), BF16),
                pltpu.VMEM((SEQ, KV * HD), BF16),
                pltpu.VMEM((KV * HD, SEQ), BF16),
                pltpu.VMEM((256, D), BF16),
                pltpu.VMEM((KV, 2 * HD, 4 * B), BF16),
                pltpu.VMEM((SB * VMAX, B), F32),
                pltpu.VMEM((SB, 8, B), F32),
                [pltpu.VMEM((B, F), BF16)] * 2,
                pltpu.VMEM((B // 2, B + B // 2), F32),
                pltpu.VMEM((VMAX - VMIN, 128), F32),
                pltpu.VMEM((B, 128), BF16),
                pltpu.VMEM((128, B), BF16),
                dma((10,)), dma((3,)), dma((R,)), dma((R,)), dma((R,)), dma((NS,)), dma((NS,)), dma((3,)), dma((NS, PER)), dma((3,)),
                dma((3,)), dma((3, R)), dma((4,)),
                pltpu.SemaphoreType.REGULAR,
            ],
            compiler_params=pltpu.CompilerParams(collective_id=0, has_side_effects=True,
                                                 vmem_limit_bytes=67043328),
        )(embeddings, valid_len, attn_gain, wq, wk, wv, wo, mlp_gain, w_gate[0], w_up[0], w_down[0],
          jnp.asarray(table))

        hid, k_t, v_t = pl.pallas_call(
            place_kernel,
            name="place",
            out_shape=tuple(jax.ShapeDtypeStruct(x.shape, BF16) for x in (hid, k_t, v_t)),
            in_specs=[any_spec] * 3,
            out_specs=(any_spec,) * 3,
            scratch_shapes=[pltpu.VMEM(x.shape, BF16) for x in (hid, k_t, v_t)] + [dma((3, 2)), dma((3, 2))],
            compiler_params=pltpu.CompilerParams(vmem_limit_bytes=67043328),
        )(hid, k_t, v_t)

        def to_cache(x):
            return x.reshape(KV, HD, SEQ).transpose(2, 0, 1)[None]

        return hid, to_cache(k_t), to_cache(v_t)

    return jax.shard_map(stage_program, mesh=mesh,
                         in_specs=(P('replica', None), P('replica'), gain_spec, spec_four, spec_four, spec_four, spec_four,
                                   gain_spec, spec_three, spec_three, spec_three),
                         out_specs=(P(('replica', 'stage'), None), P('stage', 'replica', None, None), P('stage', 'replica', None, None)),
                         check_vma=False)
```

```python
import math

import jax
import jax.numpy as jnp
import numpy as np
from jax import lax
from jax.experimental import pallas as pl
from jax.experimental.pallas import tpu as pltpu
from jax.sharding import PartitionSpec as P

EPS = 1e-5
ROPE_BASE = 10000.0
NEG = -1e30

SEQ = 1536
D = 2048
HEADS = 32
KV = 8
HD = 64
FF = 8192
STAGES = 4
B = 256
NB = SEQ // B
F = 512
NC = FF // F
NS = 3
VMIN = 768
VMAX = 1344
PIECE = SEQ // STAGES // 3
PER = B // PIECE
R = 4
LENT = R * F
SB = 4
EXP_SCALE = math.log2(math.e)

F32 = jnp.float32
BF16 = jnp.bfloat16


def rope_tables():
    inv_freq = ROPE_BASE ** (-np.arange(HD // 2, dtype=np.float64) * (2.0 / HD))
    angles = inv_freq[:, None] * np.arange(SEQ, dtype=np.float64)[None, :]
    tab = np.zeros((NB, 2, HD // 2, 256), np.float32)
    for blk in range(NB):
        cols = slice(blk * B, (blk + 1) * B)
        tab[blk, 0, :, :B] = np.cos(angles[:, cols])
        tab[blk, 1, :, :B] = np.sin(angles[:, cols])
    return tab


def dot(a, b):
    return jnp.dot(a, b, preferred_element_type=F32)


def dot_t(a, b):
    return lax.dot_general(a, b, (((1,), (1,)), ((), ())), preferred_element_type=F32)


def stage_kernel(emb, valid, again_hbm, wq, wk, wv, wo, mgain_hbm, wg, wu, wd, tab_hbm,
                 hid, kout, vout, wg_x, wu_x, wd_x,
                 tab, again, mgain, wqkv_v, wo_v, wg_s, wu_s, wd_s, resid, kc, vT, act, qT, y, mbuf, ff_s,
                 mask, vbias, kbias, qones,
                 w_sem, tab_sem, g_sem, u_sem, d_sem, in_sem, send_sem, kv_sem, piece_sem, out_sem, lend_sem, borrow_sem, pair_sem,
                 credit):
    stage = lax.axis_index("stage")
    helper = lax.rem(stage, 2) == 0
    partner = stage + 1 - 2 * lax.rem(stage, 2)
    barrier = pltpu.get_barrier_semaphore()
    for k in range(1, STAGES):
        pl.semaphore_signal(barrier, inc=1, device_id={"stage": lax.rem(stage + k, STAGES)},
                            device_id_type=pl.DeviceIdType.MESH)

    def emb_copy(i):
        return pltpu.make_async_copy(emb.at[pl.ds(pl.multiple_of(i * B, B), B), :], resid.at[lax.rem(i, NS)], in_sem.at[lax.rem(i, NS)])

    def w_copy(p):
        if p < 4:
            src = wq.at[pl.ds(p * 512, 512), :]
        elif p == 4:
            src = wk
        elif p == 5:
            src = wv
        else:
            src = wo.at[pl.ds((p - 6) * 512, 512), :]
        dst = wqkv_v.at[pl.ds(p * 512, 512), :] if p < 6 else wo_v.at[pl.ds((p - 6) * 512, 512), :]
        return pltpu.make_async_copy(src, dst, w_sem.at[p])

    def gu_copy(c, s):
        cols = pl.ds(pl.multiple_of(c * F, F), F)
        return (pltpu.make_async_copy(wg.at[:, cols], wg_s[s], g_sem.at[s]),
                pltpu.make_async_copy(wu.at[:, cols], wu_s[s], u_sem.at[s]))

    def dn_copy(c, s):
        rows = pl.ds(pl.multiple_of(c * F, F), F)
        return pltpu.make_async_copy(wd.at[rows, :], wd_s[s], d_sem.at[s])

    small_copies = [pltpu.make_async_copy(src, dst, tab_sem.at[n])
                    for n, (src, dst) in enumerate(((again_hbm, again), (mgain_hbm, mgain), (tab_hbm, tab)))]

    @pl.when(stage == 0)
    def _():
        emb_copy(0).start()

    for cp in small_copies:
        cp.start()
    for p in range(6):
        w_copy(p).start()

    for g in range(KV):
        qT[g, pl.ds((1 - g % 2) * HD, HD), :] = jnp.zeros((HD, 4 * B), BF16)
    valid_pos = valid[0]
    row = lax.broadcasted_iota(jnp.int32, vbias.shape, 0) + VMIN
    vbias[...] = jnp.where(row < valid_pos, 0.0, NEG).astype(F32)
    row = lax.broadcasted_iota(jnp.int32, kbias.shape, 0) + VMIN
    lane = lax.broadcasted_iota(jnp.int32, kbias.shape, 1)
    kbias[...] = jnp.where((lane == 0) & (row >= valid_pos), NEG, 0.0).astype(BF16)
    row = lax.broadcasted_iota(jnp.int32, qones.shape, 0)
    qones[...] = jnp.where(row == 0, 1.0, 0.0).astype(BF16)

    def norm(slot, gain_ref, main=None):
        for r in range(0, B, 16):
            x = resid[slot, pl.ds(r, 16), :].astype(F32)
            inv = lax.rsqrt(jnp.mean(x * x, axis=-1, keepdims=True) + EPS)
            x = (x * inv * gain_ref[...]).astype(BF16)
            for half in range(2):
                cols = slice(half * (D // 2), (half + 1) * (D // 2))
                part = x[:, cols]
                if main is not None:
                    sent = qT[half * 2 + r // 128, pl.ds(r % 128, 16), :]
                    part = jnp.where(main, part.astype(F32), sent.astype(F32)).astype(BF16)
                act[pl.ds(r, 16), cols] = part

    def rope(x, cos, sin):
        front = x[:HD // 2]
        back = x[HD // 2:]
        return front * cos - back * sin, back * cos + front * sin

    def project(i):
        cos = tab[i, 0]
        sin = tab[i, 1]

        kt = dot_t(wqkv_v[pl.ds(2048, 512), :], act[...])
        parts = []
        for h in range(KV):
            parts += list(rope(kt[h * HD:(h + 1) * HD], cos, sin))
        for half in range(2):
            kh = jnp.concatenate(parts[half * 8:half * 8 + 8], axis=0).astype(BF16)
            ff_s[1][:, pl.ds(half * 256, 256)] = kh
            kc[pl.ds(pl.multiple_of(i * B, B), B), pl.ds(half * 256, 256)] = kh.T
        for pair in range(4):
            qt = dot_t(wqkv_v[pl.ds(pair * 512, 512), :], act[...])
            for h in range(8):
                f, b = rope(qt[h * HD:(h + 1) * HD], cos, sin)
                g = pair * 2 + h // 4
                row = (g % 2) * HD
                cols = pl.ds((h % 4) * B, B)
                qT[g, pl.ds(row, HD // 2), cols] = (f * 0.125).astype(BF16)
                qT[g, pl.ds(row + HD // 2, HD // 2), cols] = (b * 0.125).astype(BF16)

        vt = dot_t(wqkv_v[pl.ds(2560, 512), :], act[...])
        vT[:, pl.ds(pl.multiple_of(i * B, B), B)] = vt.astype(BF16)

    def make_mask(i):
        key = lax.broadcasted_iota(jnp.int32, mask.shape, 0)
        tok = lax.broadcasted_iota(jnp.int32, mask.shape, 1)
        key = jnp.where(tok < B, key, key + B // 2)
        tok = jnp.where(tok < B, tok, tok - B // 2)
        ok = (key <= tok) & (key + i * B < valid_pos)
        mask[...] = jnp.where(ok, 0.0, NEG).astype(F32)

    def attend(n):
        spans = [(c * B, min(B, VMAX - c * B), 0) for c in range(n + 1)]
        if spans[-1][1] == B:
            spans[-1:] = [(n * B, B // 2, 0), (n * B + B // 2, B // 2, B // 2)]
        total = spans[-1][0] + spans[-1][1]
        ahead_by = 1 if n == NB - 2 else 2

        def scores(g, u):
            kcols = pl.ds(pl.multiple_of((g // 2) * 128, 128), 128)
            q = qT[g, :, pl.ds((u % 4) * B, B)]
            m = None
            for start, rows, lane in spans:
                keys = kc[pl.ds(start, rows), kcols]
                if start >= n * B:
                    s = dot(keys, q[:, lane:]) + mask[pl.ds(0, rows), pl.ds(2 * lane, B - lane)]
                elif start >= VMIN and n == NB - 1:
                    bias = vbias[pl.ds(start - VMIN, rows), :]
                    s = dot(keys, q) + jnp.concatenate([bias, bias], axis=1)
                elif start >= VMIN:
                    bias = kbias[pl.ds(start - VMIN, rows), :]
                    s = dot(jnp.concatenate([keys, bias], axis=1), jnp.concatenate([q, qones[...]], axis=0))
                else:
                    s = dot(keys, q)
                y[pl.ds((u % SB) * total + start, rows), pl.ds(lane, B - lane)] = s
                cm = jnp.max(s.reshape(rows // 8, 8, B - lane), axis=0)
                if lane:
                    m = jnp.concatenate([m[:, :lane], jnp.maximum(m[:, lane:], cm)], axis=1)
                else:
                    m = cm if m is None else jnp.maximum(m, cm)
            mbuf[u % SB] = m

        def weighted(g, u):
            mc = jnp.max(mbuf[u % SB], axis=0, keepdims=True) * EXP_SCALE
            l = None
            probs = []
            for start, rows, lane in spans:
                sc = y[pl.ds((u % SB) * total + start, rows), pl.ds(lane, B - lane)]
                p = jnp.exp2(sc * EXP_SCALE - mc[:, lane:])
                ls = jnp.sum(p.reshape(rows // 8, 8, B - lane), axis=0)
                p = p.astype(BF16)
                if lane:
                    l = jnp.concatenate([l[:, :lane], l[:, lane:] + ls], axis=1)
                    p = jnp.concatenate([jnp.zeros((rows, lane), BF16), p], axis=1)
                else:
                    l = ls if l is None else l + ls
                probs.append(p)
            o = dot(vT[pl.ds(pl.multiple_of(g * HD, HD), HD), pl.ds(0, total)], jnp.concatenate(probs, axis=0))
            return (o * (1.0 / jnp.sum(l, axis=0, keepdims=True))).astype(BF16)

        def put_out(g):
            act[:, pl.ds(pl.multiple_of(g * 256, 256), 256)] = ff_s[0][:, pl.ds(0, 256)].T

        for u in range(ahead_by):
            scores(0, u)

        def group_pair(pair, _):
            g = pair * 2
            outs = []
            for u in range(8):
                ahead = u + ahead_by
                scores(g + ahead // 4 if ahead < 8 else lax.rem(g + 2, KV), ahead)
                outs.append(weighted(g + u // 4, u))
                if u == 0:
                    put_out(lax.rem(g + KV - 1, KV))
                if u == 3:
                    act[:, pl.ds(pl.multiple_of(g * 256, 256), 256)] = jnp.concatenate(outs, axis=0).T
                    outs = []
            for h in range(4):
                ff_s[0][pl.ds(h * HD, HD), pl.ds(0, 256)] = outs[h]
            return 0

        lax.fori_loop(0, KV // 2, group_pair, 0)
        put_out(KV - 1)

    def out_proj(slot):
        for n in range(4):
            cols = pl.ds(n * 512, 512)
            o = dot(act[pl.ds(0, B), :], wo_v[:, cols])
            resid[slot, :, cols] = (resid[slot, :, cols].astype(F32) + o).astype(BF16)

    def lend_copies(c):
        sem = lend_sem
        cols = pl.ds(pl.multiple_of(FF - LENT + c * F, F), F)
        rows = pl.ds(pl.multiple_of(c * F, F), F)
        return [pltpu.make_async_remote_copy(src, dst, sem.at[n], borrow_sem.at[n, c], device_id={"stage": partner},
                                             device_id_type=pl.DeviceIdType.MESH)
                for n, (src, dst) in enumerate(((wg.at[:, cols], wg_x.at[:, rows]), (wu.at[:, cols], wu_x.at[:, rows]),
                                                (wd.at[cols, :], wd_x.at[rows, :])))]

    def borrowed_copies(c):
        part = pl.ds(c * F, F)
        return (pltpu.make_async_copy(wg_x.at[:, part], wg_s[c], g_sem.at[c]),
                pltpu.make_async_copy(wu_x.at[:, part], wu_s[c], u_sem.at[c]),
                pltpu.make_async_copy(wd_x.at[part, :], wd_s[c], d_sem.at[c]))

    def pair_copy(src, dst, n):
        return pltpu.make_async_remote_copy(src, dst, pair_sem.at[0, n], pair_sem.at[1, n],
                                            device_id={"stage": partner}, device_id_type=pl.DeviceIdType.MESH)

    def act_copies():
        return [pair_copy(act.at[pl.ds(r * 128, 128), pl.ds(half * 1024, 1024)], qT.at[half * 2 + r], half * 2 + r)
                for half in range(2) for r in range(2)]

    def sum_copy():
        return pair_copy(y.at[pl.ds(0, 8 * B), :], y.at[pl.ds(8 * B, 8 * B), :], 4)

    def gate_up(s):
        x = act[pl.ds(0, B), :]
        gate = dot(x, wg_s[s][...])
        up = dot(x, wu_s[s][...])
        ff_s[s % 2][...] = (gate * jax.nn.sigmoid(gate) * up).astype(BF16)

    def down(s):
        x = ff_s[s % 2][...]
        for n in range(8):
            rows = pl.ds(n * B, B)
            y[rows, :] = y[rows, :] + dot(x, wd_s[s][:, pl.ds(n * 256, 256)])

    def wait_gu(s):
        for cp in gu_copy(0, s):
            cp.wait()

    def wait_dn(s):
        dn_copy(0, s).wait()

    def start_gu(c, s, ok):
        @pl.when(ok)
        def _():
            for cp in gu_copy(lax.rem(c, NC), s):
                cp.start()

    def start_dn(c, s, ok):
        @pl.when(ok)
        def _():
            dn_copy(lax.rem(c, NC), s).start()

    def mlp(i):
        more = i + 1 < NB
        shared = (i == NB - 1) & jnp.logical_not(helper)
        mine = jnp.where(shared, NC - R, NC)
        wait_gu(0)
        gate_up(0)
        start_gu(R, 0, i < NB)

        def steps(it, _):
            c = it * R
            for u in range(R):
                if u % 2 == 0:
                    wait_gu((u + 1) % R)
                    wait_gu((u + 2) % R)
                    wait_dn(u)
                    wait_dn(u + 1)
                gate_up((u + 1) % R)
                start_gu(c + u + 1 + R, (u + 1) % R, more | (c + u + 1 + R < mine))
                down(u)
                start_dn(c + u + R, u, more | (c + u + R < mine))
            return 0

        lax.fori_loop(0, jnp.where(i < NB, jnp.where(shared, NC // R - 2, NC // R - 1), 0), steps, 0)
        for u in range(R):
            if u % 2 == 0:
                wait_gu(u + 1)
                if u + 2 < R:
                    wait_gu(u + 2)
                wait_dn(u)
                wait_dn(u + 1)
            if u + 1 < R:
                gate_up(u + 1)
                start_gu(u + 1, u + 1, more)
            down(u)
            start_dn(u, u, more)

    def next_copy(i):
        slot = lax.rem(i, NS)
        return pltpu.make_async_remote_copy(resid.at[slot], resid.at[slot], send_sem.at[slot], in_sem.at[slot],
                                            device_id={"stage": lax.rem(stage + 1, STAGES)},
                                            device_id_type=pl.DeviceIdType.MESH)

    def piece_copy(i, r):
        slot = lax.rem(i, NS)
        piece = i * PER + r
        row = lax.rem(piece, 3)
        src = resid.at[slot, pl.ds(r * PIECE, PIECE), :]
        dst = hid.at[pl.ds(pl.multiple_of(row * PIECE, PIECE), PIECE), :]
        remote = pltpu.make_async_remote_copy(src, dst, piece_sem.at[slot, r], out_sem.at[row],
                                              device_id={"stage": piece // 3}, device_id_type=pl.DeviceIdType.MESH)
        return remote, pltpu.make_async_copy(src, dst, out_sem.at[row]), piece // 3 == STAGES - 1

    def k_copy(i, half):
        cols = pl.ds(pl.multiple_of(i * B, B), B)
        return pltpu.make_async_copy(ff_s[1].at[:, pl.ds(half * 256, 256)], kout.at[pl.ds(half * 256, 256), cols],
                                     kv_sem.at[half])

    def v_copy(i):
        cols = pl.ds(pl.multiple_of(i * B, B), B)
        return pltpu.make_async_copy(vT.at[:, cols], vout.at[:, cols], kv_sem.at[2])

    last = stage == STAGES - 1

    def block(i, _):
        slot = lax.rem(i, NS)
        main = i < NB
        shared = (i == NB - 1) & jnp.logical_not(helper)

        @pl.when(main)
        def _():
            emb_copy(i).wait()

            @pl.when(i == 0)
            def _():
                for cp in small_copies:
                    cp.wait()

            norm(slot, again)

            @pl.when(i == 0)
            def _():
                for p in range(6):
                    w_copy(p).wait()
                for p in range(6, 10):
                    w_copy(p).start()
                for c in range(2):
                    start_gu(c, c, True)
                    start_dn(c, c, True)

            project(i)

            @pl.when(i == 0)
            def _():
                for c in range(2, R):
                    start_gu(c, c, True)
                    start_dn(c, c, True)
                pl.semaphore_wait(barrier, STAGES - 1)

            make_mask(i)
            k_copy(i, 0).start()
            k_copy(i, 1).start()
            v_copy(i).start()

            @pl.when(jnp.logical_not(helper) & (i < R))
            def _():
                for cp in lend_copies(i):
                    cp.start()

        for n in range(NB):
            @pl.when(i == n)
            def _():
                attend(n)

        @pl.when(main)
        def _():
            @pl.when((i >= 1) & jnp.logical_not(last))
            def _():
                next_copy(i - 1).wait_send()

            for r in range(PER):
                remote, local, mine = piece_copy(i - 1, r)

                @pl.when((i >= 1) & last & jnp.logical_not(mine))
                def _():
                    remote.wait_send()

            @pl.when((stage > 0) & (i >= 1) & (i - 1 + NS < NB))
            def _():
                pl.semaphore_signal(credit, inc=1, device_id={"stage": lax.rem(stage + STAGES - 1, STAGES)},
                                    device_id_type=pl.DeviceIdType.MESH)

            @pl.when((stage == 0) & (i + 1 < NB))
            def _():
                emb_copy(i + 1).start()

            @pl.when(i == 0)
            def _():
                for p in range(6, 10):
                    w_copy(p).wait()

            @pl.when(jnp.logical_not(helper) & (i < R))
            def _():
                for cp in lend_copies(i):
                    cp.wait_send()

            k_copy(i, 0).wait()
            k_copy(i, 1).wait()
            v_copy(i).wait()

        @pl.when(jnp.logical_not(main))
        def _():
            for c in range(R):
                for cp in lend_copies(c):
                    cp.wait_recv()
                for cp in borrowed_copies(c):
                    cp.start()
            for cp in act_copies():
                cp.wait_recv()

        out_proj(slot)
        norm(slot, mgain, main)
        for n in range(8):
            h = resid[slot, :, pl.ds(n * 256, 256)].astype(F32)
            y[pl.ds(n * B, B), :] = jnp.where(main, h, 0.0)

        @pl.when(shared)
        def _():
            for cp in act_copies():
                cp.start()

        mlp(i)
        for n in range(8):
            resid[slot, :, pl.ds(n * 256, 256)] = y[pl.ds(n * B, B), :].astype(BF16)

        @pl.when(shared)
        def _():
            for cp in act_copies():
                cp.wait_send()
            sum_copy().wait_recv()
            for n in range(8):
                h = y[pl.ds(n * B, B), :] + y[pl.ds((n + 8) * B, B), :]
                resid[slot, :, pl.ds(n * 256, 256)] = h.astype(BF16)

        @pl.when(jnp.logical_not(main))
        def _():
            sum_copy().start()
            sum_copy().wait_send()

        @pl.when(main)
        def _():
            @pl.when(jnp.logical_not(last) & (i >= NS))
            def _():
                pl.semaphore_wait(credit, 1)

            @pl.when(jnp.logical_not(last))
            def _():
                next_copy(i).start()

            for r in range(PER):
                remote, local, mine = piece_copy(i, r)

                @pl.when(last & jnp.logical_not(mine))
                def _():
                    remote.start()

                @pl.when(last & mine)
                def _():
                    local.start()

        return 0

    lax.fori_loop(0, NB + jnp.where(helper, 1, 0), block, 0)

    @pl.when(jnp.logical_not(last))
    def _():
        next_copy(NB - 1).wait_send()

    for row in range(3):
        piece_copy(row // PER, row % PER)[1].wait()

def place_kernel(hid, k_t, v_t, hid_out, k_out, v_out, hid_v, k_v, v_v, in_sem, out_sem):
    halves = []
    for n, (src, buf, dst) in enumerate(((hid, hid_v, hid_out), (k_t, k_v, k_out), (v_t, v_v, v_out))):
        rows = src.shape[0] // 2
        for half in range(2):
            part = pl.ds(half * rows, rows)
            halves.append((pltpu.make_async_copy(src.at[part], buf.at[part], in_sem.at[n, half]),
                           pltpu.make_async_copy(buf.at[part], dst.at[part], out_sem.at[n, half])))
    for load, _ in halves:
        load.start()
    for load, store in halves:
        load.wait()
        store.start()
    for _, store in halves:
        store.wait()


def solution(mesh):
    gain_spec = P('stage', None)
    spec_three = P('stage', None, None)
    spec_four = P('stage', None, None, None)
    table = rope_tables()
    dma = pltpu.SemaphoreType.DMA

    def stage_program(embeddings, valid_len, attn_gain, w_q, w_k, w_v, w_o, mlp_gain, w_gate, w_up, w_down):
        wq = w_q[0].transpose(1, 2, 0).reshape(HEADS * HD, D)
        wk = w_k[0].transpose(1, 2, 0).reshape(KV * HD, D)
        wv = w_v[0].transpose(1, 2, 0).reshape(KV * HD, D)
        wo = w_o[0].reshape(HEADS * HD, D)
        any_spec = pl.BlockSpec(memory_space=pl.ANY)
        vmem_spec = pl.BlockSpec(memory_space=pltpu.VMEM)
        smem_spec = pl.BlockSpec(memory_space=pltpu.SMEM)
        hid, k_t, v_t, _, _, _ = pl.pallas_call(
            stage_kernel,
            name="stage_pipeline",
            out_shape=(jax.ShapeDtypeStruct((SEQ // STAGES, D), BF16),
                       jax.ShapeDtypeStruct((KV * HD, SEQ), BF16),
                       jax.ShapeDtypeStruct((KV * HD, SEQ), BF16),
                       jax.ShapeDtypeStruct((D, LENT), BF16),
                       jax.ShapeDtypeStruct((D, LENT), BF16),
                       jax.ShapeDtypeStruct((LENT, D), BF16)),
            in_specs=[any_spec, smem_spec, any_spec, any_spec, any_spec, any_spec, any_spec, any_spec,
                      any_spec, any_spec, any_spec, any_spec],
            out_specs=(any_spec,) * 6,
            scratch_shapes=[
                pltpu.VMEM((NB, 2, HD // 2, 256), F32),
                pltpu.VMEM((1, D), F32),
                pltpu.VMEM((1, D), F32),
                pltpu.VMEM((3072, D), BF16),
                pltpu.VMEM((D, D), BF16),
                [pltpu.VMEM((D, F), BF16)] * R,
                [pltpu.VMEM((D, F), BF16)] * R,
                [pltpu.VMEM((F, D), BF16)] * R,
                pltpu.VMEM((NS, B, D), BF16),
                pltpu.VMEM((SEQ, KV * HD), BF16),
                pltpu.VMEM((KV * HD, SEQ), BF16),
                pltpu.VMEM((256, D), BF16),
                pltpu.VMEM((KV, 2 * HD, 4 * B), BF16),
                pltpu.VMEM((SB * VMAX, B), F32),
                pltpu.VMEM((SB, 8, B), F32),
                [pltpu.VMEM((B, F), BF16)] * 2,
                pltpu.VMEM((B // 2, B + B // 2), F32),
                pltpu.VMEM((VMAX - VMIN, 128), F32),
                pltpu.VMEM((B, 128), BF16),
                pltpu.VMEM((128, B), BF16),
                dma((10,)), dma((3,)), dma((R,)), dma((R,)), dma((R,)), dma((NS,)), dma((NS,)), dma((3,)), dma((NS, PER)), dma((3,)),
                dma((3,)), dma((3, R)), dma((2, 5)),
                pltpu.SemaphoreType.REGULAR,
            ],
            compiler_params=pltpu.CompilerParams(collective_id=0, has_side_effects=True,
                                                 vmem_limit_bytes=67043328),
        )(embeddings, valid_len, attn_gain, wq, wk, wv, wo, mlp_gain, w_gate[0], w_up[0], w_down[0],
          jnp.asarray(table))

        hid, k_t, v_t = pl.pallas_call(
            place_kernel,
            name="place",
            out_shape=tuple(jax.ShapeDtypeStruct(x.shape, BF16) for x in (hid, k_t, v_t)),
            in_specs=[any_spec] * 3,
            out_specs=(any_spec,) * 3,
            scratch_shapes=[pltpu.VMEM(x.shape, BF16) for x in (hid, k_t, v_t)] + [dma((3, 2)), dma((3, 2))],
            compiler_params=pltpu.CompilerParams(vmem_limit_bytes=67043328),
        )(hid, k_t, v_t)

        def to_cache(x):
            return x.reshape(KV, HD, SEQ).transpose(2, 0, 1)[None]

        return hid, to_cache(k_t), to_cache(v_t)

    return jax.shard_map(stage_program, mesh=mesh,
                         in_specs=(P('replica', None), P('replica'), gain_spec, spec_four, spec_four, spec_four, spec_four,
                                   gain_spec, spec_three, spec_three, spec_three),
                         out_specs=(P(('replica', 'stage'), None), P('stage', 'replica', None, None), P('stage', 'replica', None, None)),
                         check_vma=False)
```

```python
import math

import jax
import jax.numpy as jnp
import numpy as np
from jax import lax
from jax.experimental import pallas as pl
from jax.experimental.pallas import tpu as pltpu
from jax.sharding import PartitionSpec as P

EPS = 1e-5
ROPE_BASE = 10000.0
NEG = -1e30

SEQ = 1536
D = 2048
HEADS = 32
KV = 8
HD = 64
FF = 8192
STAGES = 4
B = 256
NB = SEQ // B
F = 512
NC = FF // F
NS = 3
VMIN = 768
VMAX = 1344
PIECE = SEQ // STAGES // 3
PER = B // PIECE
R = 4
LENT = R * F
SB = 4
EXP_SCALE = math.log2(math.e)

F32 = jnp.float32
BF16 = jnp.bfloat16


def rope_tables():
    inv_freq = ROPE_BASE ** (-np.arange(HD // 2, dtype=np.float64) * (2.0 / HD))
    angles = inv_freq[:, None] * np.arange(SEQ, dtype=np.float64)[None, :]
    tab = np.zeros((NB, 2, HD // 2, 256), np.float32)
    for blk in range(NB):
        cols = slice(blk * B, (blk + 1) * B)
        tab[blk, 0, :, :B] = np.cos(angles[:, cols])
        tab[blk, 1, :, :B] = np.sin(angles[:, cols])
    return tab


def dot(a, b):
    return jnp.dot(a, b, preferred_element_type=F32)


def dot_t(a, b):
    return lax.dot_general(a, b, (((1,), (1,)), ((), ())), preferred_element_type=F32)


def stage_kernel(emb, valid, again_hbm, wq, wk, wv, wo, mgain_hbm, wg, wu, wd, tab_hbm,
                 hid, kout, vout, wg_x, wu_x, wd_x,
                 tab, again, mgain, wqkv_v, wo_v, wg_s, wu_s, wd_s, resid, kc, vT, act, qT, y, mbuf, ff_s,
                 mask, vbias, kbias, qones,
                 w_sem, tab_sem, g_sem, u_sem, d_sem, in_sem, send_sem, kv_sem, piece_sem, out_sem, lend_sem, borrow_sem, pair_sem,
                 credit):
    stage = lax.axis_index("stage")
    helper = lax.rem(stage, 2) == 0
    partner = stage + 1 - 2 * lax.rem(stage, 2)
    barrier = pltpu.get_barrier_semaphore()
    for k in range(1, STAGES):
        pl.semaphore_signal(barrier, inc=1, device_id={"stage": lax.rem(stage + k, STAGES)},
                            device_id_type=pl.DeviceIdType.MESH)

    def emb_copy(i):
        return pltpu.make_async_copy(emb.at[pl.ds(pl.multiple_of(i * B, B), B), :], resid.at[lax.rem(i, NS)], in_sem.at[lax.rem(i, NS)])

    def w_copy(p):
        if p < 4:
            src = wq.at[pl.ds(p * 512, 512), :]
        elif p == 4:
            src = wk
        elif p == 5:
            src = wv
        else:
            src = wo.at[pl.ds((p - 6) * 512, 512), :]
        dst = wqkv_v.at[pl.ds(p * 512, 512), :] if p < 6 else wo_v.at[pl.ds((p - 6) * 512, 512), :]
        return pltpu.make_async_copy(src, dst, w_sem.at[p])

    def gu_copy(c, s):
        cols = pl.ds(pl.multiple_of(c * F, F), F)
        return (pltpu.make_async_copy(wg.at[:, cols], wg_s[s], g_sem.at[s]),
                pltpu.make_async_copy(wu.at[:, cols], wu_s[s], u_sem.at[s]))

    def dn_copy(c, s):
        rows = pl.ds(pl.multiple_of(c * F, F), F)
        return pltpu.make_async_copy(wd.at[rows, :], wd_s[s], d_sem.at[s])

    small_copies = [pltpu.make_async_copy(src, dst, tab_sem.at[n])
                    for n, (src, dst) in enumerate(((again_hbm, again), (mgain_hbm, mgain), (tab_hbm, tab)))]

    @pl.when(stage == 0)
    def _():
        emb_copy(0).start()

    for cp in small_copies:
        cp.start()
    for p in range(6):
        w_copy(p).start()

    for g in range(KV):
        qT[g, pl.ds((1 - g % 2) * HD, HD), :] = jnp.zeros((HD, 4 * B), BF16)
    valid_pos = valid[0]
    row = lax.broadcasted_iota(jnp.int32, vbias.shape, 0) + VMIN
    vbias[...] = jnp.where(row < valid_pos, 0.0, NEG).astype(F32)
    row = lax.broadcasted_iota(jnp.int32, kbias.shape, 0) + VMIN
    lane = lax.broadcasted_iota(jnp.int32, kbias.shape, 1)
    kbias[...] = jnp.where((lane == 0) & (row >= valid_pos), NEG, 0.0).astype(BF16)
    row = lax.broadcasted_iota(jnp.int32, qones.shape, 0)
    qones[...] = jnp.where(row == 0, 1.0, 0.0).astype(BF16)

    def norm(slot, gain_ref):
        for r in range(0, B, 16):
            x = resid[slot, pl.ds(r, 16), :].astype(F32)
            inv = lax.rsqrt(jnp.mean(x * x, axis=-1, keepdims=True) + EPS)
            act[pl.ds(r, 16), :] = (x * inv * gain_ref[...]).astype(BF16)

    def rope(x, cos, sin):
        front = x[:HD // 2]
        back = x[HD // 2:]
        return front * cos - back * sin, back * cos + front * sin

    def project(i):
        cos = tab[i, 0]
        sin = tab[i, 1]

        kt = dot_t(wqkv_v[pl.ds(2048, 512), :], act[...])
        parts = []
        for h in range(KV):
            parts += list(rope(kt[h * HD:(h + 1) * HD], cos, sin))
        for half in range(2):
            kh = jnp.concatenate(parts[half * 8:half * 8 + 8], axis=0).astype(BF16)
            ff_s[1][:, pl.ds(half * 256, 256)] = kh
            kc[pl.ds(pl.multiple_of(i * B, B), B), pl.ds(half * 256, 256)] = kh.T
        vt = dot_t(wqkv_v[pl.ds(2560, 512), :], act[...])
        vT[:, pl.ds(pl.multiple_of(i * B, B), B)] = vt.astype(BF16)

        for pair in range(4):
            qt = dot_t(wqkv_v[pl.ds(pair * 512, 512), :], act[...])
            for h in range(8):
                f, b = rope(qt[h * HD:(h + 1) * HD], cos, sin)
                g = pair * 2 + h // 4
                row = (g % 2) * HD
                cols = pl.ds((h % 4) * B, B)
                qT[g, pl.ds(row, HD // 2), cols] = (f * 0.125).astype(BF16)
                qT[g, pl.ds(row + HD // 2, HD // 2), cols] = (b * 0.125).astype(BF16)

    def make_mask(i):
        key = lax.broadcasted_iota(jnp.int32, mask.shape, 0)
        tok = lax.broadcasted_iota(jnp.int32, mask.shape, 1)
        key = jnp.where(tok < B, key, key + B // 2)
        tok = jnp.where(tok < B, tok, tok - B // 2)
        ok = (key <= tok) & (key + i * B < valid_pos)
        mask[...] = jnp.where(ok, 0.0, NEG).astype(F32)

    def attend(n):
        spans = [(c * B, min(B, VMAX - c * B), 0) for c in range(n + 1)]
        if spans[-1][1] == B:
            spans[-1:] = [(n * B, B // 2, 0), (n * B + B // 2, B // 2, B // 2)]
        total = spans[-1][0] + spans[-1][1]
        ahead_by = 1 if n == NB - 2 else 2

        def scores(g, u):
            kcols = pl.ds(pl.multiple_of((g // 2) * 128, 128), 128)
            q = qT[g, :, pl.ds((u % 4) * B, B)]
            m = None
            for start, rows, lane in spans:
                keys = kc[pl.ds(start, rows), kcols]
                if start >= n * B:
                    s = dot(keys, q[:, lane:]) + mask[pl.ds(0, rows), pl.ds(2 * lane, B - lane)]
                elif start >= VMIN and n == NB - 1:
                    bias = vbias[pl.ds(start - VMIN, rows), :]
                    s = dot(keys, q) + jnp.concatenate([bias, bias], axis=1)
                elif start >= VMIN:
                    bias = kbias[pl.ds(start - VMIN, rows), :]
                    s = dot(jnp.concatenate([keys, bias], axis=1), jnp.concatenate([q, qones[...]], axis=0))
                else:
                    s = dot(keys, q)
                y[pl.ds((u % SB) * total + start, rows), pl.ds(lane, B - lane)] = s
                cm = jnp.max(s.reshape(rows // 8, 8, B - lane), axis=0)
                if lane:
                    m = jnp.concatenate([m[:, :lane], jnp.maximum(m[:, lane:], cm)], axis=1)
                else:
                    m = cm if m is None else jnp.maximum(m, cm)
            mbuf[u % SB] = m

        def weighted(g, u):
            mc = jnp.max(mbuf[u % SB], axis=0, keepdims=True) * EXP_SCALE
            l = None
            probs = []
            for start, rows, lane in spans:
                sc = y[pl.ds((u % SB) * total + start, rows), pl.ds(lane, B - lane)]
                p = jnp.exp2(sc * EXP_SCALE - mc[:, lane:])
                ls = jnp.sum(p.reshape(rows // 8, 8, B - lane), axis=0)
                p = p.astype(BF16)
                if lane:
                    l = jnp.concatenate([l[:, :lane], l[:, lane:] + ls], axis=1)
                    p = jnp.concatenate([jnp.zeros((rows, lane), BF16), p], axis=1)
                else:
                    l = ls if l is None else l + ls
                probs.append(p)
            o = dot(vT[pl.ds(pl.multiple_of(g * HD, HD), HD), pl.ds(0, total)], jnp.concatenate(probs, axis=0))
            return (o * (1.0 / jnp.sum(l, axis=0, keepdims=True))).astype(BF16)

        def put_out(g):
            act[:, pl.ds(pl.multiple_of(g * 256, 256), 256)] = ff_s[0][:, pl.ds(0, 256)].T

        for u in range(ahead_by):
            scores(0, u)

        def group_pair(pair, _):
            g = pair * 2
            outs = []
            for u in range(8):
                ahead = u + ahead_by
                scores(g + ahead // 4 if ahead < 8 else lax.rem(g + 2, KV), ahead)
                outs.append(weighted(g + u // 4, u))
                if u == 0:
                    put_out(lax.rem(g + KV - 1, KV))
                if u == 3:
                    act[:, pl.ds(pl.multiple_of(g * 256, 256), 256)] = jnp.concatenate(outs, axis=0).T
                    outs = []
            for h in range(4):
                ff_s[0][pl.ds(h * HD, HD), pl.ds(0, 256)] = outs[h]
            return 0

        lax.fori_loop(0, KV // 2, group_pair, 0)
        put_out(KV - 1)

    def out_proj(slot):
        for n in range(4):
            cols = pl.ds(n * 512, 512)
            o = dot(act[pl.ds(0, B), :], wo_v[:, cols])
            resid[slot, :, cols] = (resid[slot, :, cols].astype(F32) + o).astype(BF16)

    def lend_copies(c):
        sem = lend_sem
        cols = pl.ds(pl.multiple_of(FF - LENT + c * F, F), F)
        rows = pl.ds(pl.multiple_of(c * F, F), F)
        return [pltpu.make_async_remote_copy(src, dst, sem.at[n], borrow_sem.at[n, c], device_id={"stage": partner},
                                             device_id_type=pl.DeviceIdType.MESH)
                for n, (src, dst) in enumerate(((wg.at[:, cols], wg_x.at[:, rows]), (wu.at[:, cols], wu_x.at[:, rows]),
                                                (wd.at[cols, :], wd_x.at[rows, :])))]

    def borrowed_copies(c):
        part = pl.ds(c * F, F)
        return (pltpu.make_async_copy(wg_x.at[:, part], wg_s[c], g_sem.at[c]),
                pltpu.make_async_copy(wu_x.at[:, part], wu_s[c], u_sem.at[c]),
                pltpu.make_async_copy(wd_x.at[part, :], wd_s[c], d_sem.at[c]))

    def pair_copy(src, dst, n):
        return pltpu.make_async_remote_copy(src, dst, pair_sem.at[2 * n], pair_sem.at[2 * n + 1],
                                            device_id={"stage": partner}, device_id_type=pl.DeviceIdType.MESH)

    def act_copy():
        return pair_copy(act, act, 0)

    def sum_copy():
        return pair_copy(y.at[pl.ds(0, 8 * B), :], y.at[pl.ds(8 * B, 8 * B), :], 1)

    def gate_up(s):
        x = act[pl.ds(0, B), :]
        gate = dot(x, wg_s[s][...])
        up = dot(x, wu_s[s][...])
        ff_s[s % 2][...] = (gate * jax.nn.sigmoid(gate) * up).astype(BF16)

    def down(s):
        x = ff_s[s % 2][...]
        for n in range(8):
            rows = pl.ds(n * B, B)
            y[rows, :] = y[rows, :] + dot(x, wd_s[s][:, pl.ds(n * 256, 256)])

    def wait_gu(s):
        for cp in gu_copy(0, s):
            cp.wait()

    def wait_dn(s):
        dn_copy(0, s).wait()

    def start_gu(c, s, ok):
        @pl.when(ok)
        def _():
            for cp in gu_copy(lax.rem(c, NC), s):
                cp.start()

    def start_dn(c, s, ok):
        @pl.when(ok)
        def _():
            dn_copy(lax.rem(c, NC), s).start()

    def mlp(i):
        more = i + 1 < NB
        shared = (i == NB - 1) & jnp.logical_not(helper)
        mine = jnp.where(shared, NC - R, NC)
        wait_gu(0)
        gate_up(0)
        start_gu(R, 0, i < NB)

        def steps(it, _):
            c = it * R
            for u in range(R):
                if u % 2 == 0:
                    wait_gu((u + 1) % R)
                    wait_gu((u + 2) % R)
                    wait_dn(u)
                    wait_dn(u + 1)
                gate_up((u + 1) % R)
                start_gu(c + u + 1 + R, (u + 1) % R, more | (c + u + 1 + R < mine))
                down(u)
                start_dn(c + u + R, u, more | (c + u + R < mine))
            return 0

        lax.fori_loop(0, jnp.where(i < NB, jnp.where(shared, NC // R - 2, NC // R - 1), 0), steps, 0)
        for u in range(R):
            if u % 2 == 0:
                wait_gu(u + 1)
                if u + 2 < R:
                    wait_gu(u + 2)
                wait_dn(u)
                wait_dn(u + 1)
            if u + 1 < R:
                gate_up(u + 1)
                start_gu(u + 1, u + 1, more)
            down(u)
            start_dn(u, u, more)

    def next_copy(i):
        slot = lax.rem(i, NS)
        return pltpu.make_async_remote_copy(resid.at[slot], resid.at[slot], send_sem.at[slot], in_sem.at[slot],
                                            device_id={"stage": lax.rem(stage + 1, STAGES)},
                                            device_id_type=pl.DeviceIdType.MESH)

    def piece_copy(i, r):
        slot = lax.rem(i, NS)
        piece = i * PER + r
        row = lax.rem(piece, 3)
        src = resid.at[slot, pl.ds(r * PIECE, PIECE), :]
        dst = hid.at[pl.ds(pl.multiple_of(row * PIECE, PIECE), PIECE), :]
        remote = pltpu.make_async_remote_copy(src, dst, piece_sem.at[slot, r], out_sem.at[row],
                                              device_id={"stage": piece // 3}, device_id_type=pl.DeviceIdType.MESH)
        return remote, pltpu.make_async_copy(src, dst, out_sem.at[row]), piece // 3 == STAGES - 1

    def k_copy(i, half):
        cols = pl.ds(pl.multiple_of(i * B, B), B)
        return pltpu.make_async_copy(ff_s[1].at[:, pl.ds(half * 256, 256)], kout.at[pl.ds(half * 256, 256), cols],
                                     kv_sem.at[half])

    def v_copy(i):
        cols = pl.ds(pl.multiple_of(i * B, B), B)
        return pltpu.make_async_copy(vT.at[:, cols], vout.at[:, cols], kv_sem.at[2])

    last = stage == STAGES - 1

    def block(i, _):
        slot = lax.rem(i, NS)
        main = i < NB
        shared = (i == NB - 1) & jnp.logical_not(helper)

        @pl.when(main)
        def _():
            emb_copy(i).wait()

            @pl.when(i == 0)
            def _():
                for cp in small_copies:
                    cp.wait()

            norm(slot, again)

            @pl.when(i == 0)
            def _():
                for p in range(6):
                    w_copy(p).wait()
                for p in range(6, 10):
                    w_copy(p).start()
                for c in range(2):
                    start_gu(c, c, True)
                    start_dn(c, c, True)

            project(i)

            @pl.when(i == 0)
            def _():
                for c in range(2, R):
                    start_gu(c, c, True)
                    start_dn(c, c, True)
                pl.semaphore_wait(barrier, STAGES - 1)

            make_mask(i)
            k_copy(i, 0).start()
            k_copy(i, 1).start()
            v_copy(i).start()

        for n in range(NB):
            @pl.when(i == n)
            def _():
                attend(n)

        @pl.when(main)
        def _():
            @pl.when((i >= 1) & jnp.logical_not(last))
            def _():
                next_copy(i - 1).wait_send()

            for r in range(PER):
                remote, local, mine = piece_copy(i - 1, r)

                @pl.when((i >= 1) & last & jnp.logical_not(mine))
                def _():
                    remote.wait_send()

            @pl.when((stage > 0) & (i >= 1) & (i - 1 + NS < NB))
            def _():
                pl.semaphore_signal(credit, inc=1, device_id={"stage": lax.rem(stage + STAGES - 1, STAGES)},
                                    device_id_type=pl.DeviceIdType.MESH)

            @pl.when((stage == 0) & (i + 1 < NB))
            def _():
                emb_copy(i + 1).start()

            @pl.when(i == 0)
            def _():
                for p in range(6, 10):
                    w_copy(p).wait()

            k_copy(i, 0).wait()
            k_copy(i, 1).wait()
            v_copy(i).wait()
            out_proj(slot)
            norm(slot, mgain)
            for n in range(8):
                y[pl.ds(n * B, B), :] = resid[slot, :, pl.ds(n * 256, 256)].astype(F32)

            @pl.when(shared)
            def _():
                act_copy().start()

        @pl.when(jnp.logical_not(main))
        def _():
            for c in range(R):
                for cp in lend_copies(c):
                    cp.wait_recv()
                for cp in borrowed_copies(c):
                    cp.start()
            y[pl.ds(0, 8 * B), :] = jnp.zeros((8 * B, B), F32)
            act_copy().wait_recv()

        mlp(i)
        for n in range(8):
            resid[slot, :, pl.ds(n * 256, 256)] = y[pl.ds(n * B, B), :].astype(BF16)

        @pl.when(shared)
        def _():
            act_copy().wait_send()
            sum_copy().wait_recv()
            for n in range(8):
                h = y[pl.ds(n * B, B), :] + y[pl.ds((n + 8) * B, B), :]
                resid[slot, :, pl.ds(n * 256, 256)] = h.astype(BF16)

        @pl.when(jnp.logical_not(main))
        def _():
            sum_copy().start()
            sum_copy().wait_send()

        @pl.when(main)
        def _():
            @pl.when(jnp.logical_not(last) & (i >= NS))
            def _():
                pl.semaphore_wait(credit, 1)

            @pl.when(jnp.logical_not(last))
            def _():
                next_copy(i).start()

            for r in range(PER):
                remote, local, mine = piece_copy(i, r)

                @pl.when(last & jnp.logical_not(mine))
                def _():
                    remote.start()

                @pl.when(last & mine)
                def _():
                    local.start()

            @pl.when(jnp.logical_not(helper) & (i >= 1) & (i <= R))
            def _():
                for cp in lend_copies(i - 1):
                    cp.wait_send()

            @pl.when(jnp.logical_not(helper) & (i < R))
            def _():
                for cp in lend_copies(i):
                    cp.start()

        return 0

    lax.fori_loop(0, NB + jnp.where(helper, 1, 0), block, 0)

    @pl.when(jnp.logical_not(last))
    def _():
        next_copy(NB - 1).wait_send()

    for row in range(3):
        piece_copy(row // PER, row % PER)[1].wait()

def place_kernel(hid, k_t, v_t, hid_out, k_out, v_out, hid_v, k_v, v_v, in_sem, out_sem):
    halves = []
    for n, (src, buf, dst) in enumerate(((hid, hid_v, hid_out), (k_t, k_v, k_out), (v_t, v_v, v_out))):
        rows = src.shape[0] // 2
        for half in range(2):
            part = pl.ds(half * rows, rows)
            halves.append((pltpu.make_async_copy(src.at[part], buf.at[part], in_sem.at[n, half]),
                           pltpu.make_async_copy(buf.at[part], dst.at[part], out_sem.at[n, half])))
    for load, _ in halves:
        load.start()
    for load, store in halves:
        load.wait()
        store.start()
    for _, store in halves:
        store.wait()


def solution(mesh):
    gain_spec = P('stage', None)
    spec_three = P('stage', None, None)
    spec_four = P('stage', None, None, None)
    table = rope_tables()
    dma = pltpu.SemaphoreType.DMA

    def stage_program(embeddings, valid_len, attn_gain, w_q, w_k, w_v, w_o, mlp_gain, w_gate, w_up, w_down):
        wq = w_q[0].transpose(1, 2, 0).reshape(HEADS * HD, D)
        wk = w_k[0].transpose(1, 2, 0).reshape(KV * HD, D)
        wv = w_v[0].transpose(1, 2, 0).reshape(KV * HD, D)
        wo = w_o[0].reshape(HEADS * HD, D)
        any_spec = pl.BlockSpec(memory_space=pl.ANY)
        vmem_spec = pl.BlockSpec(memory_space=pltpu.VMEM)
        smem_spec = pl.BlockSpec(memory_space=pltpu.SMEM)
        hid, k_t, v_t, _, _, _ = pl.pallas_call(
            stage_kernel,
            name="stage_pipeline",
            out_shape=(jax.ShapeDtypeStruct((SEQ // STAGES, D), BF16),
                       jax.ShapeDtypeStruct((KV * HD, SEQ), BF16),
                       jax.ShapeDtypeStruct((KV * HD, SEQ), BF16),
                       jax.ShapeDtypeStruct((D, LENT), BF16),
                       jax.ShapeDtypeStruct((D, LENT), BF16),
                       jax.ShapeDtypeStruct((LENT, D), BF16)),
            in_specs=[any_spec, smem_spec, any_spec, any_spec, any_spec, any_spec, any_spec, any_spec,
                      any_spec, any_spec, any_spec, any_spec],
            out_specs=(any_spec,) * 6,
            scratch_shapes=[
                pltpu.VMEM((NB, 2, HD // 2, 256), F32),
                pltpu.VMEM((1, D), F32),
                pltpu.VMEM((1, D), F32),
                pltpu.VMEM((3072, D), BF16),
                pltpu.VMEM((D, D), BF16),
                [pltpu.VMEM((D, F), BF16)] * R,
                [pltpu.VMEM((D, F), BF16)] * R,
                [pltpu.VMEM((F, D), BF16)] * R,
                pltpu.VMEM((NS, B, D), BF16),
                pltpu.VMEM((SEQ, KV * HD), BF16),
                pltpu.VMEM((KV * HD, SEQ), BF16),
                pltpu.VMEM((256, D), BF16),
                pltpu.VMEM((KV, 2 * HD, 4 * B), BF16),
                pltpu.VMEM((SB * VMAX, B), F32),
                pltpu.VMEM((SB, 8, B), F32),
                [pltpu.VMEM((B, F), BF16)] * 2,
                pltpu.VMEM((B // 2, B + B // 2), F32),
                pltpu.VMEM((VMAX - VMIN, 128), F32),
                pltpu.VMEM((B, 128), BF16),
                pltpu.VMEM((128, B), BF16),
                dma((10,)), dma((3,)), dma((R,)), dma((R,)), dma((R,)), dma((NS,)), dma((NS,)), dma((3,)), dma((NS, PER)), dma((3,)),
                dma((3,)), dma((3, R)), dma((4,)),
                pltpu.SemaphoreType.REGULAR,
            ],
            compiler_params=pltpu.CompilerParams(collective_id=0, has_side_effects=True,
                                                 vmem_limit_bytes=67043328),
        )(embeddings, valid_len, attn_gain, wq, wk, wv, wo, mlp_gain, w_gate[0], w_up[0], w_down[0],
          jnp.asarray(table))

        hid, k_t, v_t = pl.pallas_call(
            place_kernel,
            name="place",
            out_shape=tuple(jax.ShapeDtypeStruct(x.shape, BF16) for x in (hid, k_t, v_t)),
            in_specs=[any_spec] * 3,
            out_specs=(any_spec,) * 3,
            scratch_shapes=[pltpu.VMEM(x.shape, BF16) for x in (hid, k_t, v_t)] + [dma((3, 2)), dma((3, 2))],
            compiler_params=pltpu.CompilerParams(vmem_limit_bytes=67043328),
        )(hid, k_t, v_t)

        def to_cache(x):
            return x.reshape(KV, HD, SEQ).transpose(2, 0, 1)[None]

        return hid, to_cache(k_t), to_cache(v_t)

    return jax.shard_map(stage_program, mesh=mesh,
                         in_specs=(P('replica', None), P('replica'), gain_spec, spec_four, spec_four, spec_four, spec_four,
                                   gain_spec, spec_three, spec_three, spec_three),
                         out_specs=(P(('replica', 'stage'), None), P('stage', 'replica', None, None), P('stage', 'replica', None, None)),
                         check_vma=False)
```

```python
import math

import jax
import jax.numpy as jnp
import numpy as np
from jax import lax
from jax.experimental import pallas as pl
from jax.experimental.pallas import tpu as pltpu
from jax.sharding import PartitionSpec as P

EPS = 1e-5
ROPE_BASE = 10000.0
NEG = -1e30

SEQ = 1536
D = 2048
HEADS = 32
KV = 8
HD = 64
FF = 8192
STAGES = 4
B = 256
NB = SEQ // B
F = 512
NC = FF // F
NS = 3
VMIN = 768
VMAX = 1344
PIECE = SEQ // STAGES // 3
PER = B // PIECE
R = 4
LEND_AT = (NC - R + (NC - R) * (NB - 1)) % NC * F
LENT = R * F
SB = 4
EXP_SCALE = math.log2(math.e)

F32 = jnp.float32
BF16 = jnp.bfloat16


def rope_tables():
    inv_freq = ROPE_BASE ** (-np.arange(HD // 2, dtype=np.float64) * (2.0 / HD))
    angles = inv_freq[:, None] * np.arange(SEQ, dtype=np.float64)[None, :]
    tab = np.zeros((NB, 2, HD // 2, 256), np.float32)
    for blk in range(NB):
        cols = slice(blk * B, (blk + 1) * B)
        tab[blk, 0, :, :B] = np.cos(angles[:, cols])
        tab[blk, 1, :, :B] = np.sin(angles[:, cols])
    return tab


def dot(a, b):
    return jnp.dot(a, b, preferred_element_type=F32)


def dot_t(a, b):
    return lax.dot_general(a, b, (((1,), (1,)), ((), ())), preferred_element_type=F32)


def stage_kernel(emb, valid, again_hbm, wq, wk, wv, wo, mgain_hbm, wg, wu, wd, tab_hbm,
                 hid, kout, vout, wg_x, wu_x, wd_x,
                 tab, again, mgain, wqkv_v, wo_v, wg_s, wu_s, wd_s, resid, kc, vT, act, qT, y, mbuf, ff_s,
                 mask, vbias, kbias, qones,
                 w_sem, tab_sem, g_sem, u_sem, d_sem, in_sem, send_sem, kv_sem, piece_sem, out_sem, lend_sem, borrow_sem, pair_sem,
                 credit):
    stage = lax.axis_index("stage")
    helper = lax.rem(stage, 2) == 0
    partner = stage + 1 - 2 * lax.rem(stage, 2)
    barrier = pltpu.get_barrier_semaphore()
    for k in range(1, STAGES):
        pl.semaphore_signal(barrier, inc=1, device_id={"stage": lax.rem(stage + k, STAGES)},
                            device_id_type=pl.DeviceIdType.MESH)

    def emb_copy(i):
        return pltpu.make_async_copy(emb.at[pl.ds(pl.multiple_of(i * B, B), B), :], resid.at[lax.rem(i, NS)], in_sem.at[lax.rem(i, NS)])

    def w_copy(p):
        if p < 4:
            src = wq.at[pl.ds(p * 512, 512), :]
        elif p == 4:
            src = wk
        elif p == 5:
            src = wv
        else:
            src = wo.at[pl.ds((p - 6) * 512, 512), :]
        dst = wqkv_v.at[pl.ds(p * 512, 512), :] if p < 6 else wo_v.at[pl.ds((p - 6) * 512, 512), :]
        return pltpu.make_async_copy(src, dst, w_sem.at[p])

    def gu_copy(c, s):
        cols = pl.ds(pl.multiple_of(c * F, F), F)
        return (pltpu.make_async_copy(wg.at[:, cols], wg_s[s], g_sem.at[s]),
                pltpu.make_async_copy(wu.at[:, cols], wu_s[s], u_sem.at[s]))

    def dn_copy(c, s):
        rows = pl.ds(pl.multiple_of(c * F, F), F)
        return pltpu.make_async_copy(wd.at[rows, :], wd_s[s], d_sem.at[s])

    small_copies = [pltpu.make_async_copy(src, dst, tab_sem.at[n])
                    for n, (src, dst) in enumerate(((again_hbm, again), (mgain_hbm, mgain), (tab_hbm, tab)))]

    @pl.when(stage == 0)
    def _():
        emb_copy(0).start()

    for cp in small_copies:
        cp.start()
    for p in range(6):
        w_copy(p).start()

    for g in range(KV):
        qT[g, pl.ds((1 - g % 2) * HD, HD), :] = jnp.zeros((HD, 4 * B), BF16)
    valid_pos = valid[0]
    row = lax.broadcasted_iota(jnp.int32, vbias.shape, 0) + VMIN
    vbias[...] = jnp.where(row < valid_pos, 0.0, NEG).astype(F32)
    row = lax.broadcasted_iota(jnp.int32, kbias.shape, 0) + VMIN
    lane = lax.broadcasted_iota(jnp.int32, kbias.shape, 1)
    kbias[...] = jnp.where((lane == 0) & (row >= valid_pos), NEG, 0.0).astype(BF16)
    row = lax.broadcasted_iota(jnp.int32, qones.shape, 0)
    qones[...] = jnp.where(row == 0, 1.0, 0.0).astype(BF16)

    def norm(slot, gain_ref):
        for r in range(0, B, 16):
            x = resid[slot, pl.ds(r, 16), :].astype(F32)
            inv = lax.rsqrt(jnp.mean(x * x, axis=-1, keepdims=True) + EPS)
            act[pl.ds(r, 16), :] = (x * inv * gain_ref[...]).astype(BF16)

    def rope(x, cos, sin):
        front = x[:HD // 2]
        back = x[HD // 2:]
        return front * cos - back * sin, back * cos + front * sin

    def project(i):
        cos = tab[i, 0]
        sin = tab[i, 1]

        kt = dot_t(wqkv_v[pl.ds(2048, 512), :], act[...])
        parts = []
        for h in range(KV):
            parts += list(rope(kt[h * HD:(h + 1) * HD], cos, sin))
        for half in range(2):
            kh = jnp.concatenate(parts[half * 8:half * 8 + 8], axis=0).astype(BF16)
            ff_s[1][:, pl.ds(half * 256, 256)] = kh
            kc[pl.ds(pl.multiple_of(i * B, B), B), pl.ds(half * 256, 256)] = kh.T
        vt = dot_t(wqkv_v[pl.ds(2560, 512), :], act[...])
        vT[:, pl.ds(pl.multiple_of(i * B, B), B)] = vt.astype(BF16)

        for pair in range(4):
            qt = dot_t(wqkv_v[pl.ds(pair * 512, 512), :], act[...])
            for h in range(8):
                f, b = rope(qt[h * HD:(h + 1) * HD], cos, sin)
                g = pair * 2 + h // 4
                row = (g % 2) * HD
                cols = pl.ds((h % 4) * B, B)
                qT[g, pl.ds(row, HD // 2), cols] = (f * 0.125).astype(BF16)
                qT[g, pl.ds(row + HD // 2, HD // 2), cols] = (b * 0.125).astype(BF16)

    def make_mask(i):
        key = lax.broadcasted_iota(jnp.int32, mask.shape, 0)
        tok = lax.broadcasted_iota(jnp.int32, mask.shape, 1)
        key = jnp.where(tok < B, key, key + B // 2)
        tok = jnp.where(tok < B, tok, tok - B // 2)
        ok = (key <= tok) & (key + i * B < valid_pos)
        mask[...] = jnp.where(ok, 0.0, NEG).astype(F32)

    def attend(n):
        spans = [(c * B, min(B, VMAX - c * B), 0) for c in range(n + 1)]
        if spans[-1][1] == B:
            spans[-1:] = [(n * B, B // 2, 0), (n * B + B // 2, B // 2, B // 2)]
        total = spans[-1][0] + spans[-1][1]
        ahead_by = 1 if n == NB - 2 else 2

        def scores(g, u):
            kcols = pl.ds(pl.multiple_of((g // 2) * 128, 128), 128)
            q = qT[g, :, pl.ds((u % 4) * B, B)]
            m = None
            for start, rows, lane in spans:
                keys = kc[pl.ds(start, rows), kcols]
                if start >= n * B:
                    s = dot(keys, q[:, lane:]) + mask[pl.ds(0, rows), pl.ds(2 * lane, B - lane)]
                elif start >= VMIN and n == NB - 1:
                    bias = vbias[pl.ds(start - VMIN, rows), :]
                    s = dot(keys, q) + jnp.concatenate([bias, bias], axis=1)
                elif start >= VMIN:
                    bias = kbias[pl.ds(start - VMIN, rows), :]
                    s = dot(jnp.concatenate([keys, bias], axis=1), jnp.concatenate([q, qones[...]], axis=0))
                else:
                    s = dot(keys, q)
                y[pl.ds((u % SB) * total + start, rows), pl.ds(lane, B - lane)] = s
                cm = jnp.max(s.reshape(rows // 8, 8, B - lane), axis=0)
                if lane:
                    m = jnp.concatenate([m[:, :lane], jnp.maximum(m[:, lane:], cm)], axis=1)
                else:
                    m = cm if m is None else jnp.maximum(m, cm)
            mbuf[u % SB] = m

        def weighted(g, u):
            mc = jnp.max(mbuf[u % SB], axis=0, keepdims=True) * EXP_SCALE
            l = None
            probs = []
            for start, rows, lane in spans:
                sc = y[pl.ds((u % SB) * total + start, rows), pl.ds(lane, B - lane)]
                p = jnp.exp2(sc * EXP_SCALE - mc[:, lane:])
                ls = jnp.sum(p.reshape(rows // 8, 8, B - lane), axis=0)
                p = p.astype(BF16)
                if lane:
                    l = jnp.concatenate([l[:, :lane], l[:, lane:] + ls], axis=1)
                    p = jnp.concatenate([jnp.zeros((rows, lane), BF16), p], axis=1)
                else:
                    l = ls if l is None else l + ls
                probs.append(p)
            o = dot(vT[pl.ds(pl.multiple_of(g * HD, HD), HD), pl.ds(0, total)], jnp.concatenate(probs, axis=0))
            return (o * (1.0 / jnp.sum(l, axis=0, keepdims=True))).astype(BF16)

        def put_out(g):
            act[:, pl.ds(pl.multiple_of(g * 256, 256), 256)] = ff_s[0][:, pl.ds(0, 256)].T

        for u in range(ahead_by):
            scores(0, u)

        def group_pair(pair, _):
            g = pair * 2
            outs = []
            for u in range(8):
                ahead = u + ahead_by
                scores(g + ahead // 4 if ahead < 8 else lax.rem(g + 2, KV), ahead)
                outs.append(weighted(g + u // 4, u))
                if u == 0:
                    put_out(lax.rem(g + KV - 1, KV))
                if u == 3:
                    act[:, pl.ds(pl.multiple_of(g * 256, 256), 256)] = jnp.concatenate(outs, axis=0).T
                    outs = []
            for h in range(4):
                ff_s[0][pl.ds(h * HD, HD), pl.ds(0, 256)] = outs[h]
            return 0

        lax.fori_loop(0, KV // 2, group_pair, 0)
        put_out(KV - 1)

    def out_proj(slot):
        for n in range(4):
            cols = pl.ds(n * 512, 512)
            o = dot(act[pl.ds(0, B), :], wo_v[:, cols])
            resid[slot, :, cols] = (resid[slot, :, cols].astype(F32) + o).astype(BF16)

    def lend_copies(c):
        sem = lend_sem
        cols = pl.ds(pl.multiple_of(LEND_AT + c * F, F), F)
        rows = pl.ds(pl.multiple_of(c * F, F), F)
        return [pltpu.make_async_remote_copy(src, dst, sem.at[n], borrow_sem.at[n, c], device_id={"stage": partner},
                                             device_id_type=pl.DeviceIdType.MESH)
                for n, (src, dst) in enumerate(((wg.at[:, cols], wg_x.at[:, rows]), (wu.at[:, cols], wu_x.at[:, rows]),
                                                (wd.at[cols, :], wd_x.at[rows, :])))]

    def borrowed_copies(c):
        part = pl.ds(c * F, F)
        return (pltpu.make_async_copy(wg_x.at[:, part], wg_s[c], g_sem.at[c]),
                pltpu.make_async_copy(wu_x.at[:, part], wu_s[c], u_sem.at[c]),
                pltpu.make_async_copy(wd_x.at[part, :], wd_s[c], d_sem.at[c]))

    def pair_copy(src, dst, n):
        return pltpu.make_async_remote_copy(src, dst, pair_sem.at[2 * n], pair_sem.at[2 * n + 1],
                                            device_id={"stage": partner}, device_id_type=pl.DeviceIdType.MESH)

    def act_copy():
        return pair_copy(act, act, 0)

    def sum_copy():
        return pair_copy(y.at[pl.ds(0, 8 * B), :], y.at[pl.ds(8 * B, 8 * B), :], 1)

    def gate_up(s, first=0, rows=B):
        x = act[pl.ds(first, rows), :]
        gate = dot(x, wg_s[s][...])
        up = dot(x, wu_s[s][...])
        ff_s[s % 2][pl.ds(first, rows), :] = (gate * jax.nn.sigmoid(gate) * up).astype(BF16)

    def down(s, first=0, rows=B):
        x = ff_s[s % 2][pl.ds(first, rows), :]
        for n in range(8):
            part = pl.ds(n * B + first, rows)
            y[part, :] = y[part, :] + dot(x, wd_s[s][:, pl.ds(n * 256, 256)])

    def wait_gu(s):
        for cp in gu_copy(0, s):
            cp.wait()

    def wait_dn(s):
        dn_copy(0, s).wait()

    def start_gu(c, s, ok):
        @pl.when(ok)
        def _():
            for cp in gu_copy(lax.rem(c, NC), s):
                cp.start()

    def start_dn(c, s, ok):
        @pl.when(ok)
        def _():
            dn_copy(lax.rem(c, NC), s).start()

    def mlp(i, half_done):
        shared = (i == NB - 1) & jnp.logical_not(helper)
        mine = jnp.where(shared, NC - R, NC)

        def fetch(start, idx, slot):
            start(idx + (NC - R) * i, slot, (i < NB) & (idx < mine))

        @pl.when((i == 0) | (i == NB))
        def _():
            wait_gu(0)

        gate_up(0)
        fetch(start_gu, R, 0)

        def steps(it, _):
            c = it * R
            for u in range(R):
                if u % 2 == 0:
                    @pl.when((i == 0) | (it > 0))
                    def _():
                        wait_gu(u + 1)
                        wait_dn(u)
                        wait_dn(u + 1)
                        if u + 2 < R:
                            wait_gu(u + 2)

                    if u + 2 == R:
                        wait_gu(0)
                gate_up((u + 1) % R)
                fetch(start_gu, c + u + 1 + R, (u + 1) % R)
                down(u)
                fetch(start_dn, c + u + R, u)
            return 0

        lax.fori_loop(0, jnp.where(i < NB, jnp.where(shared, NC // R - 2, NC // R - 1), 0), steps, 0)
        for half in range(2):
            for u in range(R):
                if u % 2 == 0 and half == 0:
                    wait_gu(u + 1)
                    if u + 2 < R:
                        wait_gu(u + 2)
                    wait_dn(u)
                    wait_dn(u + 1)
                if u + 1 < R:
                    gate_up(u + 1, half * PIECE, PIECE)
                down(u, half * PIECE, PIECE)
            half_done(half)

    def next_copy(i, r):
        slot = lax.rem(i, NS)
        part = resid.at[slot, pl.ds(r * PIECE, PIECE), :]
        return pltpu.make_async_remote_copy(part, part, send_sem.at[slot, r], in_sem.at[slot],
                                            device_id={"stage": lax.rem(stage + 1, STAGES)},
                                            device_id_type=pl.DeviceIdType.MESH)

    def piece_copy(i, r):
        slot = lax.rem(i, NS)
        piece = i * PER + r
        row = lax.rem(piece, 3)
        src = resid.at[slot, pl.ds(r * PIECE, PIECE), :]
        dst = hid.at[pl.ds(pl.multiple_of(row * PIECE, PIECE), PIECE), :]
        remote = pltpu.make_async_remote_copy(src, dst, piece_sem.at[slot, r], out_sem.at[row],
                                              device_id={"stage": piece // 3}, device_id_type=pl.DeviceIdType.MESH)
        return remote, pltpu.make_async_copy(src, dst, out_sem.at[row]), piece // 3 == STAGES - 1

    def k_copy(i, half):
        cols = pl.ds(pl.multiple_of(i * B, B), B)
        return pltpu.make_async_copy(ff_s[1].at[:, pl.ds(half * 256, 256)], kout.at[pl.ds(half * 256, 256), cols],
                                     kv_sem.at[half])

    def v_copy(i):
        cols = pl.ds(pl.multiple_of(i * B, B), B)
        return pltpu.make_async_copy(vT.at[:, cols], vout.at[:, cols], kv_sem.at[2])

    last = stage == STAGES - 1

    def block(i, _):
        slot = lax.rem(i, NS)
        main = i < NB
        shared = (i == NB - 1) & jnp.logical_not(helper)

        @pl.when(main)
        def _():
            emb_copy(i).wait()

            @pl.when(i == 0)
            def _():
                for cp in small_copies:
                    cp.wait()

            norm(slot, again)

            @pl.when(i == 0)
            def _():
                for p in range(6):
                    w_copy(p).wait()
                for p in range(6, 10):
                    w_copy(p).start()
                for c in range(2):
                    start_gu(c, c, True)
                    start_dn(c, c, True)

            project(i)

            @pl.when(i == 0)
            def _():
                for c in range(2, R):
                    start_gu(c, c, True)
                    start_dn(c, c, True)
                pl.semaphore_wait(barrier, STAGES - 1)

            make_mask(i)
            k_copy(i, 0).start()
            k_copy(i, 1).start()
            v_copy(i).start()

        for n in range(NB):
            @pl.when(i == n)
            def _():
                attend(n)

        @pl.when(main)
        def _():
            @pl.when((i >= 1) & jnp.logical_not(last))
            def _():
                for r in range(PER):
                    next_copy(i - 1, r).wait_send()

            for r in range(PER):
                remote, local, mine = piece_copy(i - 1, r)

                @pl.when((i >= 1) & last & jnp.logical_not(mine))
                def _():
                    remote.wait_send()

            @pl.when((stage > 0) & (i >= 1) & (i - 1 + NS < NB))
            def _():
                pl.semaphore_signal(credit, inc=1, device_id={"stage": lax.rem(stage + STAGES - 1, STAGES)},
                                    device_id_type=pl.DeviceIdType.MESH)

            @pl.when((stage == 0) & (i + 1 < NB))
            def _():
                emb_copy(i + 1).start()

            @pl.when(i == 0)
            def _():
                for p in range(6, 10):
                    w_copy(p).wait()

            @pl.when(jnp.logical_not(last) & (i >= NS))
            def _():
                pl.semaphore_wait(credit, 1)

            k_copy(i, 0).wait()
            k_copy(i, 1).wait()
            v_copy(i).wait()
            out_proj(slot)
            norm(slot, mgain)
            for n in range(8):
                y[pl.ds(n * B, B), :] = resid[slot, :, pl.ds(n * 256, 256)].astype(F32)

            @pl.when(shared)
            def _():
                act_copy().start()

        @pl.when(jnp.logical_not(main))
        def _():
            for c in range(R):
                for cp in lend_copies(c):
                    cp.wait_recv()
                for cp in borrowed_copies(c):
                    cp.start()
            y[pl.ds(0, 8 * B), :] = jnp.zeros((8 * B, B), F32)
            act_copy().wait_recv()

        def send(r, ok):
            remote, local, mine = piece_copy(i, r)

            @pl.when(ok & jnp.logical_not(last))
            def _():
                next_copy(i, r).start()

            @pl.when(ok & last & jnp.logical_not(mine))
            def _():
                remote.start()

            @pl.when(ok & last & mine)
            def _():
                local.start()

        def half_done(half):
            for n in range(8):
                resid[slot, pl.ds(half * PIECE, PIECE), pl.ds(n * 256, 256)] = \
                    y[pl.ds(n * B + half * PIECE, PIECE), :].astype(BF16)
            send(half, main & jnp.logical_not(shared))

        mlp(i, half_done)

        @pl.when(shared)
        def _():
            act_copy().wait_send()
            sum_copy().wait_recv()
            for n in range(8):
                h = y[pl.ds(n * B, B), :] + y[pl.ds((n + 8) * B, B), :]
                resid[slot, :, pl.ds(n * 256, 256)] = h.astype(BF16)

        for r in range(PER):
            send(r, shared)

        @pl.when(jnp.logical_not(main))
        def _():
            sum_copy().start()
            sum_copy().wait_send()

        @pl.when(main)
        def _():
            @pl.when(jnp.logical_not(helper) & (i >= 1) & (i <= R))
            def _():
                for cp in lend_copies(i - 1):
                    cp.wait_send()

            @pl.when(jnp.logical_not(helper) & (i < R))
            def _():
                for cp in lend_copies(i):
                    cp.start()

        return 0

    lax.fori_loop(0, NB + jnp.where(helper, 1, 0), block, 0)

    @pl.when(jnp.logical_not(last))
    def _():
        for r in range(PER):
            next_copy(NB - 1, r).wait_send()

    for row in range(3):
        piece_copy(row // PER, row % PER)[1].wait()

def place_kernel(hid, k_t, v_t, hid_out, k_out, v_out, hid_v, k_v, v_v, in_sem, out_sem):
    halves = []
    for n, (src, buf, dst) in enumerate(((hid, hid_v, hid_out), (k_t, k_v, k_out), (v_t, v_v, v_out))):
        rows = src.shape[0] // 2
        for half in range(2):
            part = pl.ds(half * rows, rows)
            halves.append((pltpu.make_async_copy(src.at[part], buf.at[part], in_sem.at[n, half]),
                           pltpu.make_async_copy(buf.at[part], dst.at[part], out_sem.at[n, half])))
    for load, _ in halves:
        load.start()
    for load, store in halves:
        load.wait()
        store.start()
    for _, store in halves:
        store.wait()


def solution(mesh):
    gain_spec = P('stage', None)
    spec_three = P('stage', None, None)
    spec_four = P('stage', None, None, None)
    table = rope_tables()
    dma = pltpu.SemaphoreType.DMA

    def stage_program(embeddings, valid_len, attn_gain, w_q, w_k, w_v, w_o, mlp_gain, w_gate, w_up, w_down):
        wq = w_q[0].transpose(1, 2, 0).reshape(HEADS * HD, D)
        wk = w_k[0].transpose(1, 2, 0).reshape(KV * HD, D)
        wv = w_v[0].transpose(1, 2, 0).reshape(KV * HD, D)
        wo = w_o[0].reshape(HEADS * HD, D)
        any_spec = pl.BlockSpec(memory_space=pl.ANY)
        vmem_spec = pl.BlockSpec(memory_space=pltpu.VMEM)
        smem_spec = pl.BlockSpec(memory_space=pltpu.SMEM)
        hid, k_t, v_t, _, _, _ = pl.pallas_call(
            stage_kernel,
            name="stage_pipeline",
            out_shape=(jax.ShapeDtypeStruct((SEQ // STAGES, D), BF16),
                       jax.ShapeDtypeStruct((KV * HD, SEQ), BF16),
                       jax.ShapeDtypeStruct((KV * HD, SEQ), BF16),
                       jax.ShapeDtypeStruct((D, LENT), BF16),
                       jax.ShapeDtypeStruct((D, LENT), BF16),
                       jax.ShapeDtypeStruct((LENT, D), BF16)),
            in_specs=[any_spec, smem_spec, any_spec, any_spec, any_spec, any_spec, any_spec, any_spec,
                      any_spec, any_spec, any_spec, any_spec],
            out_specs=(any_spec,) * 6,
            scratch_shapes=[
                pltpu.VMEM((NB, 2, HD // 2, 256), F32),
                pltpu.VMEM((1, D), F32),
                pltpu.VMEM((1, D), F32),
                pltpu.VMEM((3072, D), BF16),
                pltpu.VMEM((D, D), BF16),
                [pltpu.VMEM((D, F), BF16)] * R,
                [pltpu.VMEM((D, F), BF16)] * R,
                [pltpu.VMEM((F, D), BF16)] * R,
                pltpu.VMEM((NS, B, D), BF16),
                pltpu.VMEM((SEQ, KV * HD), BF16),
                pltpu.VMEM((KV * HD, SEQ), BF16),
                pltpu.VMEM((256, D), BF16),
                pltpu.VMEM((KV, 2 * HD, 4 * B), BF16),
                pltpu.VMEM((SB * VMAX, B), F32),
                pltpu.VMEM((SB, 8, B), F32),
                [pltpu.VMEM((B, F), BF16)] * 2,
                pltpu.VMEM((B // 2, B + B // 2), F32),
                pltpu.VMEM((VMAX - VMIN, 128), F32),
                pltpu.VMEM((B, 128), BF16),
                pltpu.VMEM((128, B), BF16),
                dma((10,)), dma((3,)), dma((R,)), dma((R,)), dma((R,)), dma((NS,)), dma((NS, PER)), dma((3,)), dma((NS, PER)), dma((3,)),
                dma((3,)), dma((3, R)), dma((4,)),
                pltpu.SemaphoreType.REGULAR,
            ],
            compiler_params=pltpu.CompilerParams(collective_id=0, has_side_effects=True,
                                                 vmem_limit_bytes=67043328),
        )(embeddings, valid_len, attn_gain, wq, wk, wv, wo, mlp_gain, w_gate[0], w_up[0], w_down[0],
          jnp.asarray(table))

        hid, k_t, v_t = pl.pallas_call(
            place_kernel,
            name="place",
            out_shape=tuple(jax.ShapeDtypeStruct(x.shape, BF16) for x in (hid, k_t, v_t)),
            in_specs=[any_spec] * 3,
            out_specs=(any_spec,) * 3,
            scratch_shapes=[pltpu.VMEM(x.shape, BF16) for x in (hid, k_t, v_t)] + [dma((3, 2)), dma((3, 2))],
            compiler_params=pltpu.CompilerParams(vmem_limit_bytes=67043328),
        )(hid, k_t, v_t)

        def to_cache(x):
            return x.reshape(KV, HD, SEQ).transpose(2, 0, 1)[None]

        return hid, to_cache(k_t), to_cache(v_t)

    return jax.shard_map(stage_program, mesh=mesh,
                         in_specs=(P('replica', None), P('replica'), gain_spec, spec_four, spec_four, spec_four, spec_four,
                                   gain_spec, spec_three, spec_three, spec_three),
                         out_specs=(P(('replica', 'stage'), None), P('stage', 'replica', None, None), P('stage', 'replica', None, None)),
                         check_vma=False)
```

```python
import math

import jax
import jax.numpy as jnp
import numpy as np
from jax import lax
from jax.experimental import pallas as pl
from jax.experimental.pallas import tpu as pltpu
from jax.sharding import PartitionSpec as P

EPS = 1e-5
ROPE_BASE = 10000.0
NEG = -1e30

SEQ = 1536
D = 2048
HEADS = 32
KV = 8
HD = 64
FF = 8192
STAGES = 4
B = 256
NB = SEQ // B
F = 512
NC = FF // F
NS = 3
VMIN = 768
VMAX = 1344
PIECE = SEQ // STAGES // 3
PER = B // PIECE
R = 4
LEND_AT = (NC - R + (NC - R) * (NB - 1)) % NC * F
LENT = R * F
SB = 4
EXP_SCALE = math.log2(math.e)

F32 = jnp.float32
BF16 = jnp.bfloat16


def rope_tables():
    inv_freq = ROPE_BASE ** (-np.arange(HD // 2, dtype=np.float64) * (2.0 / HD))
    angles = inv_freq[:, None] * np.arange(SEQ, dtype=np.float64)[None, :]
    tab = np.zeros((NB, 2, HD // 2, 256), np.float32)
    for blk in range(NB):
        cols = slice(blk * B, (blk + 1) * B)
        tab[blk, 0, :, :B] = np.cos(angles[:, cols])
        tab[blk, 1, :, :B] = np.sin(angles[:, cols])
    return tab


def dot(a, b):
    return jnp.dot(a, b, preferred_element_type=F32)


def dot_t(a, b):
    return lax.dot_general(a, b, (((1,), (1,)), ((), ())), preferred_element_type=F32)


def stage_kernel(emb, valid, again_hbm, wq, wk, wv, wo, mgain_hbm, wg, wu, wd, tab_hbm,
                 hid, kout, vout, wg_x, wu_x, wd_x,
                 tab, again, mgain, wqkv_v, wo_v, wg_s, wu_s, wd_s, resid, kc, vT, act, qT, y, mbuf, ff_s,
                 mask, vbias, kbias, qones,
                 w_sem, tab_sem, g_sem, u_sem, d_sem, in_sem, send_sem, kv_sem, piece_sem, out_sem, lend_sem, borrow_sem, pair_sem,
                 credit):
    stage = lax.axis_index("stage")
    helper = lax.rem(stage, 2) == 0
    partner = stage + 1 - 2 * lax.rem(stage, 2)
    barrier = pltpu.get_barrier_semaphore()
    for k in range(1, STAGES):
        pl.semaphore_signal(barrier, inc=1, device_id={"stage": lax.rem(stage + k, STAGES)},
                            device_id_type=pl.DeviceIdType.MESH)

    def emb_copy(i):
        return pltpu.make_async_copy(emb.at[pl.ds(pl.multiple_of(i * B, B), B), :], resid.at[lax.rem(i, NS)], in_sem.at[lax.rem(i, NS)])

    def w_copy(p):
        if p < 4:
            src = wq.at[pl.ds(p * 512, 512), :]
        elif p == 4:
            src = wk
        elif p == 5:
            src = wv
        else:
            src = wo.at[pl.ds((p - 6) * 512, 512), :]
        dst = wqkv_v.at[pl.ds(p * 512, 512), :] if p < 6 else wo_v.at[pl.ds((p - 6) * 512, 512), :]
        return pltpu.make_async_copy(src, dst, w_sem.at[p])

    def gu_copy(c, s):
        cols = pl.ds(pl.multiple_of(c * F, F), F)
        return (pltpu.make_async_copy(wg.at[:, cols], wg_s[s], g_sem.at[s]),
                pltpu.make_async_copy(wu.at[:, cols], wu_s[s], u_sem.at[s]))

    def dn_copy(c, s):
        rows = pl.ds(pl.multiple_of(c * F, F), F)
        return pltpu.make_async_copy(wd.at[rows, :], wd_s[s], d_sem.at[s])

    small_copies = [pltpu.make_async_copy(src, dst, tab_sem.at[n])
                    for n, (src, dst) in enumerate(((again_hbm, again), (mgain_hbm, mgain), (tab_hbm, tab)))]

    @pl.when(stage == 0)
    def _():
        emb_copy(0).start()

    for cp in small_copies:
        cp.start()
    for p in range(6):
        w_copy(p).start()

    for g in range(KV):
        qT[g, pl.ds((1 - g % 2) * HD, HD), :] = jnp.zeros((HD, 4 * B), BF16)
    valid_pos = valid[0]
    row = lax.broadcasted_iota(jnp.int32, vbias.shape, 0) + VMIN
    vbias[...] = jnp.where(row < valid_pos, 0.0, NEG).astype(F32)
    row = lax.broadcasted_iota(jnp.int32, kbias.shape, 0) + VMIN
    lane = lax.broadcasted_iota(jnp.int32, kbias.shape, 1)
    kbias[...] = jnp.where((lane == 0) & (row >= valid_pos), NEG, 0.0).astype(BF16)
    row = lax.broadcasted_iota(jnp.int32, qones.shape, 0)
    qones[...] = jnp.where(row == 0, 1.0, 0.0).astype(BF16)

    def norm(slot, gain_ref):
        for r in range(0, B, 16):
            x = resid[slot, pl.ds(r, 16), :].astype(F32)
            inv = lax.rsqrt(jnp.mean(x * x, axis=-1, keepdims=True) + EPS)
            act[pl.ds(r, 16), :] = (x * inv * gain_ref[...]).astype(BF16)

    def rope(x, cos, sin):
        front = x[:HD // 2]
        back = x[HD // 2:]
        return front * cos - back * sin, back * cos + front * sin

    def project(i):
        cos = tab[i, 0]
        sin = tab[i, 1]

        kt = dot_t(wqkv_v[pl.ds(2048, 512), :], act[...])
        parts = []
        for h in range(KV):
            parts += list(rope(kt[h * HD:(h + 1) * HD], cos, sin))
        for half in range(2):
            kh = jnp.concatenate(parts[half * 8:half * 8 + 8], axis=0).astype(BF16)
            ff_s[1][:, pl.ds(half * 256, 256)] = kh
            kc[pl.ds(pl.multiple_of(i * B, B), B), pl.ds(half * 256, 256)] = kh.T
        vt = dot_t(wqkv_v[pl.ds(2560, 512), :], act[...])
        vT[:, pl.ds(pl.multiple_of(i * B, B), B)] = vt.astype(BF16)

        for pair in range(4):
            qt = dot_t(wqkv_v[pl.ds(pair * 512, 512), :], act[...])
            for h in range(8):
                f, b = rope(qt[h * HD:(h + 1) * HD], cos, sin)
                g = pair * 2 + h // 4
                row = (g % 2) * HD
                cols = pl.ds((h % 4) * B, B)
                qT[g, pl.ds(row, HD // 2), cols] = (f * 0.125).astype(BF16)
                qT[g, pl.ds(row + HD // 2, HD // 2), cols] = (b * 0.125).astype(BF16)

    def make_mask(i):
        key = lax.broadcasted_iota(jnp.int32, mask.shape, 0)
        tok = lax.broadcasted_iota(jnp.int32, mask.shape, 1)
        key = jnp.where(tok < B, key, key + B // 2)
        tok = jnp.where(tok < B, tok, tok - B // 2)
        ok = (key <= tok) & (key + i * B < valid_pos)
        mask[...] = jnp.where(ok, 0.0, NEG).astype(F32)

    def attend(n):
        spans = [(c * B, min(B, VMAX - c * B), 0) for c in range(n + 1)]
        if spans[-1][1] == B:
            spans[-1:] = [(n * B, B // 2, 0), (n * B + B // 2, B // 2, B // 2)]
        total = spans[-1][0] + spans[-1][1]
        ahead_by = 1 if n == NB - 2 else 2

        def scores(g, u):
            kcols = pl.ds(pl.multiple_of((g // 2) * 128, 128), 128)
            q = qT[g, :, pl.ds((u % 4) * B, B)]
            m = None
            for start, rows, lane in spans:
                keys = kc[pl.ds(start, rows), kcols]
                if start >= n * B:
                    s = dot(keys, q[:, lane:]) + mask[pl.ds(0, rows), pl.ds(2 * lane, B - lane)]
                elif start >= VMIN and n == NB - 1:
                    bias = vbias[pl.ds(start - VMIN, rows), :]
                    s = dot(keys, q) + jnp.concatenate([bias, bias], axis=1)
                elif start >= VMIN:
                    bias = kbias[pl.ds(start - VMIN, rows), :]
                    s = dot(jnp.concatenate([keys, bias], axis=1), jnp.concatenate([q, qones[...]], axis=0))
                else:
                    s = dot(keys, q)
                y[pl.ds((u % SB) * total + start, rows), pl.ds(lane, B - lane)] = s
                cm = jnp.max(s.reshape(rows // 8, 8, B - lane), axis=0)
                if lane:
                    m = jnp.concatenate([m[:, :lane], jnp.maximum(m[:, lane:], cm)], axis=1)
                else:
                    m = cm if m is None else jnp.maximum(m, cm)
            mbuf[u % SB] = m

        def weighted(g, u):
            mc = jnp.max(mbuf[u % SB], axis=0, keepdims=True) * EXP_SCALE
            l = None
            probs = []
            for start, rows, lane in spans:
                sc = y[pl.ds((u % SB) * total + start, rows), pl.ds(lane, B - lane)]
                p = jnp.exp2(sc * EXP_SCALE - mc[:, lane:])
                ls = jnp.sum(p.reshape(rows // 8, 8, B - lane), axis=0)
                p = p.astype(BF16)
                if lane:
                    l = jnp.concatenate([l[:, :lane], l[:, lane:] + ls], axis=1)
                    p = jnp.concatenate([jnp.zeros((rows, lane), BF16), p], axis=1)
                else:
                    l = ls if l is None else l + ls
                probs.append(p)
            o = dot(vT[pl.ds(pl.multiple_of(g * HD, HD), HD), pl.ds(0, total)], jnp.concatenate(probs, axis=0))
            return (o * (1.0 / jnp.sum(l, axis=0, keepdims=True))).astype(BF16)

        def put_out(g):
            act[:, pl.ds(pl.multiple_of(g * 256, 256), 256)] = ff_s[0][:, pl.ds(0, 256)].T

        for u in range(ahead_by):
            scores(0, u)

        def group_pair(pair, _):
            g = pair * 2
            outs = []
            for u in range(8):
                ahead = u + ahead_by
                scores(g + ahead // 4 if ahead < 8 else lax.rem(g + 2, KV), ahead)
                outs.append(weighted(g + u // 4, u))
                if u == 0:
                    put_out(lax.rem(g + KV - 1, KV))
                if u == 3:
                    act[:, pl.ds(pl.multiple_of(g * 256, 256), 256)] = jnp.concatenate(outs, axis=0).T
                    outs = []
            for h in range(4):
                ff_s[0][pl.ds(h * HD, HD), pl.ds(0, 256)] = outs[h]
            return 0

        lax.fori_loop(0, KV // 2, group_pair, 0)
        put_out(KV - 1)

    def out_proj(slot):
        for n in range(4):
            cols = pl.ds(n * 512, 512)
            o = dot(act[pl.ds(0, B), :], wo_v[:, cols])
            resid[slot, :, cols] = (resid[slot, :, cols].astype(F32) + o).astype(BF16)

    def lend_copies(c):
        sem = lend_sem
        cols = pl.ds(pl.multiple_of(LEND_AT + c * F, F), F)
        rows = pl.ds(pl.multiple_of(c * F, F), F)
        return [pltpu.make_async_remote_copy(src, dst, sem.at[n], borrow_sem.at[n, c], device_id={"stage": partner},
                                             device_id_type=pl.DeviceIdType.MESH)
                for n, (src, dst) in enumerate(((wg.at[:, cols], wg_x.at[:, rows]), (wu.at[:, cols], wu_x.at[:, rows]),
                                                (wd.at[cols, :], wd_x.at[rows, :])))]

    def borrowed_copies(c):
        part = pl.ds(c * F, F)
        return (pltpu.make_async_copy(wg_x.at[:, part], wg_s[c], g_sem.at[c]),
                pltpu.make_async_copy(wu_x.at[:, part], wu_s[c], u_sem.at[c]),
                pltpu.make_async_copy(wd_x.at[part, :], wd_s[c], d_sem.at[c]))

    def pair_copy(src, dst, n):
        return pltpu.make_async_remote_copy(src, dst, pair_sem.at[2 * n], pair_sem.at[2 * n + 1],
                                            device_id={"stage": partner}, device_id_type=pl.DeviceIdType.MESH)

    def act_copy():
        return pair_copy(act, act, 0)

    def sum_copy():
        return pair_copy(y.at[pl.ds(0, 8 * B), :], y.at[pl.ds(8 * B, 8 * B), :], 1)

    def gate_up(s, first=0, rows=B):
        x = act[pl.ds(first, rows), :]
        gate = dot(x, wg_s[s][...])
        up = dot(x, wu_s[s][...])
        ff_s[s % 2][pl.ds(first, rows), :] = (gate * jax.nn.sigmoid(gate) * up).astype(BF16)

    def down(s, first=0, rows=B):
        x = ff_s[s % 2][pl.ds(first, rows), :]
        for n in range(8):
            part = pl.ds(n * B + first, rows)
            y[part, :] = y[part, :] + dot(x, wd_s[s][:, pl.ds(n * 256, 256)])

    def wait_gu(s):
        for cp in gu_copy(0, s):
            cp.wait()

    def wait_dn(s):
        dn_copy(0, s).wait()

    def start_gu(c, s, ok):
        @pl.when(ok)
        def _():
            for cp in gu_copy(lax.rem(c, NC), s):
                cp.start()

    def start_dn(c, s, ok):
        @pl.when(ok)
        def _():
            dn_copy(lax.rem(c, NC), s).start()

    def mlp(i, half_done):
        shared = (i == NB - 1) & jnp.logical_not(helper)
        mine = jnp.where(shared, NC - R, NC)

        def fetch(start, idx, slot):
            start(idx + (NC - R) * i, slot, (i < NB) & (idx < mine))

        @pl.when((i == 0) | (i == NB))
        def _():
            wait_gu(0)

        gate_up(0)
        fetch(start_gu, R, 0)

        def steps(it, _):
            c = it * R
            for u in range(R):
                if u % 2 == 0:
                    @pl.when((i == 0) | (it > 0))
                    def _():
                        wait_gu(u + 1)
                        wait_dn(u)
                        wait_dn(u + 1)
                        if u + 2 < R:
                            wait_gu(u + 2)

                    if u + 2 == R:
                        wait_gu(0)
                gate_up((u + 1) % R)
                fetch(start_gu, c + u + 1 + R, (u + 1) % R)
                down(u)
                fetch(start_dn, c + u + R, u)
            return 0

        lax.fori_loop(0, jnp.where(i < NB, jnp.where(shared, NC // R - 2, NC // R - 1), 0), steps, 0)
        for half in range(2):
            for u in range(R):
                if u % 2 == 0 and half == 0:
                    wait_gu(u + 1)
                    if u + 2 < R:
                        wait_gu(u + 2)
                    wait_dn(u)
                    wait_dn(u + 1)
                if u + 1 < R:
                    gate_up(u + 1, half * PIECE, PIECE)
                down(u, half * PIECE, PIECE)
            half_done(half)

    def next_copy(i, r):
        slot = lax.rem(i, NS)
        part = resid.at[slot, pl.ds(r * PIECE, PIECE), :]
        return pltpu.make_async_remote_copy(part, part, send_sem.at[slot, r], in_sem.at[slot],
                                            device_id={"stage": lax.rem(stage + 1, STAGES)},
                                            device_id_type=pl.DeviceIdType.MESH)

    def piece_copy(i, r):
        slot = lax.rem(i, NS)
        piece = i * PER + r
        row = lax.rem(piece, 3)
        src = resid.at[slot, pl.ds(r * PIECE, PIECE), :]
        dst = hid.at[pl.ds(pl.multiple_of(row * PIECE, PIECE), PIECE), :]
        remote = pltpu.make_async_remote_copy(src, dst, piece_sem.at[slot, r], out_sem.at[row],
                                              device_id={"stage": piece // 3}, device_id_type=pl.DeviceIdType.MESH)
        return remote, pltpu.make_async_copy(src, dst, out_sem.at[row]), piece // 3 == STAGES - 1

    def k_copy(i, half):
        cols = pl.ds(pl.multiple_of(i * B, B), B)
        return pltpu.make_async_copy(ff_s[1].at[:, pl.ds(half * 256, 256)], kout.at[pl.ds(half * 256, 256), cols],
                                     kv_sem.at[half])

    def v_copy(i):
        cols = pl.ds(pl.multiple_of(i * B, B), B)
        return pltpu.make_async_copy(vT.at[:, cols], vout.at[:, cols], kv_sem.at[2])

    last = stage == STAGES - 1

    def block(i, _):
        slot = lax.rem(i, NS)
        main = i < NB
        shared = (i == NB - 1) & jnp.logical_not(helper)

        @pl.when(main)
        def _():
            emb_copy(i).wait()

            @pl.when((stage == 0) & (i >= 1) & (i + 1 < NB))
            def _():
                emb_copy(i + 1).start()

            @pl.when(i == 0)
            def _():
                for cp in small_copies:
                    cp.wait()

            norm(slot, again)

            @pl.when(i == 0)
            def _():
                for p in range(6):
                    w_copy(p).wait()
                for p in range(6, 10):
                    w_copy(p).start()
                for c in range(2):
                    start_gu(c, c, True)
                    start_dn(c, c, True)

            project(i)

            @pl.when(i == 0)
            def _():
                for c in range(2, R):
                    start_gu(c, c, True)
                    start_dn(c, c, True)
                pl.semaphore_wait(barrier, STAGES - 1)

            make_mask(i)
            k_copy(i, 0).start()
            k_copy(i, 1).start()
            v_copy(i).start()

        for n in range(NB):
            @pl.when(i == n)
            def _():
                attend(n)

        @pl.when(main)
        def _():
            @pl.when((i >= 1) & jnp.logical_not(last))
            def _():
                for r in range(PER):
                    next_copy(i - 1, r).wait_send()

            for r in range(PER):
                remote, local, mine = piece_copy(i - 1, r)

                @pl.when((i >= 1) & last & jnp.logical_not(mine))
                def _():
                    remote.wait_send()

            @pl.when((stage > 0) & (i >= 1) & (i - 1 + NS < NB))
            def _():
                pl.semaphore_signal(credit, inc=1, device_id={"stage": lax.rem(stage + STAGES - 1, STAGES)},
                                    device_id_type=pl.DeviceIdType.MESH)

            @pl.when((stage == 0) & (i == 0))
            def _():
                emb_copy(1).start()

            @pl.when(i == 0)
            def _():
                for p in range(6, 10):
                    w_copy(p).wait()

            @pl.when(jnp.logical_not(last) & (i >= NS))
            def _():
                pl.semaphore_wait(credit, 1)

            k_copy(i, 0).wait()
            k_copy(i, 1).wait()
            v_copy(i).wait()
            out_proj(slot)
            norm(slot, mgain)
            for n in range(8):
                y[pl.ds(n * B, B), :] = resid[slot, :, pl.ds(n * 256, 256)].astype(F32)

            @pl.when(shared)
            def _():
                act_copy().start()

        @pl.when(jnp.logical_not(main))
        def _():
            for c in range(R):
                for cp in lend_copies(c):
                    cp.wait_recv()
                for cp in borrowed_copies(c):
                    cp.start()
            y[pl.ds(0, 8 * B), :] = jnp.zeros((8 * B, B), F32)
            act_copy().wait_recv()

        def send(r, ok):
            remote, local, mine = piece_copy(i, r)

            @pl.when(ok & jnp.logical_not(last))
            def _():
                next_copy(i, r).start()

            @pl.when(ok & last & jnp.logical_not(mine))
            def _():
                remote.start()

            @pl.when(ok & last & mine)
            def _():
                local.start()

        def half_done(half):
            for n in range(8):
                resid[slot, pl.ds(half * PIECE, PIECE), pl.ds(n * 256, 256)] = \
                    y[pl.ds(n * B + half * PIECE, PIECE), :].astype(BF16)
            send(half, main & jnp.logical_not(shared))

        mlp(i, half_done)

        @pl.when(shared)
        def _():
            act_copy().wait_send()
            sum_copy().wait_recv()
            for n in range(8):
                h = y[pl.ds(n * B, B), :] + y[pl.ds((n + 8) * B, B), :]
                resid[slot, :, pl.ds(n * 256, 256)] = h.astype(BF16)

        for r in range(PER):
            send(r, shared)

        @pl.when(jnp.logical_not(main))
        def _():
            sum_copy().start()
            sum_copy().wait_send()

        @pl.when(main)
        def _():
            @pl.when(jnp.logical_not(helper) & (i >= 1) & (i <= R))
            def _():
                for cp in lend_copies(i - 1):
                    cp.wait_send()

            @pl.when(jnp.logical_not(helper) & (i < R))
            def _():
                for cp in lend_copies(i):
                    cp.start()

        return 0

    lax.fori_loop(0, NB + jnp.where(helper, 1, 0), block, 0)

    @pl.when(jnp.logical_not(last))
    def _():
        for r in range(PER):
            next_copy(NB - 1, r).wait_send()

    for row in range(3):
        piece_copy(row // PER, row % PER)[1].wait()

def place_kernel(hid, k_t, v_t, hid_out, k_out, v_out, hid_v, k_v, v_v, in_sem, out_sem):
    halves = []
    for n, (src, buf, dst) in enumerate(((hid, hid_v, hid_out), (k_t, k_v, k_out), (v_t, v_v, v_out))):
        rows = src.shape[0] // 2
        for half in range(2):
            part = pl.ds(half * rows, rows)
            halves.append((pltpu.make_async_copy(src.at[part], buf.at[part], in_sem.at[n, half]),
                           pltpu.make_async_copy(buf.at[part], dst.at[part], out_sem.at[n, half])))
    for load, _ in halves:
        load.start()
    for load, store in halves:
        load.wait()
        store.start()
    for _, store in halves:
        store.wait()


def solution(mesh):
    gain_spec = P('stage', None)
    spec_three = P('stage', None, None)
    spec_four = P('stage', None, None, None)
    table = rope_tables()
    dma = pltpu.SemaphoreType.DMA

    def stage_program(embeddings, valid_len, attn_gain, w_q, w_k, w_v, w_o, mlp_gain, w_gate, w_up, w_down):
        wq = w_q[0].transpose(1, 2, 0).reshape(HEADS * HD, D)
        wk = w_k[0].transpose(1, 2, 0).reshape(KV * HD, D)
        wv = w_v[0].transpose(1, 2, 0).reshape(KV * HD, D)
        wo = w_o[0].reshape(HEADS * HD, D)
        any_spec = pl.BlockSpec(memory_space=pl.ANY)
        vmem_spec = pl.BlockSpec(memory_space=pltpu.VMEM)
        smem_spec = pl.BlockSpec(memory_space=pltpu.SMEM)
        hid, k_t, v_t, _, _, _ = pl.pallas_call(
            stage_kernel,
            name="stage_pipeline",
            out_shape=(jax.ShapeDtypeStruct((SEQ // STAGES, D), BF16),
                       jax.ShapeDtypeStruct((KV * HD, SEQ), BF16),
                       jax.ShapeDtypeStruct((KV * HD, SEQ), BF16),
                       jax.ShapeDtypeStruct((D, LENT), BF16),
                       jax.ShapeDtypeStruct((D, LENT), BF16),
                       jax.ShapeDtypeStruct((LENT, D), BF16)),
            in_specs=[any_spec, smem_spec, any_spec, any_spec, any_spec, any_spec, any_spec, any_spec,
                      any_spec, any_spec, any_spec, any_spec],
            out_specs=(any_spec,) * 6,
            scratch_shapes=[
                pltpu.VMEM((NB, 2, HD // 2, 256), F32),
                pltpu.VMEM((1, D), F32),
                pltpu.VMEM((1, D), F32),
                pltpu.VMEM((3072, D), BF16),
                pltpu.VMEM((D, D), BF16),
                [pltpu.VMEM((D, F), BF16)] * R,
                [pltpu.VMEM((D, F), BF16)] * R,
                [pltpu.VMEM((F, D), BF16)] * R,
                pltpu.VMEM((NS, B, D), BF16),
                pltpu.VMEM((SEQ, KV * HD), BF16),
                pltpu.VMEM((KV * HD, SEQ), BF16),
                pltpu.VMEM((256, D), BF16),
                pltpu.VMEM((KV, 2 * HD, 4 * B), BF16),
                pltpu.VMEM((SB * VMAX, B), F32),
                pltpu.VMEM((SB, 8, B), F32),
                [pltpu.VMEM((B, F), BF16)] * 2,
                pltpu.VMEM((B // 2, B + B // 2), F32),
                pltpu.VMEM((VMAX - VMIN, 128), F32),
                pltpu.VMEM((B, 128), BF16),
                pltpu.VMEM((128, B), BF16),
                dma((10,)), dma((3,)), dma((R,)), dma((R,)), dma((R,)), dma((NS,)), dma((NS, PER)), dma((3,)), dma((NS, PER)), dma((3,)),
                dma((3,)), dma((3, R)), dma((4,)),
                pltpu.SemaphoreType.REGULAR,
            ],
            compiler_params=pltpu.CompilerParams(collective_id=0, has_side_effects=True,
                                                 vmem_limit_bytes=67043328),
        )(embeddings, valid_len, attn_gain, wq, wk, wv, wo, mlp_gain, w_gate[0], w_up[0], w_down[0],
          jnp.asarray(table))

        hid, k_t, v_t = pl.pallas_call(
            place_kernel,
            name="place",
            out_shape=tuple(jax.ShapeDtypeStruct(x.shape, BF16) for x in (hid, k_t, v_t)),
            in_specs=[any_spec] * 3,
            out_specs=(any_spec,) * 3,
            scratch_shapes=[pltpu.VMEM(x.shape, BF16) for x in (hid, k_t, v_t)] + [dma((3, 2)), dma((3, 2))],
            compiler_params=pltpu.CompilerParams(vmem_limit_bytes=67043328),
        )(hid, k_t, v_t)

        def to_cache(x):
            return x.reshape(KV, HD, SEQ).transpose(2, 0, 1)[None]

        return hid, to_cache(k_t), to_cache(v_t)

    return jax.shard_map(stage_program, mesh=mesh,
                         in_specs=(P('replica', None), P('replica'), gain_spec, spec_four, spec_four, spec_four, spec_four,
                                   gain_spec, spec_three, spec_three, spec_three),
                         out_specs=(P(('replica', 'stage'), None), P('stage', 'replica', None, None), P('stage', 'replica', None, None)),
                         check_vma=False)
```
